16 devices in a mesh: dp: 2 (over y, z), sp: 8 (over x, core).
Axes of the slice: x: 4, y: 2, z: 1, core: 2. Of those that a mesh axis runs over, the one named last changes fastest.
The devices are a block of a 4x4x8 slice.
Arguments:
- x_in: bfloat16 [4, 8192, 768], P('dp', 'sp'), parts along dimension 0
- grad_y: bfloat16 [4, 8192, 768], P('dp', 'sp'), parts along dimension 0
- ln_gain: float32 [768], replicated
- ln_bias: float32 [768], replicated
- w_qkv: bfloat16 [768, 2304], replicated
- w_out: bfloat16 [768, 768], replicated
- temp_tau: float32 [16], replicated
Outputs:
- output 1: bfloat16 [4, 8192, 768], P('dp', 'sp'), parts along dimension 0
- output 2: bfloat16 [4, 8192, 768], P('dp', 'sp'), parts along dimension 0
- output 3: bfloat16 [1536, 2304], P(('dp', 'sp')), parts along dimension 0
- output 4: bfloat16 [1536, 768], P(('dp', 'sp')), parts along dimension 0
- output 5: float32 [1536], P('dp'), parts along dimension 0
- output 6: float32 [1536], P('dp'), parts along dimension 0
- output 7: float32 [32], P('dp'), parts along dimension 0
There are 2 independent parts. The reference program is written for one: setup_inputs(seed, part) draws one part's arguments, and reference() takes and returns one part's arrays. A program takes and returns all parts, laid end to end along the dimension named above; an argument that names none is the same for every part.
All inputs are finite; a program needn't handle non-finite values.
Results may differ from the reference program's by a relative error of at most 0.00885654.
Values are sent between devices in bfloat16 or wider.
A program may use at most 768 MiB of HBM per device.

```python
import math
import jax
import jax.numpy as jnp
from jax import lax

NUM_IMAGES = 2
SEQ_LEN = 8192
MODEL_DIM = 768
NUM_HEADS = 16
HEAD_DIM = MODEL_DIM // NUM_HEADS
LN_EPS = 1e-6


def setup_inputs(seed: int = 0, part: int = 0) -> dict:
    base_key = jax.random.key(seed)
    part_keys = jax.random.split(jax.random.fold_in(base_key, part), 4)
    shared_keys = jax.random.split(base_key, 5)
    positions = (jnp.arange(SEQ_LEN, dtype=jnp.float32) + 0.5) / SEQ_LEN
    frequencies = jnp.arange(1, 5, dtype=jnp.float32)
    phases = 2.0 * math.pi * jax.random.uniform(part_keys[0], (NUM_IMAGES, 4), jnp.float32)
    wave_basis = jnp.sin(2.0 * math.pi * frequencies[None, :, None] * positions[None, None, :] + phases[:, :, None])
    mode_vecs = jax.random.normal(part_keys[1], (NUM_IMAGES, 4, MODEL_DIM), jnp.float32)
    trend_part = jnp.einsum("bmn,bmd->bnd", wave_basis, mode_vecs)
    noise_part = jax.random.normal(part_keys[2], (NUM_IMAGES, SEQ_LEN, MODEL_DIM), jnp.float32)
    x_in = (noise_part + trend_part).astype(jnp.bfloat16)
    grad_y = jax.random.normal(part_keys[3], (NUM_IMAGES, SEQ_LEN, MODEL_DIM), jnp.float32).astype(jnp.bfloat16)
    fan_scale = MODEL_DIM ** -0.5
    ln_gain = 1.0 + 0.3 * jax.random.normal(shared_keys[0], (MODEL_DIM,), jnp.float32)
    ln_bias = 0.3 * jax.random.normal(shared_keys[1], (MODEL_DIM,), jnp.float32)
    w_qkv = (fan_scale * jax.random.normal(shared_keys[2], (MODEL_DIM, 3 * MODEL_DIM), jnp.float32)).astype(jnp.bfloat16)
    w_out = (fan_scale * jax.random.normal(shared_keys[3], (MODEL_DIM, MODEL_DIM), jnp.float32)).astype(jnp.bfloat16)
    temp_tau = jax.random.uniform(shared_keys[4], (NUM_HEADS,), jnp.float32, 3.0, 6.0)
    return {"x_in": x_in, "grad_y": grad_y, "ln_gain": ln_gain, "ln_bias": ln_bias, "w_qkv": w_qkv, "w_out": w_out, "temp_tau": temp_tau}


def block_forward(x_in, ln_gain, ln_bias, w_qkv, w_out, temp_tau):
    x_f32 = x_in.astype(jnp.float32)
    mean_x = jnp.mean(x_f32, axis=-1, keepdims=True)
    centered = x_f32 - mean_x
    var_x = jnp.mean(centered * centered, axis=-1, keepdims=True)
    normed = (centered * lax.rsqrt(var_x + LN_EPS) * ln_gain + ln_bias).astype(jnp.bfloat16)
    qkv_all = jnp.dot(normed.reshape(NUM_IMAGES * SEQ_LEN, MODEL_DIM), w_qkv, preferred_element_type=jnp.float32).astype(jnp.bfloat16)
    qkv_heads = qkv_all.reshape(NUM_IMAGES, SEQ_LEN, 3, NUM_HEADS, HEAD_DIM)
    q_f32 = qkv_heads[:, :, 0].astype(jnp.float32)
    k_f32 = qkv_heads[:, :, 1].astype(jnp.float32)
    v_f32 = qkv_heads[:, :, 2].astype(jnp.float32)
    gram_state = jnp.einsum("bnhi,bnhj->bhij", q_f32, k_f32)
    sumsq_q = jnp.sum(q_f32 * q_f32, axis=1)
    sumsq_k = jnp.sum(k_f32 * k_f32, axis=1)
    logits = temp_tau[None, :, None, None] * gram_state / jnp.sqrt(sumsq_q[..., :, None] * sumsq_k[..., None, :])
    attn_bf16 = jax.nn.softmax(logits, axis=-1).astype(jnp.bfloat16)
    heads_out = jnp.einsum("bhij,bnhj->bnhi", attn_bf16.astype(jnp.float32), v_f32).astype(jnp.bfloat16)
    projected = jnp.dot(heads_out.reshape(NUM_IMAGES * SEQ_LEN, MODEL_DIM), w_out, preferred_element_type=jnp.float32)
    return (x_f32 + projected.reshape(NUM_IMAGES, SEQ_LEN, MODEL_DIM)).astype(jnp.bfloat16)


def reference(x_in, grad_y, ln_gain, ln_bias, w_qkv, w_out, temp_tau):
    y_out, pullback = jax.vjp(block_forward, x_in, ln_gain, ln_bias, w_qkv, w_out, temp_tau)
    grad_x, grad_gain, grad_bias, grad_wqkv, grad_wout, grad_tau = pullback(grad_y)
    return (y_out, grad_x, grad_wqkv, grad_wout, grad_gain, grad_bias, grad_tau)
```

```python
import functools

import jax
import jax.numpy as jnp
from jax import lax
from jax.experimental import pallas as pl
from jax.experimental.pallas import tpu as pltpu
from jax.sharding import PartitionSpec as P

LN_EPS = 1e-6
F32 = jnp.float32
BF16 = jnp.bfloat16
LANES = 128
TOK = 512
COLS = 256
NN = (((1,), (0,)), ((), ()))
NT = (((1,), (1,)), ((), ()))


def mm(a, b, dims=NN):
    return lax.dot_general(a, b, dims, preferred_element_type=F32)


def xca_kernel(
    n, heads,
    x_hbm, dy_hbm, gain_ref, bias_ref, wqkv_hbm, wo_hbm, tau_ref,
    y_hbm, dx_hbm, dwqkv_ref, dwo_ref, dgain_ref, dbias_ref, dtau_ref,
    x_v, dy_v, w_v, wt_v, wo_v, ut, zt, dot_v, ot, y_st,
    sq_acc, gs_out, gs_in, gs_sum, a_all, ds_out, ds_in, g_all, c_all, bd, colq, colk, dgb, gb_out, gb_all,
    part, r1, r2, r3,
    in_sem, out_sem, d2d_s, d2d_r, p1_s, p1_r, p2_s, p2_r,
    gs_s, gs_r, a_s, a_r, ds_s, ds_r, g_s, g_r, c_s, c_r, gb_s, gb_r,
):
    images, tokens, dim = x_hbm.shape
    hd = dim // heads
    rows = images * tokens
    per_dev = dim // n
    chips = n // 2
    wheads = COLS // hd
    wrow = wheads * hd
    nwin = -(-heads // wheads)
    tiles = tokens // TOK
    o_chunks = dim // COLS
    chunks = 4 * o_chunks
    me = lax.axis_index("sp")
    chip, core = me // 2, me % 2
    right = ((chip + 1) % chips) * 2 + core
    left = ((chip + chips - 1) % chips) * 2 + core
    partner = chip * 2 + (1 - core)
    cr, cl, co = (chip + 1) % chips, (chip + chips - 1) % chips, (chip + 2) % chips

    def rcopy(src, dst, ss, rs, dev):
        return pltpu.make_async_remote_copy(
            src_ref=src, dst_ref=dst, send_sem=ss, recv_sem=rs,
            device_id={"sp": dev}, device_id_type=pl.DeviceIdType.MESH)

    def cp_x(b):
        return pltpu.make_async_copy(x_hbm.at[b], x_v.at[pl.ds(b * tokens, tokens)], in_sem.at[b])

    def cp_dy(b):
        return pltpu.make_async_copy(dy_hbm.at[b], dy_v.at[pl.ds(b * tokens, tokens)], in_sem.at[2 + b])

    cp_w = pltpu.make_async_copy(wqkv_hbm, w_v, in_sem.at[4])
    cp_wo = pltpu.make_async_copy(wo_hbm, wo_v, in_sem.at[5])
    cp_w.start()
    cp_x(0).start()
    cp_x(1).start()
    cp_wo.start()
    cp_dy(0).start()
    cp_dy(1).start()

    barrier = pltpu.get_barrier_semaphore()
    for k in range(1, n):
        pl.semaphore_signal(barrier, inc=1, device_id={"sp": (me + k) % n},
                            device_id_type=pl.DeviceIdType.MESH)

    sq_acc[...] = jnp.zeros_like(sq_acc)
    bd[...] = jnp.zeros_like(bd)
    dgb[...] = jnp.zeros_like(dgb)

    cp_w.wait()

    def wt_body(i, _):
        off = pl.multiple_of(i * COLS, COLS)
        wt_v[pl.ds(off, COLS), :] = w_v[:, pl.ds(off, COLS)].T
        return 0
    lax.fori_loop(0, 3 * dim // COLS, wt_body, 0)

    def norm(xt):
        mean = jnp.sum(xt, axis=-1, keepdims=True) * (1.0 / dim)
        cen = xt - mean
        inv = lax.rsqrt(jnp.sum(cen * cen, axis=-1, keepdims=True) * (1.0 / dim) + LN_EPS)
        return cen * inv, inv

    gain_row = gain_ref[...]
    bias_row = bias_ref[...]

    lane_w = lax.broadcasted_iota(jnp.int32, (hd, LANES), 1)

    def to_pairs(blocks, out_ref):
        for d in range(n):
            picked = []
            for s in range(2):
                w, k = divmod(2 * d + s, wheads)
                strip = blocks[w][k * hd:(k + 1) * hd, :]
                shift = (s * hd - k * hd) % COLS
                if shift:
                    strip = pltpu.roll(strip, shift, 1)
                picked.append(strip[:, :LANES])
            out_ref[d, 0:hd, :] = jnp.where(lane_w < hd, picked[0], jnp.where(lane_w < 2 * hd, picked[1], 0.0))

    def gram(b, l_ref, l0, r_ref, r0):
        blocks = []
        for w in range(nwin):
            m = min(wrow, dim - w * wrow)
            lo, ro = l0 + w * wrow, r0 + w * wrow
            nw = min(COLS, dim - w * wrow)
            left_op = l_ref[lo:lo + m, b * tokens:(b + 1) * tokens]
            right_op = r_ref[ro:ro + nw, b * tokens:(b + 1) * tokens]
            g = mm(left_op, right_op, NT)
            if nw < COLS:
                g = jnp.concatenate([g, jnp.zeros((m, COLS - nw), F32)], axis=1) if nw % LANES == 0 else jnp.pad(g, ((0, 0), (0, COLS - nw)))
            blocks.append(g)
        return blocks

    for b in range(images):
        cp_x(b).wait()

        def qk_body(t, _):
            off = pl.multiple_of(b * tokens + t * TOK, TOK)
            xt = x_v[pl.ds(off, TOK), :].astype(F32)
            x_hat, _inv = norm(xt)
            u = (x_hat * gain_row + bias_row).astype(BF16)
            u_t = u.T
            ut[:, pl.ds(off, TOK)] = u_t
            for m in range(2):
                z = mm(wt_v[m * dim:(m + 1) * dim, :], ut[:, pl.ds(off, TOK)]).astype(BF16)
                zt[m * dim:(m + 1) * dim, pl.ds(off, TOK)] = z
                zf = z.astype(F32)
                sq = zf * zf
                tot = sq[:, 0:LANES]
                for j in range(1, TOK // LANES):
                    tot = tot + sq[:, j * LANES:(j + 1) * LANES]
                sq_acc[b, m] += tot
            return 0
        lax.fori_loop(0, tiles, qk_body, 0)
        to_pairs(gram(b, zt, 0, zt, dim), gs_out.at[b])
        q_row = jnp.sum(sq_acc[b, 0].T, axis=0, keepdims=True)
        k_row = jnp.sum(sq_acc[b, 1].T, axis=0, keepdims=True)
        sub8 = lax.broadcasted_iota(jnp.int32, (8, dim), 0)
        qk = jnp.where(sub8 == 0, q_row, jnp.where(sub8 == 1, k_row, 0.0))
        for d in range(n):
            s0 = d * per_dev
            base = s0 // LANES * LANES
            if base + COLS <= dim:
                wide = qk[:, base:base + COLS]
                if s0 - base:
                    wide = pltpu.roll(wide, COLS - (s0 - base), 1)
                piece = wide[:, :LANES]
            else:
                base = dim - COLS
                wide = pltpu.roll(qk[:, base:dim], COLS - (s0 - base), 1)
                piece = wide[:, :LANES]
            gs_out[b, d, hd:hd + 8, :] = piece
        if b == 0:
            pl.semaphore_wait(barrier, n - 1)
        for k in range(1, n):
            dst = (me + k) % n
            rcopy(gs_out.at[b, dst], gs_in.at[b, k - 1], gs_s.at[b, k - 1], gs_r.at[b, k - 1], dst).start()

    def v_body(t, _):
        off = pl.multiple_of(t * TOK, TOK)
        zt[2 * dim:3 * dim, pl.ds(off, TOK)] = mm(wt_v[2 * dim:3 * dim, :], ut[:, pl.ds(off, TOK)]).astype(BF16)
        return 0
    lax.fori_loop(0, images * tiles, v_body, 0)

    eye = lax.broadcasted_iota(jnp.int32, (hd, hd), 0) == lax.broadcasted_iota(jnp.int32, (hd, hd), 1)

    def col_of(row):
        return jnp.sum(jnp.where(eye, row, 0.0), axis=1, keepdims=True)

    def row_of(col):
        return jnp.sum(jnp.where(eye, col, 0.0), axis=0, keepdims=True)

    def attn_state(b, s):
        blk = gs_sum[b]
        sl = slice(s * hd, (s + 1) * hd)
        g = blk[0:hd, sl]
        qr = blk[hd:hd + 1, sl]
        kr = blk[hd + 1:hd + 2, sl]
        unit = lax.rsqrt(col_of(qr)) * lax.rsqrt(kr)
        tau = tau_ref[me * 2 + s]
        cosine = g * unit
        logits = tau * cosine
        e = jnp.exp(logits - jnp.max(logits, axis=-1, keepdims=True))
        probs = e / jnp.sum(e, axis=-1, keepdims=True)
        return cosine, logits, probs, tau * unit, qr, kr

    def pair(a0, a1):
        r = a0.shape[0]
        z = jnp.zeros((r, LANES - 2 * hd), a0.dtype)
        return jnp.concatenate([a0, a1, z], axis=1)

    def owner_forward(b):
        for k in range(1, n):
            rcopy(gs_out.at[b, 0], gs_in.at[b, k - 1], gs_s.at[b, k - 1], gs_r.at[b, k - 1], me).wait_recv()
        tot = gs_out[b, me]
        for k in range(1, n):
            tot = tot + gs_in[b, k - 1]
        gs_sum[b] = tot
        p0 = attn_state(b, 0)[2]
        p1 = attn_state(b, 1)[2]
        a_all[b, me] = pair(p0, p1).astype(BF16)
        for k in range(1, n):
            dst = (me + k) % n
            rcopy(a_all.at[b, me], a_all.at[b, me], a_s.at[b, k - 1], a_r.at[b, k - 1], dst).start()

    def owner_backward(b):
        for k in range(1, n):
            rcopy(ds_out.at[b, 0], ds_in.at[b, k - 1], ds_s.at[b, k - 1], ds_r.at[b, k - 1], me).wait_recv()
        tot = ds_out[b, me]
        for k in range(1, n):
            tot = tot + ds_in[b, k - 1]
        tot = tot.astype(BF16).astype(F32)
        gs, qs, ks, ts = [], [], [], []
        for s in range(2):
            cosine, logits, probs, scale, qr, kr = attn_state(b, s)
            dp = tot[:, s * hd:(s + 1) * hd]
            gl = probs * (dp - jnp.sum(probs * dp, axis=-1, keepdims=True))
            weighted = gl * logits
            gs.append(gl * scale)
            qs.append(-row_of(jnp.sum(weighted, axis=1, keepdims=True)) / qr)
            ks.append(-jnp.sum(weighted, axis=0, keepdims=True) / kr)
            ts.append(jnp.sum(jnp.sum(gl * cosine, axis=1, keepdims=True), axis=0, keepdims=True))
        g_all[b, me] = pair(gs[0], gs[1]).astype(BF16)
        sub = lax.broadcasted_iota(jnp.int32, (8, LANES), 0)
        lane = lax.broadcasted_iota(jnp.int32, (8, LANES), 1)
        taus = jnp.where(lane == 0, ts[0], jnp.where(lane == 1, ts[1], 0.0))
        c_all[b, me] = jnp.where(sub == 0, pair(qs[0], qs[1]), jnp.where(sub == 1, pair(ks[0], ks[1]), jnp.where(sub == 2, taus, 0.0)))
        for k in range(1, n):
            dst = (me + k) % n
            rcopy(g_all.at[b, me], g_all.at[b, me], g_s.at[b, k - 1], g_r.at[b, k - 1], dst).start()
            rcopy(c_all.at[b, me], c_all.at[b, me], c_s.at[b, k - 1], c_r.at[b, k - 1], dst).start()

    def gathered(ref, ss, rs, b):
        for k in range(1, n):
            src = (me + n - k) % n
            rcopy(ref.at[b, me], ref.at[b, src], ss.at[b, k - 1], rs.at[b, k - 1], me).wait_recv()

    def grad_heads(b):
        cp_dy(b).wait()
        if b == 0:
            cp_wo.wait()

        def body(t, _):
            off = pl.multiple_of(b * tokens + t * TOK, TOK)
            dot_v[:, pl.ds(off, TOK)] = mm(wo_v[...], dy_v[pl.ds(off, TOK), :], NT).astype(BF16)
            return 0
        lax.fori_loop(0, tiles, body, 0)
        to_pairs(gram(b, dot_v, 0, zt, 2 * dim), ds_out.at[b])
        for k in range(1, n):
            dst = (me + k) % n
            rcopy(ds_out.at[b, dst], ds_in.at[b, k - 1], ds_s.at[b, k - 1], ds_r.at[b, k - 1], dst).start()

    sj = lax.broadcasted_iota(jnp.int32, (LANES, COLS), 0)
    slane = lax.broadcasted_iota(jnp.int32, (LANES, COLS), 1)
    sels = []
    for s in range(2):
        hit = jnp.zeros((LANES, COLS), jnp.bool_)
        for k in range(wheads):
            hit = jnp.logical_or(hit, slane - k * hd == sj - s * hd)
        hit = jnp.logical_and(hit, jnp.logical_and(sj >= s * hd, sj < (s + 1) * hd))
        sels.append(jnp.where(hit, 1.0, 0.0).astype(BF16))
    blane = lax.broadcasted_iota(jnp.int32, (hd, COLS), 1)

    def build(ref, b):
        flat = ref[b].reshape(n * hd, LANES)
        for s in range(2):
            spread = mm(flat, sels[s])
            for d in range(n):
                w, k = divmod(2 * d + s, wheads)
                blk = jnp.where(jnp.logical_and(blane >= k * hd, blane < (k + 1) * hd), spread[d * hd:(d + 1) * hd], 0.0)
                bd[b, w, 0, k * hd:(k + 1) * hd, :] = blk.astype(BF16)
        for w in range(nwin):
            bd[b, w, 1] = bd[b, w, 0].T

    def windows():
        for w in range(nwin):
            r0 = w * wrow
            yield w, r0, min(wrow, dim - r0), min(COLS, dim - r0)

    def out_and_dv(b):
        def body(t, _):
            off = pl.multiple_of(b * tokens + t * TOK, TOK)
            for w, r0, m, kk in windows():
                ot[r0:r0 + m, pl.ds(off, TOK)] = mm(bd[b, w, 0, 0:m, 0:kk], zt[2 * dim + r0:2 * dim + r0 + kk, pl.ds(off, TOK)]).astype(BF16)
            for w, r0, m, kk in windows():
                zt[2 * dim + r0:2 * dim + r0 + m, pl.ds(off, TOK)] = mm(bd[b, w, 1, 0:m, 0:kk], dot_v[r0:r0 + kk, pl.ds(off, TOK)]).astype(BF16)
            return 0
        lax.fori_loop(0, tiles, body, 0)

    def dq_and_dk(b):
        ct = c_all[b].reshape(n * 8, LANES).T
        for d in range(n):
            colq[d * per_dev:(d + 1) * per_dev, :] = jnp.broadcast_to(ct[0:per_dev, 8 * d:8 * d + 1], (per_dev, LANES))
            colk[d * per_dev:(d + 1) * per_dev, :] = jnp.broadcast_to(ct[0:per_dev, 8 * d + 1:8 * d + 2], (per_dev, LANES))

        def body(t, _):
            off = pl.multiple_of(b * tokens + t * TOK, TOK)
            for w, r0, m, kk in windows():
                qw = zt[r0:r0 + kk, pl.ds(off, TOK)]
                kw = zt[dim + r0:dim + r0 + kk, pl.ds(off, TOK)]
                cq = jnp.concatenate([colq[r0:r0 + m, :]] * (TOK // LANES), axis=1)
                ck = jnp.concatenate([colk[r0:r0 + m, :]] * (TOK // LANES), axis=1)
                dq = mm(bd[b, w, 0, 0:m, 0:kk], kw) + cq * qw[0:m].astype(F32)
                dk = mm(bd[b, w, 1, 0:m, 0:kk], qw) + ck * kw[0:m].astype(F32)
                zt[r0:r0 + m, pl.ds(off, TOK)] = dq.astype(BF16)
                zt[dim + r0:dim + r0 + m, pl.ds(off, TOK)] = dk.astype(BF16)
            return 0
        lax.fori_loop(0, tiles, body, 0)

    def put_part(c, val):
        for j in range(n):
            part[c, j % 2, j // 2] = val[j * per_dev:(j + 1) * per_dev, :]

    def d2d(c):
        return rcopy(part.at[c, 1 - core], r1.at[c], d2d_s.at[c], d2d_r.at[c], partner)

    half = per_dev // 2

    def hop1(c):
        return (rcopy(r1.at[c, co, pl.ds(0, half)], r2.at[c, 0], p1_s.at[c, 0], p1_r.at[c, 0], right),
                rcopy(r1.at[c, co, pl.ds(half, half)], r2.at[c, 1], p1_s.at[c, 1], p1_r.at[c, 1], left))

    def hop2(c):
        return (rcopy(r1.at[c, cr], r3.at[c, 0], p2_s.at[c, 0], p2_r.at[c, 0], right),
                rcopy(r1.at[c, cl], r3.at[c, 1], p2_s.at[c, 1], p2_r.at[c, 1], left))

    def serve1(c):
        d2d(c).wait_recv()
        for blk in (co, cr, cl, chip):
            r1[c, blk] += part[c, core, blk]
        for h in hop1(c):
            h.start()

    def serve2(c):
        for h in hop1(c):
            h.wait_recv()
        r1[c, cr, 0:half] += r2[c, 0]
        r1[c, cl, half:per_dev] += r2[c, 1]
        for h in hop2(c):
            h.start()

    def serve3(c):
        for h in hop2(c):
            h.wait_recv()
        return (r1[c, chip] + r3[c, 0] + r3[c, 1]).astype(BF16)

    def wo_chunk(c, _):
        off = pl.multiple_of(c * COLS, COLS)
        put_part(c, mm(ot[...], dy_v[:, pl.ds(off, COLS)]))
        d2d(c).start()
        return 0

    def qkv_chunk(c, base):
        off = pl.multiple_of(base + c * COLS, COLS)
        put_part(c, mm(ut[...], zt[pl.ds(off, COLS), :], NT))
        d2d(c).start()

    owner_forward(0)
    grad_heads(0)
    owner_forward(1)
    grad_heads(1)
    gathered(a_all, a_s, a_r, 0)
    build(a_all, 0)
    out_and_dv(0)
    gathered(a_all, a_s, a_r, 1)
    build(a_all, 1)
    out_and_dv(1)
    owner_backward(0)
    wo_chunk(0, 0)

    def wo_loop(c, _):
        wo_chunk(c, 0)
        serve1(c - 1)
        return 0
    lax.fori_loop(1, o_chunks, wo_loop, 0)
    owner_backward(1)

    def v_loop(c, _):
        qkv_chunk(c, 2 * dim - o_chunks * COLS)
        serve1(c - 1)
        return 0
    lax.fori_loop(o_chunks, 2 * o_chunks, v_loop, 0)

    def s2_body(c, _):
        serve2(c)
        return 0
    lax.fori_loop(0, o_chunks, s2_body, 0)
    for b in range(images):
        gathered(g_all, g_s, g_r, b)
        gathered(c_all, c_s, c_r, b)
        build(g_all, b)
        dq_and_dk(b)

    def qk_loop(c, _):
        qkv_chunk(c, -2 * o_chunks * COLS)
        serve1(c - 1)
        return 0
    lax.fori_loop(2 * o_chunks, chunks, qk_loop, 0)
    serve1(chunks - 1)
    lax.fori_loop(o_chunks, chunks - 3, s2_body, 0)

    def y_copy(t):
        b = t // tiles
        return pltpu.make_async_copy(y_st.at[t], y_hbm.at[b, pl.ds(pl.multiple_of((t % tiles) * TOK, TOK), TOK)], out_sem.at[0, t])

    def dx_copy(t):
        b = t // tiles
        return pltpu.make_async_copy(x_v.at[pl.ds(pl.multiple_of(t * TOK, TOK), TOK)], dx_hbm.at[b, pl.ds(pl.multiple_of((t % tiles) * TOK, TOK), TOK)], out_sem.at[1, t])

    def y_body(t, _):
        off = pl.multiple_of(t * TOK, TOK)
        o = ot[:, pl.ds(off, TOK)].T
        y_st[t] = (x_v[pl.ds(off, TOK), :].astype(F32) + mm(o, wo_v[...])).astype(BF16)
        y_copy(t).start()
        return 0
    lax.fori_loop(0, images * tiles, y_body, 0)
    lax.fori_loop(chunks - 3, chunks, s2_body, 0)

    def dx_body(t, _):
        off = pl.multiple_of(t * TOK, TOK)
        du = mm(w_v[...], zt[:, pl.ds(off, TOK)]).astype(BF16).T.astype(F32)
        x_hat, inv = norm(x_v[pl.ds(off, TOK), :].astype(F32))
        prod = du * x_hat
        dgb[0] += jnp.sum(prod.reshape(TOK // 8, 8, dim), axis=0)
        dgb[1] += jnp.sum(du.reshape(TOK // 8, 8, dim), axis=0)
        a9 = du * gain_row
        m1 = jnp.sum(a9, axis=-1, keepdims=True) * (1.0 / dim)
        m2 = jnp.sum(a9 * x_hat, axis=-1, keepdims=True) * (1.0 / dim)
        gx = inv * (a9 - m1 - x_hat * m2)
        x_v[pl.ds(off, TOK), :] = (dy_v[pl.ds(off, TOK), :].astype(F32) + gx).astype(BF16)
        dx_copy(t).start()
        return 0
    lax.fori_loop(0, images * tiles, dx_body, 0)

    sub8 = lax.broadcasted_iota(jnp.int32, (8, dim), 0)
    gb = jnp.where(sub8 == 0, jnp.sum(dgb[0], axis=0, keepdims=True), jnp.where(sub8 == 1, jnp.sum(dgb[1], axis=0, keepdims=True), 0.0))
    gb_all[me] = gb
    for k in range(1, n):
        dst = (me + k) % n
        rcopy(gb_all.at[me], gb_all.at[me], gb_s.at[k - 1], gb_r.at[k - 1], dst).start()

    lane = lax.broadcasted_iota(jnp.int32, (1, LANES), 1)
    dtau = jnp.zeros((1, LANES), F32)
    for d in range(n):
        row = c_all[0, d, 2:3, :]
        for b in range(1, images):
            row = row + c_all[b, d, 2:3, :]
        if d:
            row = pltpu.roll(row, 2 * d, 1)
        dtau = jnp.where(jnp.logical_and(lane >= 2 * d, lane < 2 * d + 2), row, dtau)
    dtau_ref[...] = dtau

    def s3_wo(c, _):
        dwo_ref[:, pl.ds(pl.multiple_of(c * COLS, COLS), COLS)] = serve3(c)
        return 0
    lax.fori_loop(0, o_chunks, s3_wo, 0)

    def s3_v(c, _):
        dwqkv_ref[:, pl.ds(pl.multiple_of(2 * dim - dim + c * COLS, COLS), COLS)] = serve3(c)
        return 0
    lax.fori_loop(o_chunks, 2 * o_chunks, s3_v, 0)

    for k in range(1, n):
        src = (me + n - k) % n
        rcopy(gb_all.at[me], gb_all.at[src], gb_s.at[k - 1], gb_r.at[k - 1], me).wait_recv()
    tot = gb_all[0]
    for d in range(1, n):
        tot = tot + gb_all[d]
    dgain_ref[...] = tot[0:1, :]
    dbias_ref[...] = tot[1:2, :]

    def s3_qk(c, _):
        dwqkv_ref[:, pl.ds(pl.multiple_of(c * COLS - 2 * dim, COLS), COLS)] = serve3(c)
        return 0
    lax.fori_loop(2 * o_chunks, chunks, s3_qk, 0)

    for b in range(images):
        for k in range(1, n):
            rcopy(gs_out.at[b, 0], gs_in.at[b, k - 1], gs_s.at[b, k - 1], gs_r.at[b, k - 1], me).wait_send()
            rcopy(a_all.at[b, me], a_all.at[b, me], a_s.at[b, k - 1], a_r.at[b, k - 1], me).wait_send()
            rcopy(ds_out.at[b, 0], ds_in.at[b, k - 1], ds_s.at[b, k - 1], ds_r.at[b, k - 1], me).wait_send()
            rcopy(g_all.at[b, me], g_all.at[b, me], g_s.at[b, k - 1], g_r.at[b, k - 1], me).wait_send()
            rcopy(c_all.at[b, me], c_all.at[b, me], c_s.at[b, k - 1], c_r.at[b, k - 1], me).wait_send()
    for k in range(1, n):
        rcopy(gb_all.at[me], gb_all.at[me], gb_s.at[k - 1], gb_r.at[k - 1], me).wait_send()

    def drain(c, _):
        d2d(c).wait_send()
        for h in hop1(c) + hop2(c):
            h.wait_send()
        return 0
    lax.fori_loop(0, chunks, drain, 0)

    def drain_out(t, _):
        y_copy(t).wait()
        dx_copy(t).wait()
        return 0
    lax.fori_loop(0, images * tiles, drain_out, 0)


def solution(mesh):
    n = mesh.shape["sp"]

    def local_step(x_in, grad_y, ln_gain, ln_bias, w_qkv, w_out, temp_tau):
        images, tokens, dim = x_in.shape
        heads = temp_tau.shape[0]
        hd = dim // heads
        rows = images * tokens
        per_dev = dim // n
        chunks = 4 * dim // COLS
        nwin = -(-heads // (COLS // hd))
        any_spec = pl.BlockSpec(memory_space=pl.ANY)
        vmem = pl.BlockSpec(memory_space=pltpu.VMEM)
        smem = pl.BlockSpec(memory_space=pltpu.SMEM)
        dma = pltpu.SemaphoreType.DMA
        pairs = (images, n - 1)
        out = pl.pallas_call(
            functools.partial(xca_kernel, n, heads),
            out_shape=(
                jax.ShapeDtypeStruct(x_in.shape, BF16),
                jax.ShapeDtypeStruct(x_in.shape, BF16),
                jax.ShapeDtypeStruct((per_dev, 3 * dim), BF16),
                jax.ShapeDtypeStruct((per_dev, dim), BF16),
                jax.ShapeDtypeStruct((1, dim), F32),
                jax.ShapeDtypeStruct((1, dim), F32),
                jax.ShapeDtypeStruct((1, LANES), F32),
            ),
            in_specs=[any_spec, any_spec, vmem, vmem, any_spec, any_spec, smem],
            out_specs=(any_spec, any_spec, vmem, vmem, vmem, vmem, vmem),
            scratch_shapes=[
                pltpu.VMEM((rows, dim), BF16),
                pltpu.VMEM((rows, dim), BF16),
                pltpu.VMEM((dim, 3 * dim), BF16),
                pltpu.VMEM((3 * dim, dim), BF16),
                pltpu.VMEM((dim, dim), BF16),
                pltpu.VMEM((dim, rows), BF16),
                pltpu.VMEM((3 * dim, rows), BF16),
                pltpu.VMEM((dim, rows), BF16),
                pltpu.VMEM((dim, rows), BF16),
                pltpu.VMEM((rows // TOK, TOK, dim), BF16),
                pltpu.VMEM((images, 2, dim, LANES), F32),
                pltpu.VMEM((images, n, hd + 8, LANES), F32),
                pltpu.VMEM((images, n - 1, hd + 8, LANES), F32),
                pltpu.VMEM((images, hd + 8, LANES), F32),
                pltpu.VMEM((images, n, hd, LANES), BF16),
                pltpu.VMEM((images, n, hd, LANES), F32),
                pltpu.VMEM((images, n - 1, hd, LANES), F32),
                pltpu.VMEM((images, n, hd, LANES), BF16),
                pltpu.VMEM((images, n, 8, LANES), F32),
                pltpu.VMEM((images, nwin, 2, COLS, COLS), BF16),
                pltpu.VMEM((dim, LANES), F32),
                pltpu.VMEM((dim, LANES), F32),
                pltpu.VMEM((2, 8, dim), F32),
                pltpu.VMEM((8, dim), F32),
                pltpu.VMEM((n, 8, dim), F32),
                pltpu.VMEM((chunks, 2, n // 2, per_dev, COLS), F32),
                pltpu.VMEM((chunks, n // 2, per_dev, COLS), F32),
                pltpu.VMEM((chunks, 2, per_dev // 2, COLS), F32),
                pltpu.VMEM((chunks, 2, per_dev, COLS), F32),
                dma((6,)), dma((2, rows // TOK)),
                dma((chunks,)), dma((chunks,)),
                dma((chunks, 2)), dma((chunks, 2)), dma((chunks, 2)), dma((chunks, 2)),
                dma(pairs), dma(pairs), dma(pairs), dma(pairs), dma(pairs), dma(pairs),
                dma(pairs), dma(pairs), dma(pairs), dma(pairs),
                dma((n - 1,)), dma((n - 1,)),
            ],
            compiler_params=pltpu.CompilerParams(
                collective_id=0, has_side_effects=True, vmem_limit_bytes=67043328),
            name="xca_block",
        )(x_in, grad_y, ln_gain.reshape(1, dim), ln_bias.reshape(1, dim), w_qkv, w_out, temp_tau)
        y, dx, dwqkv, dwo, dgain, dbias, dtau = out
        return y, dx, dwqkv, dwo, dgain.reshape(dim), dbias.reshape(dim), dtau[0, :heads]

    tok = P("dp", "sp", None)
    return jax.shard_map(
        local_step, mesh=mesh,
        in_specs=(tok, tok, P(), P(), P(), P(), P()),
        out_specs=(tok, tok, P(("dp", "sp"), None), P(("dp", "sp"), None), P("dp"), P("dp"), P("dp")),
        check_vma=False)
```

```python
import functools

import jax
import jax.numpy as jnp
from jax import lax
from jax.experimental import pallas as pl
from jax.experimental.pallas import tpu as pltpu
from jax.sharding import PartitionSpec as P

LN_EPS = 1e-6
F32 = jnp.float32
BF16 = jnp.bfloat16
LANES = 128
TOK = 512
COLS = 256
NN = (((1,), (0,)), ((), ()))
NT = (((1,), (1,)), ((), ()))


def mm(a, b, dims=NN):
    return lax.dot_general(a, b, dims, preferred_element_type=F32)


def xca_kernel(
    n, heads,
    x_hbm, dy_hbm, gain_hbm, bias_hbm, wqkv_hbm, wo_hbm, tau_hbm,
    y_hbm, dx_hbm, dwqkv_ref, dwo_ref, dgain_ref, dbias_ref, dtau_ref,
    gain_ref, bias_ref, tau_ref, x_v, dy_v, w_v, wt_v, wo_v, ut, zt, dot_v, ot,
    sq_acc, gs_out, gs_in, gs_sum, a_all, ds_out, ds_in, g_all, c_all, bd, colq, colk, dgb, gb_all,
    part, r1, r2, r3,
    in_sem, out_sem, d2d_s, d2d_r, p1_s, p1_r, p2_s, p2_r,
    gs_s, gs_r, a_s, a_r, ds_s, ds_r, g_s, g_r, c_s, c_r, gb_s, gb_r,
):
    images, tokens, dim = x_hbm.shape
    hd = dim // heads
    rows = images * tokens
    per_dev = dim // n
    chips = n // 2
    wheads = COLS // hd
    wrow = wheads * hd
    nwin = -(-heads // wheads)
    tiles = tokens // TOK
    o_chunks = dim // COLS
    chunks = 4 * o_chunks
    me = lax.axis_index("sp")
    chip, core = me // 2, me % 2
    right = ((chip + 1) % chips) * 2 + core
    left = ((chip + chips - 1) % chips) * 2 + core
    partner = chip * 2 + (1 - core)
    cr, cl, co = (chip + 1) % chips, (chip + chips - 1) % chips, (chip + 2) % chips

    far_first = sorted(range(1, n), key=lambda k: abs(2 * k - n))

    def rcopy(src, dst, ss, rs, dev):
        return pltpu.make_async_remote_copy(
            src_ref=src, dst_ref=dst, send_sem=ss, recv_sem=rs,
            device_id={"sp": dev}, device_id_type=pl.DeviceIdType.MESH)

    def cp_x(b, t):
        return pltpu.make_async_copy(x_hbm.at[b, pl.ds(t * TOK, TOK)], x_v.at[pl.ds(b * tokens + t * TOK, TOK)], in_sem.at[b * tiles + t])

    def cp_dy(b):
        return pltpu.make_async_copy(dy_hbm.at[b], dy_v.at[pl.ds(b * tokens, tokens)], in_sem.at[images * tiles + b])

    base = images * tiles + images
    cp_small = [pltpu.make_async_copy(h, v, in_sem.at[base + i]) for i, (h, v) in enumerate(
        ((gain_hbm, gain_ref), (bias_hbm, bias_ref), (tau_hbm, tau_ref)))]
    base += 3
    cp_wqk = pltpu.make_async_copy(wqkv_hbm.at[:, pl.ds(0, 2 * dim)], w_v.at[:, pl.ds(0, 2 * dim)], in_sem.at[base])
    cp_wv = pltpu.make_async_copy(wqkv_hbm.at[:, pl.ds(2 * dim, dim)], w_v.at[:, pl.ds(2 * dim, dim)], in_sem.at[base + 1])
    cp_wo = pltpu.make_async_copy(wo_hbm, wo_v, in_sem.at[base + 2])
    for c in cp_small:
        c.start()
    cp_x(0, 0).start()
    cp_wqk.start()
    cp_x(0, 1).start()

    barrier = pltpu.get_barrier_semaphore()
    for k in range(1, n):
        pl.semaphore_signal(barrier, inc=1, device_id={"sp": (me + k) % n},
                            device_id_type=pl.DeviceIdType.MESH)
    sq_acc[...] = jnp.zeros_like(sq_acc)
    bd[...] = jnp.zeros_like(bd)
    dgb[...] = jnp.zeros_like(dgb)
    for c in cp_small:
        c.wait()
    cp_x(0, 0).wait()

    def norm(xt):
        mean = jnp.sum(xt, axis=-1, keepdims=True) * (1.0 / dim)
        cen = xt - mean
        inv = lax.rsqrt(jnp.sum(cen * cen, axis=-1, keepdims=True) * (1.0 / dim) + LN_EPS)
        return cen * inv, inv

    gain_row = gain_ref[...].reshape(1, dim)
    bias_row = bias_ref[...].reshape(1, dim)

    def norm_rows(r0, count):
        x_hat, _inv = norm(x_v[pl.ds(r0, count), :].astype(F32))
        ut[:, pl.ds(r0, count)] = (x_hat * gain_row + bias_row).astype(BF16).T

    def transpose_w(c0, count):
        def body(i, _):
            off = pl.multiple_of(c0 + i * COLS, COLS)
            wt_v[pl.ds(off, COLS), :] = w_v[:, pl.ds(off, COLS)].T
            return 0
        lax.fori_loop(0, count // COLS, body, 0)

    lane_w = lax.broadcasted_iota(jnp.int32, (hd, LANES), 1)

    def to_pairs(blocks, out_ref, extra=None):
        for d in range(n):
            picked = []
            for s in range(2):
                w, k = divmod(2 * d + s, wheads)
                strip = blocks[w][k * hd:(k + 1) * hd, :]
                shift = (s * hd - k * hd) % COLS
                if shift:
                    strip = pltpu.roll(strip, shift, 1)
                picked.append(strip[:, :LANES])
            rest = 0.0
            if extra is not None:
                for i, col in enumerate(extra):
                    for s in range(2):
                        r0 = (2 * d + s) * hd
                        rest = jnp.where(lane_w == 2 * hd + 2 * i + s, col[r0:r0 + hd], rest)
            out_ref[d] = jnp.where(lane_w < hd, picked[0], jnp.where(lane_w < 2 * hd, picked[1], rest))

    def gram(b, l_ref, l0, r_ref, r0):
        blocks = []
        for w in range(nwin):
            m = min(wrow, dim - w * wrow)
            lo, ro = l0 + w * wrow, r0 + w * wrow
            nw = min(COLS, dim - w * wrow)
            left_op = l_ref[lo:lo + m, b * tokens:(b + 1) * tokens]
            right_op = r_ref[ro:ro + nw, b * tokens:(b + 1) * tokens]
            g = mm(left_op, right_op, NT)
            if nw < COLS:
                g = jnp.pad(g, ((0, 0), (0, COLS - nw)))
            blocks.append(g)
        return blocks

    def qk_tile(off, following, wt_cols=None):
        for m in range(2):
            z = mm(wt_v[m * dim:(m + 1) * dim, :], ut[:, pl.ds(off, TOK)]).astype(BF16)
            zt[m * dim:(m + 1) * dim, pl.ds(off, TOK)] = z
            zf = z.astype(F32)
            sq = zf * zf
            tot = sq[:, 0:LANES]
            for j in range(1, TOK // LANES):
                tot = tot + sq[:, j * LANES:(j + 1) * LANES]
            sq_acc[off // tokens, m * dim:(m + 1) * dim] += tot
        if following is not None:
            norm_rows(following, TOK)
        if wt_cols is not None:
            wt_v[wt_cols:wt_cols + dim // 2, :] = w_v[:, wt_cols:wt_cols + dim // 2].T

    def send_gram(b):
        cols = [jnp.sum(sq_acc[b, m * dim:(m + 1) * dim], axis=1, keepdims=True) for m in range(2)]
        to_pairs(gram(b, zt, 0, zt, dim), gs_out.at[b], cols)
        if b == 0:
            pl.semaphore_wait(barrier, n - 1)
        for k in far_first:
            dst = (me + k) % n
            rcopy(gs_out.at[b, dst], gs_in.at[b, k - 1], gs_s.at[b, k - 1], gs_r.at[b, k - 1], dst).start()

    norm_rows(0, TOK)
    cp_x(0, 1).wait()
    cp_wqk.wait()
    for b in range(1, images):
        for t in range(tiles):
            cp_x(b, t).start()
    cp_wv.start()
    cp_wo.start()
    for b in range(images):
        cp_dy(b).start()
    transpose_w(0, 2 * dim)

    def qk_first(t, _):
        off = pl.multiple_of(t * TOK, TOK)
        qk_tile(off, off + TOK)
        return 0
    for b in range(1, images):
        for t in range(tiles):
            cp_x(b, t).wait()
    lax.fori_loop(0, tiles, qk_first, 0)
    send_gram(0)
    cp_wv.wait()
    for t in range(tiles):
        off = tokens + t * TOK
        qk_tile(off, off + TOK if t + 1 < tiles else None, 2 * dim + t * dim // tiles)
    send_gram(1)

    def values(b):
        def v_body(t, _):
            off = pl.multiple_of(b * tokens + t * TOK, TOK)
            zt[2 * dim:3 * dim, pl.ds(off, TOK)] = mm(wt_v[2 * dim:3 * dim, :], ut[:, pl.ds(off, TOK)]).astype(BF16)
            return 0
        lax.fori_loop(0, tiles, v_body, 0)

    eye = lax.broadcasted_iota(jnp.int32, (hd, hd), 0) == lax.broadcasted_iota(jnp.int32, (hd, hd), 1)

    def row_of(col):
        return jnp.sum(jnp.where(eye, col, 0.0), axis=0, keepdims=True)

    head_lane = lax.broadcasted_iota(jnp.int32, (1, heads), 1)
    tau_row = tau_ref[...].reshape(1, heads)

    def attn_state(b, s):
        blk = gs_sum[b]
        g = blk[:, s * hd:(s + 1) * hd]
        qc = blk[:, 2 * hd + s:2 * hd + s + 1]
        kr = row_of(blk[:, 2 * hd + 2 + s:2 * hd + 3 + s])
        unit = lax.rsqrt(qc) * lax.rsqrt(kr)
        tau = jnp.sum(jnp.where(head_lane == me * 2 + s, tau_row, 0.0), axis=1, keepdims=True)
        cosine = g * unit
        logits = tau * cosine
        e = jnp.exp(logits - jnp.max(logits, axis=-1, keepdims=True))
        probs = e / jnp.sum(e, axis=-1, keepdims=True)
        return cosine, logits, probs, tau * unit, qc, kr

    def pair(a0, a1):
        r = a0.shape[0]
        z = jnp.zeros((r, LANES - 2 * hd), a0.dtype)
        return jnp.concatenate([a0, a1, z], axis=1)

    def owner_forward(b):
        for k in range(1, n):
            rcopy(gs_out.at[b, 0], gs_in.at[b, k - 1], gs_s.at[b, k - 1], gs_r.at[b, k - 1], me).wait_recv()
        tot = gs_out[b, me]
        for k in range(1, n):
            tot = tot + gs_in[b, k - 1]
        gs_sum[b] = tot
        p0 = attn_state(b, 0)[2]
        p1 = attn_state(b, 1)[2]
        a_all[b, me] = pair(p0, p1).astype(BF16)
        for k in far_first:
            dst = (me + k) % n
            rcopy(a_all.at[b, me], a_all.at[b, me], a_s.at[b, k - 1], a_r.at[b, k - 1], dst).start()

    def owner_backward():
        for b in range(images):
            for k in range(1, n):
                rcopy(ds_out.at[b, 0], ds_in.at[b, k - 1], ds_s.at[b, k - 1], ds_r.at[b, k - 1], me).wait_recv()
        sub = lax.broadcasted_iota(jnp.int32, (8, LANES), 0)
        lane = lax.broadcasted_iota(jnp.int32, (8, LANES), 1)
        for b in range(images):
            tot = ds_out[b, me]
            for k in range(1, n):
                tot = tot + ds_in[b, k - 1]
            tot = tot.astype(BF16).astype(F32)
            gs, qs, ks, ts = [], [], [], []
            for s in range(2):
                cosine, logits, probs, scale, qc, kr = attn_state(b, s)
                dp = tot[:, s * hd:(s + 1) * hd]
                gl = probs * (dp - jnp.sum(probs * dp, axis=-1, keepdims=True))
                weighted = gl * logits
                gs.append(gl * scale)
                qs.append(row_of(-jnp.sum(weighted, axis=1, keepdims=True) / qc))
                ks.append(-jnp.sum(weighted, axis=0, keepdims=True) / kr)
                ts.append(jnp.sum(jnp.sum(gl * cosine, axis=1, keepdims=True), axis=0, keepdims=True))
            g_all[b, me] = pair(gs[0], gs[1]).astype(BF16)
            taus = jnp.where(lane == 0, ts[0], jnp.where(lane == 1, ts[1], 0.0))
            c_all[b, me] = jnp.where(sub == 0, pair(qs[0], qs[1]), jnp.where(sub == 1, pair(ks[0], ks[1]), jnp.where(sub == 2, taus, 0.0)))
        for b in range(images):
            for k in far_first:
                dst = (me + k) % n
                rcopy(g_all.at[b, me], g_all.at[b, me], g_s.at[b, k - 1], g_r.at[b, k - 1], dst).start()
                rcopy(c_all.at[b, me], c_all.at[b, me], c_s.at[b, k - 1], c_r.at[b, k - 1], dst).start()

    def gathered(ref, ss, rs, b):
        for k in range(1, n):
            src = (me + n - k) % n
            rcopy(ref.at[b, me], ref.at[b, src], ss.at[b, k - 1], rs.at[b, k - 1], me).wait_recv()

    def grad_heads(b):
        cp_dy(b).wait()
        if b == 0:
            cp_wo.wait()

        def body(t, _):
            off = pl.multiple_of(b * tokens + t * TOK, TOK)
            dot_v[:, pl.ds(off, TOK)] = mm(wo_v[...], dy_v[pl.ds(off, TOK), :], NT).astype(BF16)
            return 0
        lax.fori_loop(0, tiles, body, 0)

    def send_dprobs(b):
        to_pairs(gram(b, dot_v, 0, zt, 2 * dim), ds_out.at[b])
        for k in far_first:
            dst = (me + k) % n
            rcopy(ds_out.at[b, dst], ds_in.at[b, k - 1], ds_s.at[b, k - 1], ds_r.at[b, k - 1], dst).start()

    sj = lax.broadcasted_iota(jnp.int32, (LANES, COLS), 0)
    slane = lax.broadcasted_iota(jnp.int32, (LANES, COLS), 1)
    sels = []
    for s in range(2):
        hit = jnp.zeros((LANES, COLS), jnp.bool_)
        for k in range(wheads):
            hit = jnp.logical_or(hit, slane - k * hd == sj - s * hd)
        hit = jnp.logical_and(hit, jnp.logical_and(sj >= s * hd, sj < (s + 1) * hd))
        sels.append(jnp.where(hit, 1.0, 0.0).astype(BF16))
    blane = lax.broadcasted_iota(jnp.int32, (hd, COLS), 1)

    def build(ref, b):
        flat = ref[b].reshape(n * hd, LANES)
        for s in range(2):
            spread = mm(flat, sels[s])
            for d in range(n):
                w, k = divmod(2 * d + s, wheads)
                blk = jnp.where(jnp.logical_and(blane >= k * hd, blane < (k + 1) * hd), spread[d * hd:(d + 1) * hd], 0.0)
                bd[b, w, 0, k * hd:(k + 1) * hd, :] = blk.astype(BF16)
        for w in range(nwin):
            bd[b, w, 1] = bd[b, w, 0].T

    def windows():
        for w in range(nwin):
            r0 = w * wrow
            yield w, r0, min(wrow, dim - r0), min(COLS, dim - r0)

    def heads_out(b):
        def body(t, _):
            off = pl.multiple_of(b * tokens + t * TOK, TOK)
            for w, r0, m, kk in windows():
                ot[r0:r0 + m, pl.ds(off, TOK)] = mm(bd[b, w, 0, 0:m, 0:kk], zt[2 * dim + r0:2 * dim + r0 + kk, pl.ds(off, TOK)]).astype(BF16)
            return 0
        lax.fori_loop(0, tiles, body, 0)

    def grad_values(b):
        def body(t, _):
            off = pl.multiple_of(b * tokens + t * TOK, TOK)
            for w, r0, m, kk in windows():
                zt[2 * dim + r0:2 * dim + r0 + m, pl.ds(off, TOK)] = mm(bd[b, w, 1, 0:m, 0:kk], dot_v[r0:r0 + kk, pl.ds(off, TOK)]).astype(BF16)
            return 0
        lax.fori_loop(0, tiles, body, 0)

    def dq_and_dk(b):
        ct = c_all[b].reshape(n * 8, LANES).T
        for d in range(n):
            colq[d * per_dev:(d + 1) * per_dev, :] = jnp.broadcast_to(ct[0:per_dev, 8 * d:8 * d + 1], (per_dev, LANES))
            colk[d * per_dev:(d + 1) * per_dev, :] = jnp.broadcast_to(ct[0:per_dev, 8 * d + 1:8 * d + 2], (per_dev, LANES))

        def body(t, _):
            off = pl.multiple_of(b * tokens + t * TOK, TOK)
            for w, r0, m, kk in windows():
                qw = zt[r0:r0 + kk, pl.ds(off, TOK)]
                kw = zt[dim + r0:dim + r0 + kk, pl.ds(off, TOK)]
                cq = jnp.concatenate([colq[r0:r0 + m, :]] * (TOK // LANES), axis=1)
                ck = jnp.concatenate([colk[r0:r0 + m, :]] * (TOK // LANES), axis=1)
                dq = mm(bd[b, w, 0, 0:m, 0:kk], kw) + cq * qw[0:m].astype(F32)
                dk = mm(bd[b, w, 1, 0:m, 0:kk], qw) + ck * kw[0:m].astype(F32)
                zt[r0:r0 + m, pl.ds(off, TOK)] = dq.astype(BF16)
                zt[dim + r0:dim + r0 + m, pl.ds(off, TOK)] = dk.astype(BF16)
            return 0
        lax.fori_loop(0, tiles, body, 0)

    def put_part(c, val):
        for j in range(n):
            part[c, j % 2, j // 2] = val[j * per_dev:(j + 1) * per_dev, :]

    def d2d(c):
        return rcopy(part.at[c, 1 - core], r1.at[c], d2d_s.at[c], d2d_r.at[c], partner)

    half = per_dev // 2

    def hop1(c):
        return (rcopy(r1.at[c, co, pl.ds(0, half)], r2.at[c, 0], p1_s.at[c, 0], p1_r.at[c, 0], right),
                rcopy(r1.at[c, co, pl.ds(half, half)], r2.at[c, 1], p1_s.at[c, 1], p1_r.at[c, 1], left))

    def hop2(c):
        return (rcopy(r1.at[c, cr], r3.at[c, 0], p2_s.at[c, 0], p2_r.at[c, 0], right),
                rcopy(r1.at[c, cl], r3.at[c, 1], p2_s.at[c, 1], p2_r.at[c, 1], left))

    def serve1(c):
        d2d(c).wait_recv()
        for blk in (co, cr, cl, chip):
            r1[c, blk] += part[c, core, blk]
        for h in hop1(c):
            h.start()

    def serve2(c):
        for h in hop1(c):
            h.wait_recv()
        r1[c, cr, 0:half] += r2[c, 0]
        r1[c, cl, half:per_dev] += r2[c, 1]
        for h in hop2(c):
            h.start()

    def serve3(c):
        for h in hop2(c):
            h.wait_recv()
        return (r1[c, chip] + r3[c, 0] + r3[c, 1]).astype(BF16)

    def wo_chunk(c, _):
        off = pl.multiple_of(c * COLS, COLS)
        put_part(c, mm(ot[...], dy_v[:, pl.ds(off, COLS)]))
        d2d(c).start()
        return 0

    def qkv_chunk(c, base):
        off = pl.multiple_of(base + c * COLS, COLS)
        put_part(c, mm(ut[...], zt[pl.ds(off, COLS), :], NT))
        d2d(c).start()

    values(0)
    grad_heads(0)
    send_dprobs(0)
    owner_forward(0)
    values(1)
    owner_forward(1)
    grad_heads(1)
    send_dprobs(1)
    gathered(a_all, a_s, a_r, 0)
    build(a_all, 0)
    heads_out(0)
    gathered(a_all, a_s, a_r, 1)
    build(a_all, 1)
    heads_out(1)
    wo_chunk(0, 0)

    def wo_loop(c, _):
        wo_chunk(c, 0)
        serve1(c - 1)
        return 0
    lax.fori_loop(1, o_chunks, wo_loop, 0)
    owner_backward()
    serve1(o_chunks - 1)
    grad_values(0)
    grad_values(1)
    v0 = 2 * dim - o_chunks * COLS
    qkv_chunk(o_chunks, v0)

    def s2_body(c, _):
        serve2(c)
        return 0

    def serve2_range(c0, c1):
        lax.fori_loop(c0, c1, s2_body, 0)

    serve2_range(0, 2)

    def v_loop(c, _):
        qkv_chunk(c, v0)
        serve1(c - 1)
        return 0
    lax.fori_loop(o_chunks + 1, 2 * o_chunks, v_loop, 0)
    serve2_range(2, 3)
    for b in range(images):
        gathered(g_all, g_s, g_r, b)
        gathered(c_all, c_s, c_r, b)
        build(g_all, b)
        dq_and_dk(b)
        if b == 0:
            serve1(2 * o_chunks - 1)
    serve2_range(3, 4)
    qkv_chunk(2 * o_chunks, -2 * o_chunks * COLS)

    def qk_loop(c, _):
        qkv_chunk(c, -2 * o_chunks * COLS)
        serve1(c - 1)
        return 0
    lax.fori_loop(2 * o_chunks + 1, chunks, qk_loop, 0)
    serve1(chunks - 1)
    serve2_range(4, chunks - 3)

    def tile_copy(i, t):
        b = t // tiles
        rows = pl.ds(pl.multiple_of(t * TOK, TOK), TOK)
        out_rows = pl.ds(pl.multiple_of((t % tiles) * TOK, TOK), TOK)
        src, dst = ((x_v, y_hbm), (dy_v, dx_hbm))[i]
        return pltpu.make_async_copy(src.at[rows], dst.at[b, out_rows], out_sem.at[i, t])

    def dx_body(t, _):
        off = pl.multiple_of(t * TOK, TOK)
        dot_v[:, pl.ds(off, TOK)] = mm(w_v[...], zt[:, pl.ds(off, TOK)]).astype(BF16)

        def piece(i, _):
            r = pl.ds(pl.multiple_of(off + i * LANES, LANES), LANES)
            du = dot_v[:, r].T.astype(F32)
            x_hat, inv = norm(x_v[r, :].astype(F32))
            prod = du * x_hat
            dgb[0] += jnp.sum(prod.reshape(LANES // 8, 8, dim), axis=0)
            dgb[1] += jnp.sum(du.reshape(LANES // 8, 8, dim), axis=0)
            a9 = du * gain_row
            m1 = jnp.sum(a9, axis=-1, keepdims=True) * (1.0 / dim)
            m2 = jnp.sum(a9 * x_hat, axis=-1, keepdims=True) * (1.0 / dim)
            gx = inv * (a9 - m1 - x_hat * m2)
            dy_v[r, :] = (dy_v[r, :].astype(F32) + gx).astype(BF16)
            return 0
        lax.fori_loop(0, TOK // LANES, piece, 0)
        tile_copy(1, t).start()
        return 0

    def y_body(t, _):
        off = pl.multiple_of(t * TOK, TOK)
        x_v[pl.ds(off, TOK), :] = (x_v[pl.ds(off, TOK), :].astype(F32) + mm(ot[:, pl.ds(off, TOK)].T, wo_v[...])).astype(BF16)
        tile_copy(0, t).start()
        return 0
    lax.fori_loop(0, 1, dx_body, 0)
    serve2_range(chunks - 3, chunks)
    lax.fori_loop(1, images * tiles, dx_body, 0)
    lax.fori_loop(0, images * tiles, y_body, 0)

    sub8 = lax.broadcasted_iota(jnp.int32, (8, dim), 0)
    gb = jnp.where(sub8 == 0, jnp.sum(dgb[0], axis=0, keepdims=True), jnp.where(sub8 == 1, jnp.sum(dgb[1], axis=0, keepdims=True), 0.0))
    gb_all[me] = gb
    for k in range(1, n):
        dst = (me + k) % n
        rcopy(gb_all.at[me], gb_all.at[me], gb_s.at[k - 1], gb_r.at[k - 1], dst).start()

    lane = lax.broadcasted_iota(jnp.int32, (1, LANES), 1)
    dtau = jnp.zeros((1, LANES), F32)
    for d in range(n):
        row = c_all[0, d, 2:3, :]
        for b in range(1, images):
            row = row + c_all[b, d, 2:3, :]
        if d:
            row = pltpu.roll(row, 2 * d, 1)
        dtau = jnp.where(jnp.logical_and(lane >= 2 * d, lane < 2 * d + 2), row, dtau)
    dtau_ref[...] = dtau

    def s3_wo(c, _):
        dwo_ref[:, pl.ds(pl.multiple_of(c * COLS, COLS), COLS)] = serve3(c)
        return 0
    lax.fori_loop(0, o_chunks, s3_wo, 0)

    def s3_v(c, _):
        dwqkv_ref[:, pl.ds(pl.multiple_of(2 * dim - dim + c * COLS, COLS), COLS)] = serve3(c)
        return 0
    lax.fori_loop(o_chunks, 2 * o_chunks, s3_v, 0)

    for k in range(1, n):
        src = (me + n - k) % n
        rcopy(gb_all.at[me], gb_all.at[src], gb_s.at[k - 1], gb_r.at[k - 1], me).wait_recv()
    tot = gb_all[0]
    for d in range(1, n):
        tot = tot + gb_all[d]
    dgain_ref[...] = tot[0:1, :]
    dbias_ref[...] = tot[1:2, :]

    def s3_qk(c, _):
        dwqkv_ref[:, pl.ds(pl.multiple_of(c * COLS - 2 * dim, COLS), COLS)] = serve3(c)
        return 0
    lax.fori_loop(2 * o_chunks, chunks, s3_qk, 0)

    for b in range(images):
        for k in range(1, n):
            rcopy(gs_out.at[b, 0], gs_in.at[b, k - 1], gs_s.at[b, k - 1], gs_r.at[b, k - 1], me).wait_send()
            rcopy(a_all.at[b, me], a_all.at[b, me], a_s.at[b, k - 1], a_r.at[b, k - 1], me).wait_send()
            rcopy(ds_out.at[b, 0], ds_in.at[b, k - 1], ds_s.at[b, k - 1], ds_r.at[b, k - 1], me).wait_send()
            rcopy(g_all.at[b, me], g_all.at[b, me], g_s.at[b, k - 1], g_r.at[b, k - 1], me).wait_send()
            rcopy(c_all.at[b, me], c_all.at[b, me], c_s.at[b, k - 1], c_r.at[b, k - 1], me).wait_send()
    for k in range(1, n):
        rcopy(gb_all.at[me], gb_all.at[me], gb_s.at[k - 1], gb_r.at[k - 1], me).wait_send()

    def drain(c, _):
        d2d(c).wait_send()
        for h in hop1(c) + hop2(c):
            h.wait_send()
        return 0
    lax.fori_loop(0, chunks, drain, 0)

    def drain_out(t, _):
        tile_copy(0, t).wait()
        tile_copy(1, t).wait()
        return 0
    lax.fori_loop(0, images * tiles, drain_out, 0)


def finish_kernel(heads, y_hbm, dx_hbm, dwqkv_hbm, dwo_hbm, dgain_ref, dbias_ref, dtau_ref,
                  y_out, dx_out, dwqkv_out, dwo_out, dgain_out, dbias_out, dtau_out,
                  buf, q_buf, o_buf, sem_in, sem_out):
    images, tokens, dim = y_hbm.shape
    parts = tokens // TOK
    moves = []
    for a, (src, dst) in enumerate(((y_hbm, y_out), (dx_hbm, dx_out))):
        for b in range(images):
            for t in range(parts):
                i = len(moves)
                rows = pl.ds(t * TOK, TOK)
                moves.append((src.at[b, rows], buf.at[i], dst.at[b, rows]))
    moves.append((dwqkv_hbm, q_buf, dwqkv_out))
    moves.append((dwo_hbm, o_buf, dwo_out))
    ins = [pltpu.make_async_copy(s, v, sem_in.at[i]) for i, (s, v, _d) in enumerate(moves)]
    outs = [pltpu.make_async_copy(v, d, sem_out.at[i]) for i, (_s, v, d) in enumerate(moves)]
    for c in ins:
        c.start()
    dgain_out[...] = dgain_ref[...].reshape(dgain_out.shape)
    dbias_out[...] = dbias_ref[...].reshape(dbias_out.shape)
    dtau_out[...] = dtau_ref[...].reshape(dtau_ref.shape[1])[:heads]
    for c, o in zip(ins, outs):
        c.wait()
        o.start()
    for o in outs:
        o.wait()


def solution(mesh):
    n = mesh.shape["sp"]

    def local_step(x_in, grad_y, ln_gain, ln_bias, w_qkv, w_out, temp_tau):
        images, tokens, dim = x_in.shape
        heads = temp_tau.shape[0]
        hd = dim // heads
        rows = images * tokens
        per_dev = dim // n
        chunks = 4 * dim // COLS
        nwin = -(-heads // (COLS // hd))
        any_spec = pl.BlockSpec(memory_space=pl.ANY)
        vmem = pl.BlockSpec(memory_space=pltpu.VMEM)
        dma = pltpu.SemaphoreType.DMA
        pairs = (images, n - 1)
        out = pl.pallas_call(
            functools.partial(xca_kernel, n, heads),
            out_shape=(
                jax.ShapeDtypeStruct(x_in.shape, BF16),
                jax.ShapeDtypeStruct(x_in.shape, BF16),
                jax.ShapeDtypeStruct((per_dev, 3 * dim), BF16),
                jax.ShapeDtypeStruct((per_dev, dim), BF16),
                jax.ShapeDtypeStruct((1, dim), F32),
                jax.ShapeDtypeStruct((1, dim), F32),
                jax.ShapeDtypeStruct((1, LANES), F32),
            ),
            in_specs=[any_spec] * 7,
            out_specs=(any_spec, any_spec, vmem, vmem, vmem, vmem, vmem),
            scratch_shapes=[
                pltpu.VMEM((dim,), F32),
                pltpu.VMEM((dim,), F32),
                pltpu.VMEM((heads,), F32),
                pltpu.VMEM((rows, dim), BF16),
                pltpu.VMEM((rows, dim), BF16),
                pltpu.VMEM((dim, 3 * dim), BF16),
                pltpu.VMEM((3 * dim, dim), BF16),
                pltpu.VMEM((dim, dim), BF16),
                pltpu.VMEM((dim, rows), BF16),
                pltpu.VMEM((3 * dim, rows), BF16),
                pltpu.VMEM((dim, rows), BF16),
                pltpu.VMEM((dim, rows), BF16),
                pltpu.VMEM((images, 2 * dim, LANES), F32),
                pltpu.VMEM((images, n, hd, LANES), F32),
                pltpu.VMEM((images, n - 1, hd, LANES), F32),
                pltpu.VMEM((images, hd, LANES), F32),
                pltpu.VMEM((images, n, hd, LANES), BF16),
                pltpu.VMEM((images, n, hd, LANES), F32),
                pltpu.VMEM((images, n - 1, hd, LANES), F32),
                pltpu.VMEM((images, n, hd, LANES), BF16),
                pltpu.VMEM((images, n, 8, LANES), F32),
                pltpu.VMEM((images, nwin, 2, COLS, COLS), BF16),
                pltpu.VMEM((dim, LANES), F32),
                pltpu.VMEM((dim, LANES), F32),
                pltpu.VMEM((2, 8, dim), F32),
                pltpu.VMEM((n, 8, dim), F32),
                pltpu.VMEM((chunks, 2, n // 2, per_dev, COLS), F32),
                pltpu.VMEM((chunks, n // 2, per_dev, COLS), F32),
                pltpu.VMEM((chunks, 2, per_dev // 2, COLS), F32),
                pltpu.VMEM((chunks, 2, per_dev, COLS), F32),
                dma((rows // TOK + images + 6,)), dma((2, rows // TOK)),
                dma((chunks,)), dma((chunks,)),
                dma((chunks, 2)), dma((chunks, 2)), dma((chunks, 2)), dma((chunks, 2)),
                dma(pairs), dma(pairs), dma(pairs), dma(pairs), dma(pairs), dma(pairs),
                dma(pairs), dma(pairs), dma(pairs), dma(pairs),
                dma((n - 1,)), dma((n - 1,)),
            ],
            compiler_params=pltpu.CompilerParams(
                collective_id=0, has_side_effects=True, vmem_limit_bytes=67043328),
            name="xca_block",
        )(x_in, grad_y, ln_gain, ln_bias, w_qkv, w_out, temp_tau)
        moves = 2 * rows // TOK + 2
        return pl.pallas_call(
            functools.partial(finish_kernel, heads),
            out_shape=(
                jax.ShapeDtypeStruct(x_in.shape, BF16),
                jax.ShapeDtypeStruct(x_in.shape, BF16),
                jax.ShapeDtypeStruct((per_dev, 3 * dim), BF16),
                jax.ShapeDtypeStruct((per_dev, dim), BF16),
                jax.ShapeDtypeStruct((dim,), F32),
                jax.ShapeDtypeStruct((dim,), F32),
                jax.ShapeDtypeStruct((heads,), F32),
            ),
            in_specs=[any_spec] * 4 + [vmem] * 3,
            out_specs=(any_spec,) * 4 + (vmem,) * 3,
            scratch_shapes=[
                pltpu.VMEM((2 * rows // TOK, TOK, dim), BF16),
                pltpu.VMEM((per_dev, 3 * dim), BF16),
                pltpu.VMEM((per_dev, dim), BF16),
                dma((moves,)), dma((moves,)),
            ],
            name="finish",
        )(*out)

    tok = P("dp", "sp", None)
    return jax.shard_map(
        local_step, mesh=mesh,
        in_specs=(tok, tok, P(), P(), P(), P(), P()),
        out_specs=(tok, tok, P(("dp", "sp"), None), P(("dp", "sp"), None), P("dp"), P("dp"), P("dp")),
        check_vma=False)
```

```python
import functools

import jax
import jax.numpy as jnp
from jax import lax
from jax.experimental import pallas as pl
from jax.experimental.pallas import tpu as pltpu
from jax.sharding import PartitionSpec as P

LN_EPS = 1e-6
F32 = jnp.float32
BF16 = jnp.bfloat16
LANES = 128
TOK = 512
COLS = 256
VMEM_LIMIT = 67043328
NN = (((1,), (0,)), ((), ()))
NT = (((1,), (1,)), ((), ()))


def mm(a, b, dims=NN):
    return lax.dot_general(a, b, dims, preferred_element_type=F32)


def xca_kernel(
    n, heads,
    x_hbm, dy_hbm, gain_hbm, bias_hbm, wqkv_hbm, wo_hbm, tau_hbm,
    y_hbm, dx_hbm, dwqkv_ref, dwo_ref, dgain_ref, dbias_ref, dtau_ref,
    gain_ref, bias_ref, tau_ref, x_v, dy_v, w_v, wt_v, wo_v, ut, zt, dot_v, ot,
    sq_acc, gs_out, gs_in, gs_sum, a_all, ds_out, ds_in, g_all, c_all, bd, colq, colk, dgb, gb_all,
    part, r1, r2, r3,
    in_sem, out_sem, d2d_s, d2d_r, p1_s, p1_r, p2_s, p2_r,
    gs_s, gs_r, a_s, a_r, ds_s, ds_r, g_s, g_r, c_s, c_r, gb_s, gb_r,
):
    images, tokens, dim = x_hbm.shape
    hd = dim // heads
    rows = images * tokens
    per_dev = dim // n
    chips = n // 2
    wheads = COLS // hd
    wrow = wheads * hd
    nwin = -(-heads // wheads)
    tiles = tokens // TOK
    o_chunks = dim // COLS
    chunks = 4 * o_chunks
    me = lax.axis_index("sp")
    chip, core = me // 2, me % 2
    right = ((chip + 1) % chips) * 2 + core
    left = ((chip + chips - 1) % chips) * 2 + core
    partner = chip * 2 + (1 - core)
    cr, cl, co = (chip + 1) % chips, (chip + chips - 1) % chips, (chip + 2) % chips

    peers = range(1, n)
    far_first = sorted(peers, key=lambda k: abs(2 * k - n))

    def rcopy(src, dst, ss, rs, dev):
        return pltpu.make_async_remote_copy(
            src_ref=src, dst_ref=dst, send_sem=ss, recv_sem=rs,
            device_id={"sp": dev}, device_id_type=pl.DeviceIdType.MESH)

    def cp_x(b, t):
        return pltpu.make_async_copy(x_hbm.at[b, pl.ds(t * TOK, TOK)], x_v.at[pl.ds(b * tokens + t * TOK, TOK)], in_sem.at[b * tiles + t])

    def cp_dy(b):
        return pltpu.make_async_copy(dy_hbm.at[b], dy_v.at[pl.ds(b * tokens, tokens)], in_sem.at[images * tiles + b])

    base = images * tiles + images
    cp_small = [pltpu.make_async_copy(h, v, in_sem.at[base + i]) for i, (h, v) in enumerate(
        ((gain_hbm, gain_ref), (bias_hbm, bias_ref), (tau_hbm, tau_ref)))]
    base += 3
    cp_wqk = pltpu.make_async_copy(wqkv_hbm.at[:, pl.ds(0, 2 * dim)], w_v.at[:, pl.ds(0, 2 * dim)], in_sem.at[base])
    cp_wv = pltpu.make_async_copy(wqkv_hbm.at[:, pl.ds(2 * dim, dim)], w_v.at[:, pl.ds(2 * dim, dim)], in_sem.at[base + 1])
    cp_wo = pltpu.make_async_copy(wo_hbm, wo_v, in_sem.at[base + 2])
    for c in cp_small:
        c.start()
    cp_x(0, 0).start()
    cp_wqk.start()
    cp_x(0, 1).start()

    barrier = pltpu.get_barrier_semaphore()
    for k in peers:
        pl.semaphore_signal(barrier, inc=1, device_id={"sp": (me + k) % n},
                            device_id_type=pl.DeviceIdType.MESH)
    sq_acc[...] = jnp.zeros_like(sq_acc)
    bd[...] = jnp.zeros_like(bd)
    dgb[...] = jnp.zeros_like(dgb)
    for c in cp_small:
        c.wait()
    cp_x(0, 0).wait()

    def norm(xt):
        mean = jnp.sum(xt, axis=-1, keepdims=True) * (1.0 / dim)
        cen = xt - mean
        inv = lax.rsqrt(jnp.sum(cen * cen, axis=-1, keepdims=True) * (1.0 / dim) + LN_EPS)
        return cen * inv, inv

    gain_row = gain_ref[...].reshape(1, dim)
    bias_row = bias_ref[...].reshape(1, dim)

    def norm_rows(r0, count):
        x_hat, _inv = norm(x_v[pl.ds(r0, count), :].astype(F32))
        ut[:, pl.ds(r0, count)] = (x_hat * gain_row + bias_row).astype(BF16).T

    def transpose_w(c0, count):
        def body(i, _):
            off = pl.multiple_of(c0 + i * COLS, COLS)
            wt_v[pl.ds(off, COLS), :] = w_v[:, pl.ds(off, COLS)].T
            return 0
        lax.fori_loop(0, count // COLS, body, 0)

    lane_w = lax.broadcasted_iota(jnp.int32, (hd, LANES), 1)

    def to_pairs(blocks, out_ref, extra=None):
        for d in range(n):
            picked = []
            for s in range(2):
                w, k = divmod(2 * d + s, wheads)
                strip = blocks[w][k * hd:(k + 1) * hd, :]
                shift = (s * hd - k * hd) % COLS
                if shift:
                    strip = pltpu.roll(strip, shift, 1)
                picked.append(strip[:, :LANES])
            rest = 0.0
            if extra is not None:
                for i, col in enumerate(extra):
                    for s in range(2):
                        r0 = (2 * d + s) * hd
                        rest = jnp.where(lane_w == 2 * hd + 2 * i + s, col[r0:r0 + hd], rest)
            out_ref[d] = jnp.where(lane_w < hd, picked[0], jnp.where(lane_w < 2 * hd, picked[1], rest))

    def gram(b, l_ref, l0, r_ref, r0):
        blocks = []
        for w in range(nwin):
            m = min(wrow, dim - w * wrow)
            lo, ro = l0 + w * wrow, r0 + w * wrow
            nw = min(COLS, dim - w * wrow)
            left_op = l_ref[lo:lo + m, b * tokens:(b + 1) * tokens]
            right_op = r_ref[ro:ro + nw, b * tokens:(b + 1) * tokens]
            g = mm(left_op, right_op, NT)
            if nw < COLS:
                g = jnp.pad(g, ((0, 0), (0, COLS - nw)))
            blocks.append(g)
        return blocks

    def qk_tile(off, following, wt_cols=None):
        for m in range(2):
            z = mm(wt_v[m * dim:(m + 1) * dim, :], ut[:, pl.ds(off, TOK)]).astype(BF16)
            zt[m * dim:(m + 1) * dim, pl.ds(off, TOK)] = z
            zf = z.astype(F32)
            sq = zf * zf
            tot = sq[:, 0:LANES]
            for j in range(1, TOK // LANES):
                tot = tot + sq[:, j * LANES:(j + 1) * LANES]
            sq_acc[off // tokens, m * dim:(m + 1) * dim] += tot
        if following is not None:
            norm_rows(following, TOK)
        if wt_cols is not None:
            wt_v[wt_cols:wt_cols + dim // 2, :] = w_v[:, wt_cols:wt_cols + dim // 2].T

    def send_gram(b):
        cols = [jnp.sum(sq_acc[b, m * dim:(m + 1) * dim], axis=1, keepdims=True) for m in range(2)]
        to_pairs(gram(b, zt, 0, zt, dim), gs_out.at[b], cols)
        if b == 0:
            pl.semaphore_wait(barrier, n - 1)
        for k in far_first:
            dst = (me + k) % n
            rcopy(gs_out.at[b, dst], gs_in.at[b, k], gs_s.at[b, k], gs_r.at[b, k], dst).start()

    for b in range(1, images):
        for t in range(tiles):
            cp_x(b, t).start()
    norm_rows(0, TOK)
    cp_x(0, 1).wait()
    cp_wqk.wait()
    cp_wv.start()
    cp_wo.start()
    for b in range(images):
        cp_dy(b).start()
    transpose_w(0, 2 * dim)

    def qk_first(t, _):
        off = pl.multiple_of(t * TOK, TOK)
        qk_tile(off, off + TOK)
        return 0
    for b in range(1, images):
        for t in range(tiles):
            cp_x(b, t).wait()
    lax.fori_loop(0, tiles, qk_first, 0)
    send_gram(0)
    cp_wv.wait()
    for t in range(tiles):
        off = tokens + t * TOK
        qk_tile(off, off + TOK if t + 1 < tiles else None, 2 * dim + t * dim // tiles)
    send_gram(1)

    def values(b):
        for t in range(tiles):
            tok_t = pl.ds(b * tokens + t * TOK, TOK)
            zt[2 * dim:3 * dim, tok_t] = mm(wt_v[2 * dim:3 * dim, :], ut[:, tok_t]).astype(BF16)

    eye = lax.broadcasted_iota(jnp.int32, (hd, hd), 0) == lax.broadcasted_iota(jnp.int32, (hd, hd), 1)

    def row_of(col):
        return jnp.sum(jnp.where(eye, col, 0.0), axis=0, keepdims=True)

    head_lane = lax.broadcasted_iota(jnp.int32, (1, heads), 1)
    tau_row = tau_ref[...].reshape(1, heads)

    def attn_state(b, s):
        blk = gs_sum[b]
        g = blk[:, s * hd:(s + 1) * hd]
        qc = blk[:, 2 * hd + s:2 * hd + s + 1]
        kr = row_of(blk[:, 2 * hd + 2 + s:2 * hd + 3 + s])
        unit = lax.rsqrt(qc) * lax.rsqrt(kr)
        tau = jnp.sum(jnp.where(head_lane == me * 2 + s, tau_row, 0.0), axis=1, keepdims=True)
        cosine = g * unit
        logits = tau * cosine
        e = jnp.exp(logits - jnp.max(logits, axis=-1, keepdims=True))
        probs = e / jnp.sum(e, axis=-1, keepdims=True)
        return cosine, logits, probs, tau * unit, qc, kr

    def pair(a0, a1):
        r = a0.shape[0]
        z = jnp.zeros((r, LANES - 2 * hd), a0.dtype)
        return jnp.concatenate([a0, a1, z], axis=1)

    def owner_forward(b):
        for k in peers:
            rcopy(gs_out.at[b, 0], gs_in.at[b, k], gs_s.at[b, k], gs_r.at[b, k], me).wait_recv()
        tot = gs_out[b, me]
        for k in peers:
            tot = tot + gs_in[b, k]
        gs_sum[b] = tot
        p0 = attn_state(b, 0)[2]
        p1 = attn_state(b, 1)[2]
        a_all[b, me] = pair(p0, p1).astype(BF16)
        for k in far_first:
            dst = (me + k) % n
            rcopy(a_all.at[b, me], a_all.at[b, me], a_s.at[b, k], a_r.at[b, k], dst).start()

    def owner_backward():
        for b in range(images):
            for k in peers:
                rcopy(ds_out.at[b, 0], ds_in.at[b, k], ds_s.at[b, k], ds_r.at[b, k], me).wait_recv()
        sub = lax.broadcasted_iota(jnp.int32, (8, LANES), 0)
        lane = lax.broadcasted_iota(jnp.int32, (8, LANES), 1)
        for b in range(images):
            tot = ds_out[b, me]
            for k in peers:
                tot = tot + ds_in[b, k]
            tot = tot.astype(BF16).astype(F32)
            gs, qs, ks, ts = [], [], [], []
            for s in range(2):
                cosine, logits, probs, scale, qc, kr = attn_state(b, s)
                dp = tot[:, s * hd:(s + 1) * hd]
                gl = probs * (dp - jnp.sum(probs * dp, axis=-1, keepdims=True))
                weighted = gl * logits
                gs.append(gl * scale)
                qs.append(row_of(-jnp.sum(weighted, axis=1, keepdims=True) / qc))
                ks.append(-jnp.sum(weighted, axis=0, keepdims=True) / kr)
                ts.append(jnp.sum(jnp.sum(gl * cosine, axis=1, keepdims=True), axis=0, keepdims=True))
            g_all[b, me] = pair(gs[0], gs[1]).astype(BF16)
            taus = jnp.where(lane == 0, ts[0], jnp.where(lane == 1, ts[1], 0.0))
            c_all[b, me] = jnp.where(sub == 0, pair(qs[0], qs[1]), jnp.where(sub == 1, pair(ks[0], ks[1]), jnp.where(sub == 2, taus, 0.0)))
        for b in range(images):
            for k in far_first:
                dst = (me + k) % n
                rcopy(g_all.at[b, me], g_all.at[b, me], g_s.at[b, k], g_r.at[b, k], dst).start()
                rcopy(c_all.at[b, me], c_all.at[b, me], c_s.at[b, k], c_r.at[b, k], dst).start()

    def gathered(ref, ss, rs, b):
        for k in peers:
            src = (me + n - k) % n
            rcopy(ref.at[b, me], ref.at[b, src], ss.at[b, k], rs.at[b, k], me).wait_recv()

    def grad_heads(b):
        cp_dy(b).wait()
        if b == 0:
            cp_wo.wait()

        for t in range(tiles):
            tok_t = pl.ds(b * tokens + t * TOK, TOK)
            dot_v[:, tok_t] = mm(wo_v[...], dy_v[tok_t, :], NT).astype(BF16)

    def send_dprobs(b):
        to_pairs(gram(b, dot_v, 0, zt, 2 * dim), ds_out.at[b])
        for k in far_first:
            dst = (me + k) % n
            rcopy(ds_out.at[b, dst], ds_in.at[b, k], ds_s.at[b, k], ds_r.at[b, k], dst).start()

    sj = lax.broadcasted_iota(jnp.int32, (LANES, COLS), 0)
    slane = lax.broadcasted_iota(jnp.int32, (LANES, COLS), 1)
    sels = []
    for s in range(2):
        hit = jnp.zeros((LANES, COLS), jnp.bool_)
        for k in range(wheads):
            hit = jnp.logical_or(hit, slane - k * hd == sj - s * hd)
        hit = jnp.logical_and(hit, jnp.logical_and(sj >= s * hd, sj < (s + 1) * hd))
        sels.append(jnp.where(hit, 1.0, 0.0).astype(BF16))
    blane = lax.broadcasted_iota(jnp.int32, (hd, COLS), 1)

    def build(ref, b):
        flat = ref[b].reshape(n * hd, LANES)
        for s in range(2):
            spread = mm(flat, sels[s])
            for d in range(n):
                w, k = divmod(2 * d + s, wheads)
                blk = jnp.where(jnp.logical_and(blane >= k * hd, blane < (k + 1) * hd), spread[d * hd:(d + 1) * hd], 0.0)
                bd[b, w, 0, k * hd:(k + 1) * hd, :] = blk.astype(BF16)
        for w in range(nwin):
            bd[b, w, 1] = bd[b, w, 0].T

    def windows():
        for w in range(nwin):
            r0 = w * wrow
            yield w, r0, min(wrow, dim - r0), min(COLS, dim - r0)

    def heads_out(b):
        for t in range(tiles):
            tok_t = pl.ds(b * tokens + t * TOK, TOK)
            for w, r0, m, kk in windows():
                ot[r0:r0 + m, tok_t] = mm(bd[b, w, 0, 0:m, 0:kk], zt[2 * dim + r0:2 * dim + r0 + kk, tok_t]).astype(BF16)

    def grad_values(b):
        def body(t, _):
            off = pl.multiple_of(b * tokens + t * TOK, TOK)
            for w, r0, m, kk in windows():
                zt[2 * dim + r0:2 * dim + r0 + m, pl.ds(off, TOK)] = mm(bd[b, w, 1, 0:m, 0:kk], dot_v[r0:r0 + kk, pl.ds(off, TOK)]).astype(BF16)
            return 0
        lax.fori_loop(0, tiles, body, 0)

    def dq_and_dk(b):
        ct = c_all[b].reshape(n * 8, LANES).T
        for d in range(n):
            colq[d * per_dev:(d + 1) * per_dev, :] = jnp.broadcast_to(ct[0:per_dev, 8 * d:8 * d + 1], (per_dev, LANES))
            colk[d * per_dev:(d + 1) * per_dev, :] = jnp.broadcast_to(ct[0:per_dev, 8 * d + 1:8 * d + 2], (per_dev, LANES))

        def body(t, _):
            off = pl.multiple_of(b * tokens + t * TOK, TOK)
            for w, r0, m, kk in windows():
                qw = zt[r0:r0 + kk, pl.ds(off, TOK)]
                kw = zt[dim + r0:dim + r0 + kk, pl.ds(off, TOK)]
                cq = jnp.concatenate([colq[r0:r0 + m, :]] * (TOK // LANES), axis=1)
                ck = jnp.concatenate([colk[r0:r0 + m, :]] * (TOK // LANES), axis=1)
                dq = mm(bd[b, w, 0, 0:m, 0:kk], kw) + cq * qw[0:m].astype(F32)
                dk = mm(bd[b, w, 1, 0:m, 0:kk], qw) + ck * kw[0:m].astype(F32)
                zt[r0:r0 + m, pl.ds(off, TOK)] = dq.astype(BF16)
                zt[dim + r0:dim + r0 + m, pl.ds(off, TOK)] = dk.astype(BF16)
            return 0
        lax.fori_loop(0, tiles, body, 0)

    def put_part(c, val, more=False):
        for j in range(n):
            rows_j = val[j * per_dev:(j + 1) * per_dev, :]
            if more:
                rows_j += part[c, j % 2, j // 2]
            part[c, j % 2, j // 2] = rows_j

    def d2d(c):
        return rcopy(part.at[c, 1 - core], r1.at[c], d2d_s.at[c], d2d_r.at[c], partner)

    half = per_dev // 2

    def hop1(c):
        return (rcopy(r1.at[c, co, pl.ds(0, half)], r2.at[c, 0], p1_s.at[c, 0], p1_r.at[c, 0], right),
                rcopy(r1.at[c, co, pl.ds(half, half)], r2.at[c, 1], p1_s.at[c, 1], p1_r.at[c, 1], left))

    def hop2(c):
        return (rcopy(r1.at[c, cr], r3.at[c, 0], p2_s.at[c, 0], p2_r.at[c, 0], right),
                rcopy(r1.at[c, cl], r3.at[c, 1], p2_s.at[c, 1], p2_r.at[c, 1], left))

    def serve1(c):
        d2d(c).wait_recv()
        for blk in (co, cr, cl, chip):
            r1[c, blk] += part[c, core, blk]
        for h in hop1(c):
            h.start()

    def serve2(c):
        for h in hop1(c):
            h.wait_recv()
        r1[c, cr, 0:half] += r2[c, 0]
        r1[c, cl, half:per_dev] += r2[c, 1]
        for h in hop2(c):
            h.start()

    def serve3(c):
        for h in hop2(c):
            h.wait_recv()
        return (r1[c, chip] + r3[c, 0] + r3[c, 1]).astype(BF16)

    def wo_chunk(c, b):
        off = pl.multiple_of(c * COLS, COLS)
        tok_b = slice(b * tokens, (b + 1) * tokens)
        put_part(c, mm(ot[:, tok_b], dy_v[tok_b, pl.ds(off, COLS)]), b > 0)
        if b + 1 == images:
            d2d(c).start()

    def qkv_chunk(c, base):
        off = pl.multiple_of(base + c * COLS, COLS)
        put_part(c, mm(ut[...], zt[pl.ds(off, COLS), :], NT))
        d2d(c).start()

    values(0)
    grad_heads(0)
    owner_forward(0)
    send_dprobs(0)
    values(1)
    owner_forward(1)
    grad_heads(1)
    send_dprobs(1)
    for b in range(images):
        gathered(a_all, a_s, a_r, b)
        build(a_all, b)
        heads_out(b)

        for c in range(o_chunks):
            wo_chunk(c, b)
            if b + 1 == images and c > 0:
                serve1(c - 1)
    owner_backward()
    serve1(o_chunks - 1)
    grad_values(0)
    grad_values(1)
    v0 = 2 * dim - o_chunks * COLS
    qkv_chunk(o_chunks, v0)

    def s2_body(c, _):
        serve2(c)
        return 0

    def serve2_range(c0, c1):
        lax.fori_loop(c0, c1, s2_body, 0)

    serve2_range(0, 2)

    def v_loop(c, _):
        qkv_chunk(c, v0)
        serve1(c - 1)
        return 0
    lax.fori_loop(o_chunks + 1, 2 * o_chunks, v_loop, 0)
    serve2_range(2, 3)
    for b in range(images):
        gathered(g_all, g_s, g_r, b)
        gathered(c_all, c_s, c_r, b)
        build(g_all, b)
        dq_and_dk(b)
        if b == 0:
            serve1(2 * o_chunks - 1)
    serve2_range(3, 4)
    qkv_chunk(2 * o_chunks, -2 * o_chunks * COLS)

    def qk_loop(c, _):
        qkv_chunk(c, -2 * o_chunks * COLS)
        serve1(c - 1)
        return 0
    lax.fori_loop(2 * o_chunks + 1, chunks, qk_loop, 0)
    serve1(chunks - 1)
    serve2_range(4, chunks - 3)

    def tile_copy(i, t):
        rows_t = pl.ds(pl.multiple_of(t * TOK, TOK), TOK)
        src, dst = ((x_v, y_hbm), (dy_v, dx_hbm))[i]
        return pltpu.make_async_copy(src.at[rows_t], dst.at[rows_t], out_sem.at[i, t])

    def dx_body(t, _):
        off = pl.multiple_of(t * TOK, TOK)
        dot_v[:, pl.ds(off, TOK)] = mm(w_v[...], zt[:, pl.ds(off, TOK)]).astype(BF16)

        def piece(i, _):
            r = pl.ds(pl.multiple_of(off + i * LANES, LANES), LANES)
            du = dot_v[:, r].T.astype(F32)
            x_hat, inv = norm(x_v[r, :].astype(F32))
            prod = du * x_hat
            dgb[0] += jnp.sum(prod.reshape(LANES // 8, 8, dim), axis=0)
            dgb[1] += jnp.sum(du.reshape(LANES // 8, 8, dim), axis=0)
            a9 = du * gain_row
            m1 = jnp.sum(a9, axis=-1, keepdims=True) * (1.0 / dim)
            m2 = jnp.sum(a9 * x_hat, axis=-1, keepdims=True) * (1.0 / dim)
            gx = inv * (a9 - m1 - x_hat * m2)
            dy_v[r, :] = (dy_v[r, :].astype(F32) + gx).astype(BF16)
            return 0
        lax.fori_loop(0, TOK // LANES, piece, 0)
        tile_copy(1, t).start()
        return 0

    def y_body(t, _):
        off = pl.multiple_of(t * TOK, TOK)
        x_v[pl.ds(off, TOK), :] = (x_v[pl.ds(off, TOK), :].astype(F32) + mm(ot[:, pl.ds(off, TOK)].T, wo_v[...])).astype(BF16)
        tile_copy(0, t).start()
        return 0
    lax.fori_loop(0, 1, dx_body, 0)
    serve2_range(chunks - 3, chunks)
    lax.fori_loop(1, images * tiles, dx_body, 0)
    gb_all[me] = jnp.concatenate([jnp.sum(dgb[i], axis=0).reshape(dim // LANES, LANES) for i in range(2)], axis=0)
    for k in far_first:
        rcopy(gb_all.at[me], gb_all.at[me], gb_s.at[k], gb_r.at[k], (me + k) % n).start()
    lax.fori_loop(0, images * tiles, y_body, 0)

    lane = lax.broadcasted_iota(jnp.int32, (1, LANES), 1)
    dtau = jnp.zeros((1, LANES), F32)
    for d in range(n):
        row = c_all[0, d, 2:3, :]
        for b in range(1, images):
            row = row + c_all[b, d, 2:3, :]
        if d:
            row = pltpu.roll(row, 2 * d, 1)
        dtau = jnp.where(jnp.logical_and(lane >= 2 * d, lane < 2 * d + 2), row, dtau)
    dtau_ref[...] = dtau

    def s3_wo(c, _):
        dwo_ref[:, pl.ds(pl.multiple_of(c * COLS, COLS), COLS)] = serve3(c)
        return 0
    lax.fori_loop(0, o_chunks, s3_wo, 0)

    def s3_v(c, _):
        dwqkv_ref[:, pl.ds(pl.multiple_of(2 * dim - dim + c * COLS, COLS), COLS)] = serve3(c)
        return 0
    lax.fori_loop(o_chunks, 2 * o_chunks, s3_v, 0)

    for k in peers:
        src = (me + n - k) % n
        rcopy(gb_all.at[me], gb_all.at[src], gb_s.at[k], gb_r.at[k], me).wait_recv()
    tot = gb_all[0]
    for d in range(1, n):
        tot = tot + gb_all[d]
    dgain_ref[...] = tot[:dim // LANES]
    dbias_ref[...] = tot[dim // LANES:]

    def s3_qk(c, _):
        dwqkv_ref[:, pl.ds(pl.multiple_of(c * COLS - 2 * dim, COLS), COLS)] = serve3(c)
        return 0
    lax.fori_loop(2 * o_chunks, chunks, s3_qk, 0)

    for b in range(images):
        for k in peers:
            rcopy(gs_out.at[b, 0], gs_in.at[b, k], gs_s.at[b, k], gs_r.at[b, k], me).wait_send()
            rcopy(a_all.at[b, me], a_all.at[b, me], a_s.at[b, k], a_r.at[b, k], me).wait_send()
            rcopy(ds_out.at[b, 0], ds_in.at[b, k], ds_s.at[b, k], ds_r.at[b, k], me).wait_send()
            rcopy(g_all.at[b, me], g_all.at[b, me], g_s.at[b, k], g_r.at[b, k], me).wait_send()
            rcopy(c_all.at[b, me], c_all.at[b, me], c_s.at[b, k], c_r.at[b, k], me).wait_send()
    for k in peers:
        rcopy(gb_all.at[me], gb_all.at[me], gb_s.at[k], gb_r.at[k], me).wait_send()

    def drain(c, _):
        d2d(c).wait_send()
        for h in hop1(c) + hop2(c):
            h.wait_send()
        return 0
    lax.fori_loop(0, chunks, drain, 0)
    for i in range(2):
        for t in range(images * tiles):
            tile_copy(i, t).wait()


def finish_kernel(heads, y_hbm, dx_hbm, dwqkv_ref, dwo_ref, dgain_ref, dbias_ref, dtau_ref,
                  y_out, dx_out, dwqkv_out, dwo_out, dgain_out, dbias_out, dtau_out, buf, sem_in, sem_out):
    images, tokens, dim = y_out.shape
    parts = tokens // TOK
    ins, outs = [], []
    for src, dst in ((y_hbm, y_out), (dx_hbm, dx_out)):
        for b in range(images):
            for t in range(parts):
                i = len(ins)
                ins.append(pltpu.make_async_copy(src.at[pl.ds((b * parts + t) * TOK, TOK)], buf.at[i], sem_in.at[i]))
                outs.append(pltpu.make_async_copy(buf.at[i], dst.at[b, pl.ds(t * TOK, TOK)], sem_out.at[i]))
    for c in ins:
        c.start()
    dwqkv_out[...] = dwqkv_ref[...]
    dwo_out[...] = dwo_ref[...]
    dgain_out[...] = dgain_ref[...].reshape(dgain_out.shape)
    dbias_out[...] = dbias_ref[...].reshape(dbias_out.shape)
    dtau_out[...] = dtau_ref[...].reshape(dtau_ref.shape[1])[:heads]
    for c, o in zip(ins, outs):
        c.wait()
        o.start()
    for o in outs:
        o.wait()


def solution(mesh):
    n = mesh.shape["sp"]

    def local_step(x_in, grad_y, ln_gain, ln_bias, w_qkv, w_out, temp_tau):
        images, tokens, dim = x_in.shape
        heads = temp_tau.shape[0]
        hd = dim // heads
        rows = images * tokens
        per_dev = dim // n
        chunks = 4 * dim // COLS
        nwin = -(-heads // (COLS // hd))
        any_spec = pl.BlockSpec(memory_space=pl.ANY)
        vmem = pl.BlockSpec(memory_space=pltpu.VMEM)
        dma = pltpu.SemaphoreType.DMA
        pairs = (images, n)
        out = pl.pallas_call(
            functools.partial(xca_kernel, n, heads),
            out_shape=(
                jax.ShapeDtypeStruct((rows, dim), BF16),
                jax.ShapeDtypeStruct((rows, dim), BF16),
                jax.ShapeDtypeStruct((per_dev, 3 * dim), BF16),
                jax.ShapeDtypeStruct((per_dev, dim), BF16),
                jax.ShapeDtypeStruct((dim // LANES, LANES), F32),
                jax.ShapeDtypeStruct((dim // LANES, LANES), F32),
                jax.ShapeDtypeStruct((1, LANES), F32),
            ),
            in_specs=[any_spec] * 7,
            out_specs=(any_spec,) * 2 + (vmem,) * 5,
            scratch_shapes=[
                pltpu.VMEM((dim,), F32),
                pltpu.VMEM((dim,), F32),
                pltpu.VMEM((heads,), F32),
                pltpu.VMEM((rows, dim), BF16),
                pltpu.VMEM((rows, dim), BF16),
                pltpu.VMEM((dim, 3 * dim), BF16),
                pltpu.VMEM((3 * dim, dim), BF16),
                pltpu.VMEM((dim, dim), BF16),
                pltpu.VMEM((dim, rows), BF16),
                pltpu.VMEM((3 * dim, rows), BF16),
                pltpu.VMEM((dim, rows), BF16),
                pltpu.VMEM((dim, rows), BF16),
                pltpu.VMEM((images, 2 * dim, LANES), F32),
                pltpu.VMEM((images, n, hd, LANES), F32),
                pltpu.VMEM((images, n, hd, LANES), F32),
                pltpu.VMEM((images, hd, LANES), F32),
                pltpu.VMEM((images, n, hd, LANES), BF16),
                pltpu.VMEM((images, n, hd, LANES), F32),
                pltpu.VMEM((images, n, hd, LANES), F32),
                pltpu.VMEM((images, n, hd, LANES), BF16),
                pltpu.VMEM((images, n, 8, LANES), F32),
                pltpu.VMEM((images, nwin, 2, COLS, COLS), BF16),
                pltpu.VMEM((dim, LANES), F32),
                pltpu.VMEM((dim, LANES), F32),
                pltpu.VMEM((2, 8, dim), F32),
                pltpu.VMEM((n, 2 * dim // LANES, LANES), F32),
                pltpu.VMEM((chunks, 2, n // 2, per_dev, COLS), F32),
                pltpu.VMEM((chunks, n // 2, per_dev, COLS), F32),
                pltpu.VMEM((chunks, 2, per_dev // 2, COLS), F32),
                pltpu.VMEM((chunks, 2, per_dev, COLS), F32),
                dma((rows // TOK + images + 6,)), dma((2, rows // TOK)),
                dma((chunks,)), dma((chunks,)),
                dma((chunks, 2)), dma((chunks, 2)), dma((chunks, 2)), dma((chunks, 2)),
                dma(pairs), dma(pairs), dma(pairs), dma(pairs), dma(pairs), dma(pairs),
                dma(pairs), dma(pairs), dma(pairs), dma(pairs),
                dma((n,)), dma((n,)),
            ],
            compiler_params=pltpu.CompilerParams(
                collective_id=0, has_side_effects=True, vmem_limit_bytes=VMEM_LIMIT),
            name="xca_block",
        )(x_in, grad_y, ln_gain, ln_bias, w_qkv, w_out, temp_tau)
        return pl.pallas_call(
            functools.partial(finish_kernel, heads),
            out_shape=(
                jax.ShapeDtypeStruct(x_in.shape, BF16),
                jax.ShapeDtypeStruct(x_in.shape, BF16),
                jax.ShapeDtypeStruct((per_dev, 3 * dim), BF16),
                jax.ShapeDtypeStruct((per_dev, dim), BF16),
                jax.ShapeDtypeStruct((dim,), F32),
                jax.ShapeDtypeStruct((dim,), F32),
                jax.ShapeDtypeStruct((heads,), F32),
            ),
            in_specs=[any_spec] * 2 + [vmem] * 5,
            out_specs=(any_spec,) * 2 + (vmem,) * 5,
            scratch_shapes=[
                pltpu.VMEM((2 * rows // TOK, TOK, dim), BF16),
                dma((2 * rows // TOK,)), dma((2 * rows // TOK,)),
            ],
            name="finish",
        )(*out)

    tok = P("dp", "sp", None)
    return jax.shard_map(
        local_step, mesh=mesh,
        in_specs=(tok, tok, P(), P(), P(), P(), P()),
        out_specs=(tok, tok, P(("dp", "sp"), None), P(("dp", "sp"), None), P("dp"), P("dp"), P("dp")),
        check_vma=False)
```

```python
import functools

import jax
import jax.numpy as jnp
from jax import lax
from jax.experimental import pallas as pl
from jax.experimental.pallas import tpu as pltpu
from jax.sharding import PartitionSpec as P

LN_EPS = 1e-6
F32 = jnp.float32
BF16 = jnp.bfloat16
LANES = 128
TOK = 512
COLS = 256
VMEM_LIMIT = 67043328
NN = (((1,), (0,)), ((), ()))
NT = (((1,), (1,)), ((), ()))


def mm(a, b, dims=NN):
    return lax.dot_general(a, b, dims, preferred_element_type=F32)


def xca_kernel(
    n, heads,
    x_hbm, dy_hbm, gain_hbm, bias_hbm, wqkv_hbm, wo_hbm, tau_hbm,
    y_hbm, dx_hbm, dwqkv_ref, dwo_ref, dgain_ref, dbias_ref, dtau_ref,
    gain_ref, bias_ref, tau_ref, x_v, dy_v, w_v, wt_v, wo_v, ut, zt, dot_v, ot,
    sq_acc, gs_out, gs_mid, gs_in, gs_sum, a_all, ds_out, ds_mid, ds_in, g_all, c_all, bd, colq, colk, dgb, gb_all,
    part, r1, r2, r3,
    in_sem, out_sem, d2d_s, d2d_r, p1_s, p1_r, p2_s, p2_r,
    gs_s, gs_r, a_s, a_r, ds_s, ds_r, g_s, g_r, c_s, c_r, gb_s, gb_r,
):
    images, tokens, dim = x_hbm.shape
    hd = dim // heads
    rows = images * tokens
    per_dev = dim // n
    chips = n // 2
    wheads = COLS // hd
    wrow = wheads * hd
    nwin = -(-heads // wheads)
    tiles = tokens // TOK
    o_chunks = dim // COLS
    chunks = 4 * o_chunks
    me = lax.axis_index("sp")
    chip, core = me // 2, me % 2
    right = ((chip + 1) % chips) * 2 + core
    left = ((chip + chips - 1) % chips) * 2 + core
    partner = chip * 2 + (1 - core)
    cr, cl, co = (chip + 1) % chips, (chip + chips - 1) % chips, (chip + 2) % chips

    peers = range(1, n)
    far_first = sorted(peers, key=lambda k: abs(2 * k - n))

    def rcopy(src, dst, ss, rs, dev):
        return pltpu.make_async_remote_copy(
            src_ref=src, dst_ref=dst, send_sem=ss, recv_sem=rs,
            device_id={"sp": dev}, device_id_type=pl.DeviceIdType.MESH)

    def cp_x(b, t):
        return pltpu.make_async_copy(x_hbm.at[b, pl.ds(t * TOK, TOK)], x_v.at[pl.ds(b * tokens + t * TOK, TOK)], in_sem.at[b * tiles + t])

    def cp_dy(b):
        return pltpu.make_async_copy(dy_hbm.at[b], dy_v.at[pl.ds(b * tokens, tokens)], in_sem.at[images * tiles + b])

    base = images * tiles + images
    cp_small = [pltpu.make_async_copy(h, v, in_sem.at[base + i]) for i, (h, v) in enumerate(
        ((gain_hbm, gain_ref), (bias_hbm, bias_ref), (tau_hbm, tau_ref)))]
    base += 3
    cp_wq, cp_wk, cp_wv = [pltpu.make_async_copy(wqkv_hbm.at[:, pl.ds(i * dim, dim)], w_v.at[:, pl.ds(i * dim, dim)], in_sem.at[base + i])
                           for i in range(3)]
    cp_wo = pltpu.make_async_copy(wo_hbm, wo_v, in_sem.at[base + 3])
    for c in cp_small:
        c.start()
    cp_x(0, 0).start()
    cp_wq.start()
    cp_x(0, 1).start()
    cp_wk.start()

    barrier = pltpu.get_barrier_semaphore()
    for k in peers:
        pl.semaphore_signal(barrier, inc=1, device_id={"sp": (me + k) % n},
                            device_id_type=pl.DeviceIdType.MESH)
    sq_acc[...] = jnp.zeros_like(sq_acc)
    bd[...] = jnp.zeros_like(bd)
    dgb[...] = jnp.zeros_like(dgb)
    for c in cp_small:
        c.wait()
    cp_x(0, 0).wait()

    def norm(xt):
        mean = jnp.sum(xt, axis=-1, keepdims=True) * (1.0 / dim)
        cen = xt - mean
        inv = lax.rsqrt(jnp.sum(cen * cen, axis=-1, keepdims=True) * (1.0 / dim) + LN_EPS)
        return cen * inv, inv

    gain_row = gain_ref[...].reshape(1, dim)
    bias_row = bias_ref[...].reshape(1, dim)

    def norm_rows(r0, count):
        x_hat, _inv = norm(x_v[pl.ds(r0, count), :].astype(F32))
        ut[:, pl.ds(r0, count)] = (x_hat * gain_row + bias_row).astype(BF16).T

    def transpose_w(c0, count):
        def body(i, _):
            off = pl.multiple_of(c0 + i * COLS, COLS)
            wt_v[pl.ds(off, COLS), :] = w_v[:, pl.ds(off, COLS)].T
            return 0
        lax.fori_loop(0, count // COLS, body, 0)

    other_chips = range(1, chips)

    def pair_sum(out, mid, ss, rs, b):
        return rcopy(out.at[b, 1 - core], mid.at[b], ss.at[b, 0], rs.at[b, 0], partner)

    def chip_copy(out, into, ss, rs, b, k):
        to = (chip + k) % chips
        return rcopy(out.at[b, core, to], into.at[b, k], ss.at[b, k], rs.at[b, k], to * 2 + core)

    def scatter_state(out, mid, into, ss, rs, b):
        pair_sum(out, mid, ss, rs, b).wait_recv()
        out[b, core] += mid[b]
        for k in (2, 1, 3):
            chip_copy(out, into, ss, rs, b, k).start()

    def state_total(out, into, ss, rs, b):
        tot = out[b, core, chip]
        for k in other_chips:
            tot = tot + into[b, k]
        return tot

    lane_w = lax.broadcasted_iota(jnp.int32, (hd, LANES), 1)

    def to_pairs(blocks, out_ref, extra=None):
        for d in range(n):
            picked = []
            for s in range(2):
                w, k = divmod(2 * d + s, wheads)
                strip = blocks[w][k * hd:(k + 1) * hd, :]
                shift = (s * hd - k * hd) % COLS
                if shift:
                    strip = pltpu.roll(strip, shift, 1)
                picked.append(strip[:, :LANES])
            rest = 0.0
            if extra is not None:
                for i, col in enumerate(extra):
                    for s in range(2):
                        r0 = (2 * d + s) * hd
                        rest = jnp.where(lane_w == 2 * hd + 2 * i + s, col[r0:r0 + hd], rest)
            out_ref[d % 2, d // 2] = jnp.where(lane_w < hd, picked[0], jnp.where(lane_w < 2 * hd, picked[1], rest))

    def gram(b, l_ref, l0, r_ref, r0):
        blocks = []
        for w in range(nwin):
            m = min(wrow, dim - w * wrow)
            lo, ro = l0 + w * wrow, r0 + w * wrow
            nw = min(COLS, dim - w * wrow)
            left_op = l_ref[lo:lo + m, b * tokens:(b + 1) * tokens]
            right_op = r_ref[ro:ro + nw, b * tokens:(b + 1) * tokens]
            g = mm(left_op, right_op, NT)
            if nw < COLS:
                g = jnp.pad(g, ((0, 0), (0, COLS - nw)))
            blocks.append(g)
        return blocks

    def qk_tile(off, following, wt_cols=None):
        if wt_cols == dim:
            wt_v[dim:2 * dim, :] = w_v[:, dim:2 * dim].T
        for m in range(2):
            z = mm(wt_v[m * dim:(m + 1) * dim, :], ut[:, pl.ds(off, TOK)]).astype(BF16)
            zt[m * dim:(m + 1) * dim, pl.ds(off, TOK)] = z
            zf = z.astype(F32)
            sq = zf * zf
            tot = sq[:, 0:LANES]
            for j in range(1, TOK // LANES):
                tot = tot + sq[:, j * LANES:(j + 1) * LANES]
            sq_acc[off // tokens, m * dim:(m + 1) * dim] += tot
        if following is not None:
            norm_rows(following, TOK)
        if wt_cols is not None and wt_cols > dim:
            wt_v[wt_cols:wt_cols + dim // 2, :] = w_v[:, wt_cols:wt_cols + dim // 2].T

    def send_gram(b):
        cols = [jnp.sum(sq_acc[b, m * dim:(m + 1) * dim], axis=1, keepdims=True) for m in range(2)]
        to_pairs(gram(b, zt, 0, zt, dim), gs_out.at[b], cols)
        if b == 0:
            pl.semaphore_wait(barrier, n - 1)
        pair_sum(gs_out, gs_mid, gs_s, gs_r, b).start()

    for b in range(1, images):
        for t in range(tiles):
            cp_x(b, t).start()
    norm_rows(0, TOK)
    cp_wq.wait()
    cp_wv.start()
    cp_wo.start()
    for b in range(images):
        cp_dy(b).start()
    transpose_w(0, dim)
    cp_x(0, 1).wait()
    cp_wk.wait()
    qk_tile(0, TOK, dim)
    for t in range(tiles):
        cp_x(1, t).wait()
    for t in range(1, tiles):
        qk_tile(t * TOK, (t + 1) * TOK)
    send_gram(0)
    cp_wv.wait()
    for t in range(tiles):
        if t == 1:
            scatter_state(gs_out, gs_mid, gs_in, gs_s, gs_r, 0)
        off = tokens + t * TOK
        qk_tile(off, off + TOK if t + 1 < tiles else None, 2 * dim + t * dim // tiles)
    send_gram(1)

    def values(b):
        for t in range(tiles):
            tok_t = pl.ds(b * tokens + t * TOK, TOK)
            zt[2 * dim:3 * dim, tok_t] = mm(wt_v[2 * dim:3 * dim, :], ut[:, tok_t]).astype(BF16)

    eye = lax.broadcasted_iota(jnp.int32, (hd, hd), 0) == lax.broadcasted_iota(jnp.int32, (hd, hd), 1)

    def row_of(col):
        return jnp.sum(jnp.where(eye, col, 0.0), axis=0, keepdims=True)

    head_lane = lax.broadcasted_iota(jnp.int32, (1, heads), 1)
    tau_row = tau_ref[...].reshape(1, heads)

    def attn_state(b, s):
        blk = gs_sum[b]
        g = blk[:, s * hd:(s + 1) * hd]
        qc = blk[:, 2 * hd + s:2 * hd + s + 1]
        kr = row_of(blk[:, 2 * hd + 2 + s:2 * hd + 3 + s])
        unit = lax.rsqrt(qc) * lax.rsqrt(kr)
        tau = jnp.sum(jnp.where(head_lane == me * 2 + s, tau_row, 0.0), axis=1, keepdims=True)
        cosine = g * unit
        logits = tau * cosine
        e = jnp.exp(logits - jnp.max(logits, axis=-1, keepdims=True))
        probs = e / jnp.sum(e, axis=-1, keepdims=True)
        return cosine, logits, probs, tau * unit, qc, kr

    def pair(a0, a1):
        r = a0.shape[0]
        z = jnp.zeros((r, LANES - 2 * hd), a0.dtype)
        return jnp.concatenate([a0, a1, z], axis=1)

    def owner_forward(b):
        for k in other_chips:
            chip_copy(gs_out, gs_in, gs_s, gs_r, b, k).wait_recv()
        gs_sum[b] = state_total(gs_out, gs_in, gs_s, gs_r, b)
        p0 = attn_state(b, 0)[2]
        p1 = attn_state(b, 1)[2]
        a_all[b, me] = pair(p0, p1).astype(BF16)
        for k in far_first:
            dst = (me + k) % n
            rcopy(a_all.at[b, me], a_all.at[b, me], a_s.at[b, k], a_r.at[b, k], dst).start()

    def owner_backward():
        for b in range(images):
            for k in other_chips:
                chip_copy(ds_out, ds_in, ds_s, ds_r, b, k).wait_recv()
        sub = lax.broadcasted_iota(jnp.int32, (8, LANES), 0)
        lane = lax.broadcasted_iota(jnp.int32, (8, LANES), 1)
        for b in range(images):
            tot = state_total(ds_out, ds_in, ds_s, ds_r, b).astype(BF16).astype(F32)
            gs, qs, ks, ts = [], [], [], []
            for s in range(2):
                cosine, logits, probs, scale, qc, kr = attn_state(b, s)
                dp = tot[:, s * hd:(s + 1) * hd]
                gl = probs * (dp - jnp.sum(probs * dp, axis=-1, keepdims=True))
                weighted = gl * logits
                gs.append(gl * scale)
                qs.append(row_of(-jnp.sum(weighted, axis=1, keepdims=True) / qc))
                ks.append(-jnp.sum(weighted, axis=0, keepdims=True) / kr)
                ts.append(jnp.sum(jnp.sum(gl * cosine, axis=1, keepdims=True), axis=0, keepdims=True))
            g_all[b, me] = pair(gs[0], gs[1]).astype(BF16)
            taus = jnp.where(lane == 0, ts[0], jnp.where(lane == 1, ts[1], 0.0))
            c_all[b, me] = jnp.where(sub == 0, pair(qs[0], qs[1]), jnp.where(sub == 1, pair(ks[0], ks[1]), jnp.where(sub == 2, taus, 0.0)))
        for b in range(images):
            for ref, ss, rs in states:
                for k in (4, 2, 6, 1):
                    dst = (me + k) % n if k > 1 else partner
                    rcopy(ref.at[b, me], ref.at[b, me], ss.at[b, k], rs.at[b, k], dst).start()

    states = ((g_all, g_s, g_r), (c_all, c_s, c_r))

    def pass_on(b):
        for ref, ss, rs in states:
            for k in (2, 6, 4):
                src = (me + n - k) % n
                rcopy(ref.at[b, me], ref.at[b, src], ss.at[b, k], rs.at[b, k], me).wait_recv()
                rcopy(ref.at[b, src], ref.at[b, src], ss.at[b, k + 1], rs.at[b, k + 1], partner).start()

    def passed(b):
        for ref, ss, rs in states:
            rcopy(ref.at[b, me], ref.at[b, partner], ss.at[b, 1], rs.at[b, 1], me).wait_recv()
            for k in (2, 6, 4):
                src = (partner + n - k) % n
                rcopy(ref.at[b, me], ref.at[b, src], ss.at[b, k + 1], rs.at[b, k + 1], me).wait_recv()

    def gathered(ref, ss, rs, b):
        for k in peers:
            src = (me + n - k) % n
            rcopy(ref.at[b, me], ref.at[b, src], ss.at[b, k], rs.at[b, k], me).wait_recv()

    def grad_heads(b):
        cp_dy(b).wait()
        if b == 0:
            cp_wo.wait()

        for t in range(tiles):
            tok_t = pl.ds(b * tokens + t * TOK, TOK)
            dot_v[:, tok_t] = mm(wo_v[...], dy_v[tok_t, :], NT).astype(BF16)

    def send_dprobs(b):
        to_pairs(gram(b, dot_v, 0, zt, 2 * dim), ds_out.at[b])
        pair_sum(ds_out, ds_mid, ds_s, ds_r, b).start()

    sj = lax.broadcasted_iota(jnp.int32, (LANES, COLS), 0)
    slane = lax.broadcasted_iota(jnp.int32, (LANES, COLS), 1)
    sels = []
    for s in range(2):
        hit = jnp.zeros((LANES, COLS), jnp.bool_)
        for k in range(wheads):
            hit = jnp.logical_or(hit, slane - k * hd == sj - s * hd)
        hit = jnp.logical_and(hit, jnp.logical_and(sj >= s * hd, sj < (s + 1) * hd))
        sels.append(jnp.where(hit, 1.0, 0.0).astype(BF16))
    blane = lax.broadcasted_iota(jnp.int32, (hd, COLS), 1)

    def build(ref, b):
        flat = ref[b].reshape(n * hd, LANES)
        for s in range(2):
            spread = mm(flat, sels[s])
            for d in range(n):
                w, k = divmod(2 * d + s, wheads)
                blk = jnp.where(jnp.logical_and(blane >= k * hd, blane < (k + 1) * hd), spread[d * hd:(d + 1) * hd], 0.0)
                bd[b, w, 0, k * hd:(k + 1) * hd, :] = blk.astype(BF16)
        for w in range(nwin):
            bd[b, w, 1] = bd[b, w, 0].T

    def windows():
        for w in range(nwin):
            r0 = w * wrow
            yield w, r0, min(wrow, dim - r0), min(COLS, dim - r0)

    def heads_out(b):
        for t in range(tiles):
            tok_t = pl.ds(b * tokens + t * TOK, TOK)
            for w, r0, m, kk in windows():
                ot[r0:r0 + m, tok_t] = mm(bd[b, w, 0, 0:m, 0:kk], zt[2 * dim + r0:2 * dim + r0 + kk, tok_t]).astype(BF16)

    def grad_values(b):
        def body(t, _):
            off = pl.multiple_of(b * tokens + t * TOK, TOK)
            for w, r0, m, kk in windows():
                zt[2 * dim + r0:2 * dim + r0 + m, pl.ds(off, TOK)] = mm(bd[b, w, 1, 0:m, 0:kk], dot_v[r0:r0 + kk, pl.ds(off, TOK)]).astype(BF16)
            return 0
        lax.fori_loop(0, tiles, body, 0)

    def dq_and_dk(b):
        ct = c_all[b].reshape(n * 8, LANES).T
        for d in range(n):
            colq[d * per_dev:(d + 1) * per_dev, :] = jnp.broadcast_to(ct[0:per_dev, 8 * d:8 * d + 1], (per_dev, LANES))
            colk[d * per_dev:(d + 1) * per_dev, :] = jnp.broadcast_to(ct[0:per_dev, 8 * d + 1:8 * d + 2], (per_dev, LANES))

        def body(t, _):
            off = pl.multiple_of(b * tokens + t * TOK, TOK)
            for w, r0, m, kk in windows():
                qw = zt[r0:r0 + kk, pl.ds(off, TOK)]
                kw = zt[dim + r0:dim + r0 + kk, pl.ds(off, TOK)]
                cq = jnp.concatenate([colq[r0:r0 + m, :]] * (TOK // LANES), axis=1)
                ck = jnp.concatenate([colk[r0:r0 + m, :]] * (TOK // LANES), axis=1)
                dq = mm(bd[b, w, 0, 0:m, 0:kk], kw) + cq * qw[0:m].astype(F32)
                dk = mm(bd[b, w, 1, 0:m, 0:kk], qw) + ck * kw[0:m].astype(F32)
                zt[r0:r0 + m, pl.ds(off, TOK)] = dq.astype(BF16)
                zt[dim + r0:dim + r0 + m, pl.ds(off, TOK)] = dk.astype(BF16)
            return 0
        lax.fori_loop(0, tiles, body, 0)

    def put_part(c, val):
        for j in range(n):
            part[c, j % 2, j // 2] = val[j * per_dev:(j + 1) * per_dev, :]

    def d2d(c):
        return rcopy(part.at[c, 1 - core], r1.at[c], d2d_s.at[c], d2d_r.at[c], partner)

    half = per_dev // 2

    def hop1(c):
        return (rcopy(r1.at[c, co, pl.ds(0, half)], r2.at[c, 0], p1_s.at[c, 0], p1_r.at[c, 0], right),
                rcopy(r1.at[c, co, pl.ds(half, half)], r2.at[c, 1], p1_s.at[c, 1], p1_r.at[c, 1], left))

    def hop2(c):
        return (rcopy(r1.at[c, cr], r3.at[c, 0], p2_s.at[c, 0], p2_r.at[c, 0], right),
                rcopy(r1.at[c, cl], r3.at[c, 1], p2_s.at[c, 1], p2_r.at[c, 1], left))

    def serve1(c):
        d2d(c).wait_recv()
        for blk in (co, cr, cl, chip):
            r1[c, blk] += part[c, core, blk]
        for h in hop1(c):
            h.start()

    def serve2(c):
        for h in hop1(c):
            h.wait_recv()
        r1[c, cr, 0:half] += r2[c, 0]
        r1[c, cl, half:per_dev] += r2[c, 1]
        for h in hop2(c):
            h.start()

    def serve3(c):
        for h in hop2(c):
            h.wait_recv()
        return (r1[c, chip] + r3[c, 0] + r3[c, 1]).astype(BF16)

    def wo_chunk(c):
        off = pl.multiple_of(c * COLS, COLS)
        put_part(c, mm(ot[...], dy_v[:, pl.ds(off, COLS)]))
        d2d(c).start()

    def qkv_chunk(c, base):
        off = pl.multiple_of(base + c * COLS, COLS)
        put_part(c, mm(ut[...], zt[pl.ds(off, COLS), :], NT))
        d2d(c).start()

    values(0)
    scatter_state(gs_out, gs_mid, gs_in, gs_s, gs_r, 1)
    grad_heads(0)
    owner_forward(0)
    send_dprobs(0)
    values(1)
    scatter_state(ds_out, ds_mid, ds_in, ds_s, ds_r, 0)
    owner_forward(1)
    grad_heads(1)
    send_dprobs(1)
    gathered(a_all, a_s, a_r, 0)
    build(a_all, 0)
    heads_out(0)
    scatter_state(ds_out, ds_mid, ds_in, ds_s, ds_r, 1)
    gathered(a_all, a_s, a_r, 1)
    build(a_all, 1)
    heads_out(1)

    def wo_loop(c, _):
        wo_chunk(c)

        @pl.when(c > 0)
        def _():
            serve1(c - 1)
        return 0
    lax.fori_loop(0, o_chunks, wo_loop, 0)
    owner_backward()
    serve1(o_chunks - 1)
    grad_values(0)
    grad_values(1)
    v0 = 2 * dim - o_chunks * COLS
    qkv_chunk(o_chunks, v0)

    def s2_body(c, _):
        serve2(c)
        return 0

    def serve2_range(c0, c1):
        lax.fori_loop(c0, c1, s2_body, 0)

    serve2_range(0, 2)

    def v_loop(c, _):
        qkv_chunk(c, v0)
        serve1(c - 1)
        return 0
    lax.fori_loop(o_chunks + 1, 2 * o_chunks, v_loop, 0)
    for b in range(images):
        pass_on(b)
    serve2_range(2, 3)
    for b in range(images):
        passed(b)
        build(g_all, b)
        dq_and_dk(b)
        if b == 0:
            serve1(2 * o_chunks - 1)
    serve2_range(3, 4)
    qkv_chunk(2 * o_chunks, -2 * o_chunks * COLS)

    def qk_loop(c, _):
        qkv_chunk(c, -2 * o_chunks * COLS)
        serve1(c - 1)
        return 0
    lax.fori_loop(2 * o_chunks + 1, chunks, qk_loop, 0)
    serve1(chunks - 1)
    serve2_range(4, chunks - 3)

    def tile_copy(i, t):
        rows_t = pl.ds(pl.multiple_of(t * TOK, TOK), TOK)
        src, dst = ((x_v, y_hbm), (dy_v, dx_hbm))[i]
        return pltpu.make_async_copy(src.at[rows_t], dst.at[rows_t], out_sem.at[i, t])

    def dx_body(t, _):
        off = pl.multiple_of(t * TOK, TOK)
        dot_v[:, pl.ds(off, TOK)] = mm(w_v[...], zt[:, pl.ds(off, TOK)]).astype(BF16)

        def piece(i, _):
            r = pl.ds(pl.multiple_of(off + i * LANES, LANES), LANES)
            du = dot_v[:, r].T.astype(F32)
            xt = x_v[r, :].astype(F32)
            x_v[r, :] = (xt + mm(ot[:, r].T, wo_v[...])).astype(BF16)
            x_hat, inv = norm(xt)
            prod = du * x_hat
            dgb[0] += jnp.sum(prod.reshape(LANES // 8, 8, dim), axis=0)
            dgb[1] += jnp.sum(du.reshape(LANES // 8, 8, dim), axis=0)
            a9 = du * gain_row
            m1 = jnp.sum(a9, axis=-1, keepdims=True) * (1.0 / dim)
            m2 = jnp.sum(a9 * x_hat, axis=-1, keepdims=True) * (1.0 / dim)
            gx = inv * (a9 - m1 - x_hat * m2)
            dy_v[r, :] = (dy_v[r, :].astype(F32) + gx).astype(BF16)
            return 0
        lax.fori_loop(0, TOK // LANES, piece, 0)
        tile_copy(0, t).start()
        tile_copy(1, t).start()
        return 0

    lax.fori_loop(0, 1, dx_body, 0)
    serve2_range(chunks - 3, chunks)
    lax.fori_loop(1, images * tiles, dx_body, 0)
    gb_all[me] = jnp.concatenate([jnp.sum(dgb[i], axis=0).reshape(dim // LANES, LANES) for i in range(2)], axis=0)
    for k in far_first:
        rcopy(gb_all.at[me], gb_all.at[me], gb_s.at[k], gb_r.at[k], (me + k) % n).start()

    lane = lax.broadcasted_iota(jnp.int32, (1, LANES), 1)
    dtau = jnp.zeros((1, LANES), F32)
    for d in range(n):
        row = c_all[0, d, 2:3, :]
        for b in range(1, images):
            row = row + c_all[b, d, 2:3, :]
        if d:
            row = pltpu.roll(row, 2 * d, 1)
        dtau = jnp.where(jnp.logical_and(lane >= 2 * d, lane < 2 * d + 2), row, dtau)
    dtau_ref[...] = dtau

    def s3_wo(c, _):
        dwo_ref[:, pl.ds(pl.multiple_of(c * COLS, COLS), COLS)] = serve3(c)
        return 0
    lax.fori_loop(0, o_chunks, s3_wo, 0)

    def s3_v(c, _):
        dwqkv_ref[:, pl.ds(pl.multiple_of(2 * dim - dim + c * COLS, COLS), COLS)] = serve3(c)
        return 0
    lax.fori_loop(o_chunks, 2 * o_chunks, s3_v, 0)

    for k in peers:
        src = (me + n - k) % n
        rcopy(gb_all.at[me], gb_all.at[src], gb_s.at[k], gb_r.at[k], me).wait_recv()
    tot = gb_all[0]
    for d in range(1, n):
        tot = tot + gb_all[d]
    dgain_ref[...] = tot[:dim // LANES]
    dbias_ref[...] = tot[dim // LANES:]

    def s3_qk(c, _):
        dwqkv_ref[:, pl.ds(pl.multiple_of(c * COLS - 2 * dim, COLS), COLS)] = serve3(c)
        return 0
    lax.fori_loop(2 * o_chunks, chunks, s3_qk, 0)

    for b in range(images):
        for out, mid, into, ss, rs in ((gs_out, gs_mid, gs_in, gs_s, gs_r), (ds_out, ds_mid, ds_in, ds_s, ds_r)):
            pair_sum(out, mid, ss, rs, b).wait_send()
            for k in other_chips:
                chip_copy(out, into, ss, rs, b, k).wait_send()
        for k in peers:
            rcopy(a_all.at[b, me], a_all.at[b, me], a_s.at[b, k], a_r.at[b, k], me).wait_send()
            rcopy(g_all.at[b, me], g_all.at[b, me], g_s.at[b, k], g_r.at[b, k], me).wait_send()
            rcopy(c_all.at[b, me], c_all.at[b, me], c_s.at[b, k], c_r.at[b, k], me).wait_send()
    for k in peers:
        rcopy(gb_all.at[me], gb_all.at[me], gb_s.at[k], gb_r.at[k], me).wait_send()

    def drain(c, _):
        d2d(c).wait_send()
        for h in hop1(c) + hop2(c):
            h.wait_send()
        return 0
    lax.fori_loop(0, chunks, drain, 0)
    for i in range(2):
        for t in range(images * tiles):
            tile_copy(i, t).wait()


def finish_kernel(heads, y_hbm, dx_hbm, dwqkv_ref, dwo_ref, dgain_ref, dbias_ref, dtau_ref,
                  y_out, dx_out, dwqkv_out, dwo_out, dgain_out, dbias_out, dtau_out, buf, sem_in, sem_out):
    images, tokens, dim = y_out.shape
    parts = tokens // TOK
    ins, outs = [], []
    for src, dst in ((y_hbm, y_out), (dx_hbm, dx_out)):
        for b in range(images):
            for t in range(parts):
                i = len(ins)
                ins.append(pltpu.make_async_copy(src.at[pl.ds((b * parts + t) * TOK, TOK)], buf.at[i], sem_in.at[i]))
                outs.append(pltpu.make_async_copy(buf.at[i], dst.at[b, pl.ds(t * TOK, TOK)], sem_out.at[i]))
    for c in ins:
        c.start()
    dwqkv_out[...] = dwqkv_ref[...]
    dwo_out[...] = dwo_ref[...]
    dgain_out[...] = dgain_ref[...].reshape(dgain_out.shape)
    dbias_out[...] = dbias_ref[...].reshape(dbias_out.shape)
    dtau_out[...] = dtau_ref[...].reshape(dtau_ref.shape[1])[:heads]
    for c, o in zip(ins, outs):
        c.wait()
        o.start()
    for o in outs:
        o.wait()


def solution(mesh):
    n = mesh.shape["sp"]

    def local_step(x_in, grad_y, ln_gain, ln_bias, w_qkv, w_out, temp_tau):
        images, tokens, dim = x_in.shape
        heads = temp_tau.shape[0]
        hd = dim // heads
        rows = images * tokens
        per_dev = dim // n
        chunks = 4 * dim // COLS
        nwin = -(-heads // (COLS // hd))
        any_spec = pl.BlockSpec(memory_space=pl.ANY)
        vmem = pl.BlockSpec(memory_space=pltpu.VMEM)
        dma = pltpu.SemaphoreType.DMA
        pairs = (images, n)
        out = pl.pallas_call(
            functools.partial(xca_kernel, n, heads),
            out_shape=(
                jax.ShapeDtypeStruct((rows, dim), BF16),
                jax.ShapeDtypeStruct((rows, dim), BF16),
                jax.ShapeDtypeStruct((per_dev, 3 * dim), BF16),
                jax.ShapeDtypeStruct((per_dev, dim), BF16),
                jax.ShapeDtypeStruct((dim // LANES, LANES), F32),
                jax.ShapeDtypeStruct((dim // LANES, LANES), F32),
                jax.ShapeDtypeStruct((1, LANES), F32),
            ),
            in_specs=[any_spec] * 7,
            out_specs=(any_spec,) * 2 + (vmem,) * 5,
            scratch_shapes=[
                pltpu.VMEM((dim,), F32),
                pltpu.VMEM((dim,), F32),
                pltpu.VMEM((heads,), F32),
                pltpu.VMEM((rows, dim), BF16),
                pltpu.VMEM((rows, dim), BF16),
                pltpu.VMEM((dim, 3 * dim), BF16),
                pltpu.VMEM((3 * dim, dim), BF16),
                pltpu.VMEM((dim, dim), BF16),
                pltpu.VMEM((dim, rows), BF16),
                pltpu.VMEM((3 * dim, rows), BF16),
                pltpu.VMEM((dim, rows), BF16),
                pltpu.VMEM((dim, rows), BF16),
                pltpu.VMEM((images, 2 * dim, LANES), F32),
                pltpu.VMEM((images, 2, n // 2, hd, LANES), F32),
                pltpu.VMEM((images, n // 2, hd, LANES), F32),
                pltpu.VMEM((images, n // 2, hd, LANES), F32),
                pltpu.VMEM((images, hd, LANES), F32),
                pltpu.VMEM((images, n, hd, LANES), BF16),
                pltpu.VMEM((images, 2, n // 2, hd, LANES), F32),
                pltpu.VMEM((images, n // 2, hd, LANES), F32),
                pltpu.VMEM((images, n // 2, hd, LANES), F32),
                pltpu.VMEM((images, n, hd, LANES), BF16),
                pltpu.VMEM((images, n, 8, LANES), F32),
                pltpu.VMEM((images, nwin, 2, COLS, COLS), BF16),
                pltpu.VMEM((dim, LANES), F32),
                pltpu.VMEM((dim, LANES), F32),
                pltpu.VMEM((2, 8, dim), F32),
                pltpu.VMEM((n, 2 * dim // LANES, LANES), F32),
                pltpu.VMEM((chunks, 2, n // 2, per_dev, COLS), F32),
                pltpu.VMEM((chunks, n // 2, per_dev, COLS), F32),
                pltpu.VMEM((chunks, 2, per_dev // 2, COLS), F32),
                pltpu.VMEM((chunks, 2, per_dev, COLS), F32),
                dma((rows // TOK + images + 7,)), dma((2, rows // TOK)),
                dma((chunks,)), dma((chunks,)),
                dma((chunks, 2)), dma((chunks, 2)), dma((chunks, 2)), dma((chunks, 2)),
                dma(pairs), dma(pairs), dma(pairs), dma(pairs), dma(pairs), dma(pairs),
                dma(pairs), dma(pairs), dma(pairs), dma(pairs),
                dma((n,)), dma((n,)),
            ],
            compiler_params=pltpu.CompilerParams(
                collective_id=0, has_side_effects=True, vmem_limit_bytes=VMEM_LIMIT),
            name="xca_block",
        )(x_in, grad_y, ln_gain, ln_bias, w_qkv, w_out, temp_tau)
        return pl.pallas_call(
            functools.partial(finish_kernel, heads),
            out_shape=(
                jax.ShapeDtypeStruct(x_in.shape, BF16),
                jax.ShapeDtypeStruct(x_in.shape, BF16),
                jax.ShapeDtypeStruct((per_dev, 3 * dim), BF16),
                jax.ShapeDtypeStruct((per_dev, dim), BF16),
                jax.ShapeDtypeStruct((dim,), F32),
                jax.ShapeDtypeStruct((dim,), F32),
                jax.ShapeDtypeStruct((heads,), F32),
            ),
            in_specs=[any_spec] * 2 + [vmem] * 5,
            out_specs=(any_spec,) * 2 + (vmem,) * 5,
            scratch_shapes=[
                pltpu.VMEM((2 * rows // TOK, TOK, dim), BF16),
                dma((2 * rows // TOK,)), dma((2 * rows // TOK,)),
            ],
            name="finish",
        )(*out)

    tok = P("dp", "sp", None)
    return jax.shard_map(
        local_step, mesh=mesh,
        in_specs=(tok, tok, P(), P(), P(), P(), P()),
        out_specs=(tok, tok, P(("dp", "sp"), None), P(("dp", "sp"), None), P("dp"), P("dp"), P("dp")),
        check_vma=False)
```

```python
import functools

import jax
import jax.numpy as jnp
from jax import lax
from jax.experimental import pallas as pl
from jax.experimental.pallas import tpu as pltpu
from jax.sharding import PartitionSpec as P

LN_EPS = 1e-6
F32 = jnp.float32
BF16 = jnp.bfloat16
LANES = 128
TOK = 512
COLS = 256
VMEM_LIMIT = 67043328
NN = (((1,), (0,)), ((), ()))
NT = (((1,), (1,)), ((), ()))


def mm(a, b, dims=NN):
    return lax.dot_general(a, b, dims, preferred_element_type=F32)


def xca_kernel(
    n, heads,
    x_hbm, dy_hbm, gain_hbm, bias_hbm, wqkv_hbm, wo_hbm, tau_hbm,
    y_hbm, dx_hbm, dwqkv_hbm, dwo_hbm, dgain_hbm, dbias_hbm, dtau_hbm,
    dwqkv_ref, dwo_ref, dgain_ref, dbias_ref, dtau_ref, gain_ref, bias_ref, tau_ref, x_v, dy_v, w_v, wt_v, wo_v, ut, zt, dot_v, ot,
    sq_acc, gs_out, gs_mid, gs_in, gs_sum, a_all, ds_out, ds_mid, ds_in, g_all, c_all, bd, colq, colk, dgb, gb_all,
    part, r1, r2, r3,
    in_sem, out_sem, w_sem, d2d_s, d2d_r, p1_s, p1_r, p2_s, p2_r,
    gs_s, gs_r, a_s, a_r, ds_s, ds_r, g_s, g_r, c_s, c_r, gb_s, gb_r,
):
    images, tokens, dim = x_hbm.shape
    hd = dim // heads
    rows = images * tokens
    per_dev = dim // n
    chips = n // 2
    wheads = COLS // hd
    wrow = wheads * hd
    nwin = -(-heads // wheads)
    tiles = tokens // TOK
    o_chunks = dim // COLS
    chunks = 4 * o_chunks
    me = lax.axis_index("sp")
    chip, core = me // 2, me % 2
    right = ((chip + 1) % chips) * 2 + core
    left = ((chip + chips - 1) % chips) * 2 + core
    partner = chip * 2 + (1 - core)
    cr, cl, co = (chip + 1) % chips, (chip + chips - 1) % chips, (chip + 2) % chips

    peers = range(1, n)
    far_first = sorted(peers, key=lambda k: abs(2 * k - n))

    def rcopy(src, dst, ss, rs, dev):
        return pltpu.make_async_remote_copy(
            src_ref=src, dst_ref=dst, send_sem=ss, recv_sem=rs,
            device_id={"sp": dev}, device_id_type=pl.DeviceIdType.MESH)

    def cp_x(b, t):
        return pltpu.make_async_copy(x_hbm.at[b, pl.ds(t * TOK, TOK)], x_v.at[pl.ds(b * tokens + t * TOK, TOK)], in_sem.at[b * tiles + t])

    def cp_dy(b):
        return pltpu.make_async_copy(dy_hbm.at[b], dy_v.at[pl.ds(b * tokens, tokens)], in_sem.at[images * tiles + b])

    base = images * tiles + images
    cp_small = [pltpu.make_async_copy(h, v, in_sem.at[base + i]) for i, (h, v) in enumerate(
        ((gain_hbm, gain_ref), (bias_hbm, bias_ref), (tau_hbm, tau_ref)))]
    base += 3
    cp_wq, cp_wk, cp_wv = [pltpu.make_async_copy(wqkv_hbm.at[:, pl.ds(i * dim, dim)], w_v.at[:, pl.ds(i * dim, dim)], in_sem.at[base + i])
                           for i in range(3)]
    cp_wo = pltpu.make_async_copy(wo_hbm, wo_v, in_sem.at[base + 3])
    for c in cp_small:
        c.start()
    cp_x(0, 0).start()
    cp_wq.start()
    cp_x(0, 1).start()
    cp_wk.start()

    barrier = pltpu.get_barrier_semaphore()
    for k in peers:
        pl.semaphore_signal(barrier, inc=1, device_id={"sp": (me + k) % n},
                            device_id_type=pl.DeviceIdType.MESH)
    sq_acc[...] = jnp.zeros_like(sq_acc)
    bd[...] = jnp.zeros_like(bd)
    dgb[...] = jnp.zeros_like(dgb)
    for c in cp_small:
        c.wait()
    cp_x(0, 0).wait()

    def phase(f, *args):
        f(*args)

    def norm(xt):
        mean = jnp.sum(xt, axis=-1, keepdims=True) * (1.0 / dim)
        cen = xt - mean
        inv = lax.rsqrt(jnp.sum(cen * cen, axis=-1, keepdims=True) * (1.0 / dim) + LN_EPS)
        return cen * inv, inv

    gain_row = gain_ref[...].reshape(1, dim)
    bias_row = bias_ref[...].reshape(1, dim)

    def norm_rows(r0, count):
        x_hat, _inv = norm(x_v[pl.ds(r0, count), :].astype(F32))
        ut[:, pl.ds(r0, count)] = (x_hat * gain_row + bias_row).astype(BF16).T

    def transpose_w(c0, count):
        def body(i, _):
            off = pl.multiple_of(c0 + i * COLS, COLS)
            wt_v[pl.ds(off, COLS), :] = w_v[:, pl.ds(off, COLS)].T
            return 0
        lax.fori_loop(0, count // COLS, body, 0)

    other_chips = range(1, chips)

    def pair_sum(out, mid, ss, rs, b):
        return rcopy(out.at[b, 1 - core], mid.at[b], ss.at[0], rs.at[b, 0], partner)

    def chip_copy(out, into, ss, rs, b, k):
        to = (chip + k) % chips
        return rcopy(out.at[b, core, to], into.at[b, k], ss.at[1], rs.at[b, k], to * 2 + core)

    def scatter_state(out, mid, into, ss, rs, b):
        pair_sum(out, mid, ss, rs, b).wait_recv()
        out[b, core] += mid[b]
        for k in (2, 1, 3):
            chip_copy(out, into, ss, rs, b, k).start()

    def state_total(out, into, ss, rs, b):
        tot = out[b, core, chip]
        for k in other_chips:
            tot = tot + into[b, k]
        return tot

    lane_w = lax.broadcasted_iota(jnp.int32, (hd, LANES), 1)

    def to_pairs(blocks, out_ref, extra=None):
        for d in range(n):
            picked = []
            for s in range(2):
                w, k = divmod(2 * d + s, wheads)
                strip = blocks[w][k * hd:(k + 1) * hd, :]
                shift = (s * hd - k * hd) % COLS
                if shift:
                    strip = pltpu.roll(strip, shift, 1)
                picked.append(strip[:, :LANES])
            rest = 0.0
            if extra is not None:
                for i, col in enumerate(extra):
                    for s in range(2):
                        r0 = (2 * d + s) * hd
                        rest = jnp.where(lane_w == 2 * hd + 2 * i + s, col[r0:r0 + hd], rest)
            out_ref[d % 2, d // 2] = jnp.where(lane_w < hd, picked[0], jnp.where(lane_w < 2 * hd, picked[1], rest))

    def gram(b, l_ref, l0, r_ref, r0):
        blocks = []
        for w in range(nwin):
            m = min(wrow, dim - w * wrow)
            lo, ro = l0 + w * wrow, r0 + w * wrow
            nw = min(COLS, dim - w * wrow)
            left_op = l_ref[lo:lo + m, b * tokens:(b + 1) * tokens]
            right_op = r_ref[ro:ro + nw, b * tokens:(b + 1) * tokens]
            g = mm(left_op, right_op, NT)
            if nw < COLS:
                g = jnp.pad(g, ((0, 0), (0, COLS - nw)))
            blocks.append(g)
        return blocks

    def qk_tile(off, following, wt_cols=None):
        if wt_cols == dim:
            wt_v[dim:2 * dim, :] = w_v[:, dim:2 * dim].T
        for m in range(2):
            z = mm(wt_v[m * dim:(m + 1) * dim, :], ut[:, pl.ds(off, TOK)]).astype(BF16)
            zt[m * dim:(m + 1) * dim, pl.ds(off, TOK)] = z
            zf = z.astype(F32)
            sq = zf * zf
            tot = sq[:, 0:LANES]
            for j in range(1, TOK // LANES):
                tot = tot + sq[:, j * LANES:(j + 1) * LANES]
            sq_acc[off // tokens, m * dim:(m + 1) * dim] += tot
        if following is not None:
            norm_rows(following, TOK)
        if wt_cols is not None and wt_cols > dim:
            wt_v[wt_cols:wt_cols + dim // 2, :] = w_v[:, wt_cols:wt_cols + dim // 2].T

    def send_gram(b):
        cols = [jnp.sum(sq_acc[b, m * dim:(m + 1) * dim], axis=1, keepdims=True) for m in range(2)]
        to_pairs(gram(b, zt, 0, zt, dim), gs_out.at[b], cols)
        if b == 0:
            pl.semaphore_wait(barrier, n - 1)
        pair_sum(gs_out, gs_mid, gs_s, gs_r, b).start()

    for b in range(1, images):
        for t in range(tiles):
            cp_x(b, t).start()
    phase(norm_rows, 0, TOK)
    cp_wq.wait()
    cp_wv.start()
    cp_wo.start()
    for b in range(images):
        cp_dy(b).start()
    transpose_w(0, dim)
    cp_x(0, 1).wait()
    cp_wk.wait()
    phase(qk_tile, 0, TOK, dim)
    for t in range(tiles):
        cp_x(1, t).wait()
    for t in range(1, tiles):
        phase(qk_tile, t * TOK, (t + 1) * TOK)
    phase(send_gram, 0)
    cp_wv.wait()
    for t in range(tiles):
        if t == 1:
            phase(scatter_state, gs_out, gs_mid, gs_in, gs_s, gs_r, 0)
        off = tokens + t * TOK
        phase(qk_tile, off, off + TOK if t + 1 < tiles else None, 2 * dim + t * dim // tiles)
    phase(send_gram, 1)

    def values(b):
        for t in range(tiles):
            tok_t = pl.ds(b * tokens + t * TOK, TOK)
            zt[2 * dim:3 * dim, tok_t] = mm(wt_v[2 * dim:3 * dim, :], ut[:, tok_t]).astype(BF16)

    eye = lax.broadcasted_iota(jnp.int32, (hd, hd), 0) == lax.broadcasted_iota(jnp.int32, (hd, hd), 1)

    def row_of(col):
        return jnp.sum(jnp.where(eye, col, 0.0), axis=0, keepdims=True)

    head_lane = lax.broadcasted_iota(jnp.int32, (1, heads), 1)
    tau_row = tau_ref[...].reshape(1, heads)

    def attn_state(b, s):
        blk = gs_sum[b]
        g = blk[:, s * hd:(s + 1) * hd]
        qc = blk[:, 2 * hd + s:2 * hd + s + 1]
        kr = row_of(blk[:, 2 * hd + 2 + s:2 * hd + 3 + s])
        unit = lax.rsqrt(qc) * lax.rsqrt(kr)
        tau = jnp.sum(jnp.where(head_lane == me * 2 + s, tau_row, 0.0), axis=1, keepdims=True)
        cosine = g * unit
        logits = tau * cosine
        e = jnp.exp(logits - jnp.max(logits, axis=-1, keepdims=True))
        probs = e / jnp.sum(e, axis=-1, keepdims=True)
        return cosine, logits, probs, tau * unit, qc, kr

    def pair(a0, a1):
        r = a0.shape[0]
        z = jnp.zeros((r, LANES - 2 * hd), a0.dtype)
        return jnp.concatenate([a0, a1, z], axis=1)

    def owner_forward(b):
        for k in other_chips:
            chip_copy(gs_out, gs_in, gs_s, gs_r, b, k).wait_recv()
        gs_sum[b] = state_total(gs_out, gs_in, gs_s, gs_r, b)
        p0 = attn_state(b, 0)[2]
        p1 = attn_state(b, 1)[2]
        a_all[b, me] = pair(p0, p1).astype(BF16)
        for k in far_first:
            dst = (me + k) % n
            rcopy(a_all.at[b, me], a_all.at[b, me], a_s.at[0], a_r.at[b, k], dst).start()

    def owner_backward():
        for b in range(images):
            for k in other_chips:
                chip_copy(ds_out, ds_in, ds_s, ds_r, b, k).wait_recv()
        sub = lax.broadcasted_iota(jnp.int32, (8, LANES), 0)
        lane = lax.broadcasted_iota(jnp.int32, (8, LANES), 1)
        for b in range(images):
            tot = state_total(ds_out, ds_in, ds_s, ds_r, b).astype(BF16).astype(F32)
            gs, qs, ks, ts = [], [], [], []
            for s in range(2):
                cosine, logits, probs, scale, qc, kr = attn_state(b, s)
                dp = tot[:, s * hd:(s + 1) * hd]
                gl = probs * (dp - jnp.sum(probs * dp, axis=-1, keepdims=True))
                weighted = gl * logits
                gs.append(gl * scale)
                qs.append(row_of(-jnp.sum(weighted, axis=1, keepdims=True) / qc))
                ks.append(-jnp.sum(weighted, axis=0, keepdims=True) / kr)
                ts.append(jnp.sum(jnp.sum(gl * cosine, axis=1, keepdims=True), axis=0, keepdims=True))
            g_all[b, me] = pair(gs[0], gs[1]).astype(BF16)
            taus = jnp.where(lane == 0, ts[0], jnp.where(lane == 1, ts[1], 0.0))
            c_all[b, me] = jnp.where(sub == 0, pair(qs[0], qs[1]), jnp.where(sub == 1, pair(ks[0], ks[1]), jnp.where(sub == 2, taus, 0.0)))
        for b in range(images):
            for ref, ss, rs in states:
                for k in (4, 2, 6, 1):
                    dst = (me + k) % n if k > 1 else partner
                    rcopy(ref.at[b, me], ref.at[b, me], ss.at[0], rs.at[b, k], dst).start()

    states = ((g_all, g_s, g_r), (c_all, c_s, c_r))

    def pass_on(b):
        for ref, ss, rs in states:
            for k in (2, 6, 4):
                src = (me + n - k) % n
                rcopy(ref.at[b, me], ref.at[b, src], ss.at[0], rs.at[b, k], me).wait_recv()
                rcopy(ref.at[b, src], ref.at[b, src], ss.at[0], rs.at[b, k + 1], partner).start()

    def passed(b):
        for ref, ss, rs in states:
            rcopy(ref.at[b, me], ref.at[b, partner], ss.at[0], rs.at[b, 1], me).wait_recv()
            for k in (2, 6, 4):
                src = (partner + n - k) % n
                rcopy(ref.at[b, me], ref.at[b, src], ss.at[0], rs.at[b, k + 1], me).wait_recv()

    def gathered(ref, ss, rs, b):
        for k in peers:
            src = (me + n - k) % n
            rcopy(ref.at[b, me], ref.at[b, src], ss.at[0], rs.at[b, k], me).wait_recv()

    def grad_heads(b):
        cp_dy(b).wait()
        if b == 0:
            cp_wo.wait()

        for t in range(tiles):
            tok_t = pl.ds(b * tokens + t * TOK, TOK)
            dot_v[:, tok_t] = mm(wo_v[...], dy_v[tok_t, :], NT).astype(BF16)

    def send_dprobs(b):
        to_pairs(gram(b, dot_v, 0, zt, 2 * dim), ds_out.at[b])
        pair_sum(ds_out, ds_mid, ds_s, ds_r, b).start()

    sj = lax.broadcasted_iota(jnp.int32, (LANES, COLS), 0)
    slane = lax.broadcasted_iota(jnp.int32, (LANES, COLS), 1)
    sels = []
    for s in range(2):
        hit = jnp.zeros((LANES, COLS), jnp.bool_)
        for k in range(wheads):
            hit = jnp.logical_or(hit, slane - k * hd == sj - s * hd)
        hit = jnp.logical_and(hit, jnp.logical_and(sj >= s * hd, sj < (s + 1) * hd))
        sels.append(jnp.where(hit, 1.0, 0.0).astype(BF16))
    blane = lax.broadcasted_iota(jnp.int32, (hd, COLS), 1)

    def build(ref, b):
        flat = ref[b].reshape(n * hd, LANES)
        for s in range(2):
            spread = mm(flat, sels[s])
            for d in range(n):
                w, k = divmod(2 * d + s, wheads)
                blk = jnp.where(jnp.logical_and(blane >= k * hd, blane < (k + 1) * hd), spread[d * hd:(d + 1) * hd], 0.0)
                bd[b, w, 0, k * hd:(k + 1) * hd, :] = blk.astype(BF16)
        for w in range(nwin):
            bd[b, w, 1] = bd[b, w, 0].T

    def windows():
        for w in range(nwin):
            r0 = w * wrow
            yield w, r0, min(wrow, dim - r0), min(COLS, dim - r0)

    def heads_out(b):
        for t in range(tiles):
            tok_t = pl.ds(b * tokens + t * TOK, TOK)
            for w, r0, m, kk in windows():
                ot[r0:r0 + m, tok_t] = mm(bd[b, w, 0, 0:m, 0:kk], zt[2 * dim + r0:2 * dim + r0 + kk, tok_t]).astype(BF16)

    def grad_values(b):
        def body(t, _):
            off = pl.multiple_of(b * tokens + t * TOK, TOK)
            for w, r0, m, kk in windows():
                zt[2 * dim + r0:2 * dim + r0 + m, pl.ds(off, TOK)] = mm(bd[b, w, 1, 0:m, 0:kk], dot_v[r0:r0 + kk, pl.ds(off, TOK)]).astype(BF16)
            return 0
        lax.fori_loop(0, tiles, body, 0)

    def dq_and_dk(b):
        ct = c_all[b].reshape(n * 8, LANES).T
        for d in range(n):
            colq[d * per_dev:(d + 1) * per_dev, :] = jnp.broadcast_to(ct[0:per_dev, 8 * d:8 * d + 1], (per_dev, LANES))
            colk[d * per_dev:(d + 1) * per_dev, :] = jnp.broadcast_to(ct[0:per_dev, 8 * d + 1:8 * d + 2], (per_dev, LANES))

        def body(t, _):
            off = pl.multiple_of(b * tokens + t * TOK, TOK)
            for w, r0, m, kk in windows():
                qw = zt[r0:r0 + kk, pl.ds(off, TOK)]
                kw = zt[dim + r0:dim + r0 + kk, pl.ds(off, TOK)]
                cq = jnp.concatenate([colq[r0:r0 + m, :]] * (TOK // LANES), axis=1)
                ck = jnp.concatenate([colk[r0:r0 + m, :]] * (TOK // LANES), axis=1)
                dq = mm(bd[b, w, 0, 0:m, 0:kk], kw) + cq * qw[0:m].astype(F32)
                dk = mm(bd[b, w, 1, 0:m, 0:kk], qw) + ck * kw[0:m].astype(F32)
                zt[r0:r0 + m, pl.ds(off, TOK)] = dq.astype(BF16)
                zt[dim + r0:dim + r0 + m, pl.ds(off, TOK)] = dk.astype(BF16)
            return 0
        lax.fori_loop(0, tiles, body, 0)

    def put_part(c, val):
        for j in range(n):
            part[c, j % 2, j // 2] = val[j * per_dev:(j + 1) * per_dev, :]

    def d2d(c):
        return rcopy(part.at[c, 1 - core], r1.at[c], d2d_s.at[0], d2d_r.at[c], partner)

    half = per_dev // 2

    def hop1(c):
        return (rcopy(r1.at[c, co, pl.ds(0, half)], r2.at[c, 0], p1_s.at[0], p1_r.at[c, 0], right),
                rcopy(r1.at[c, co, pl.ds(half, half)], r2.at[c, 1], p1_s.at[0], p1_r.at[c, 1], left))

    def hop2(c):
        return (rcopy(r1.at[c, cr], r3.at[c, 0], p2_s.at[0], p2_r.at[c, 0], right),
                rcopy(r1.at[c, cl], r3.at[c, 1], p2_s.at[0], p2_r.at[c, 1], left))

    def serve1(c):
        d2d(c).wait_recv()
        for blk in (co, cr, cl, chip):
            r1[c, blk] += part[c, core, blk]
        for h in hop1(c):
            h.start()

    def serve2(c):
        for h in hop1(c):
            h.wait_recv()
        r1[c, cr, 0:half] += r2[c, 0]
        r1[c, cl, half:per_dev] += r2[c, 1]
        for h in hop2(c):
            h.start()

    def serve3(c):
        for h in hop2(c):
            h.wait_recv()
        return (r1[c, chip] + r3[c, 0] + r3[c, 1]).astype(BF16)

    def wo_chunk(c):
        off = pl.multiple_of(c * COLS, COLS)
        put_part(c, mm(ot[...], dy_v[:, pl.ds(off, COLS)]))
        d2d(c).start()

    def qkv_chunk(c, base):
        off = pl.multiple_of(base + c * COLS, COLS)
        put_part(c, mm(ut[...], zt[pl.ds(off, COLS), :], NT))
        d2d(c).start()

    phase(values, 0)
    phase(scatter_state, gs_out, gs_mid, gs_in, gs_s, gs_r, 1)
    phase(grad_heads, 0)
    phase(owner_forward, 0)
    phase(send_dprobs, 0)
    phase(values, 1)
    phase(scatter_state, ds_out, ds_mid, ds_in, ds_s, ds_r, 0)
    phase(owner_forward, 1)
    phase(grad_heads, 1)
    phase(send_dprobs, 1)
    gathered(a_all, a_s, a_r, 0)
    phase(build, a_all, 0)
    phase(heads_out, 0)
    phase(scatter_state, ds_out, ds_mid, ds_in, ds_s, ds_r, 1)
    gathered(a_all, a_s, a_r, 1)
    phase(build, a_all, 1)
    phase(heads_out, 1)

    def wo_loop(c, _):
        wo_chunk(c)

        @pl.when(c > 0)
        def _():
            serve1(c - 1)
        return 0
    lax.fori_loop(0, o_chunks, wo_loop, 0)
    phase(owner_backward)
    serve1(o_chunks - 1)
    grad_values(0)
    grad_values(1)
    v0 = 2 * dim - o_chunks * COLS
    qkv_chunk(o_chunks, v0)

    def s2_body(c, _):
        serve2(c)
        return 0

    def serve2_range(c0, c1):
        lax.fori_loop(c0, c1, s2_body, 0)

    serve2_range(0, 2)

    def v_loop(c, _):
        qkv_chunk(c, v0)
        serve1(c - 1)
        return 0
    lax.fori_loop(o_chunks + 1, 2 * o_chunks, v_loop, 0)
    for b in range(images):
        pass_on(b)
    serve2_range(2, 3)
    for b in range(images):
        passed(b)
        phase(build, g_all, b)
        dq_and_dk(b)
        if b == 0:
            serve1(2 * o_chunks - 1)
    serve2_range(3, 4)
    qkv_chunk(2 * o_chunks, -2 * o_chunks * COLS)

    def qk_loop(c, _):
        qkv_chunk(c, -2 * o_chunks * COLS)
        serve1(c - 1)
        return 0
    lax.fori_loop(2 * o_chunks + 1, chunks, qk_loop, 0)
    serve1(chunks - 1)
    serve2_range(4, chunks - 3)

    def tile_copy(i, t):
        rows_t = pl.ds(pl.multiple_of(t * TOK, TOK), TOK)
        src, dst = ((x_v, y_hbm), (dy_v, dx_hbm))[i]
        return pltpu.make_async_copy(src.at[rows_t], dst.at[rows_t], out_sem.at[i])

    def dx_body(t, _):
        off = pl.multiple_of(t * TOK, TOK)
        dot_v[:, pl.ds(off, TOK)] = mm(w_v[...], zt[:, pl.ds(off, TOK)]).astype(BF16)

        def piece(i, _):
            r = pl.ds(pl.multiple_of(off + i * LANES, LANES), LANES)
            du = dot_v[:, r].T.astype(F32)
            xt = x_v[r, :].astype(F32)
            x_v[r, :] = (xt + mm(ot[:, r].T, wo_v[...])).astype(BF16)
            x_hat, inv = norm(xt)
            prod = du * x_hat
            dgb[0] += jnp.sum(prod.reshape(LANES // 8, 8, dim), axis=0)
            dgb[1] += jnp.sum(du.reshape(LANES // 8, 8, dim), axis=0)
            a9 = du * gain_row
            m1 = jnp.sum(a9, axis=-1, keepdims=True) * (1.0 / dim)
            m2 = jnp.sum(a9 * x_hat, axis=-1, keepdims=True) * (1.0 / dim)
            gx = inv * (a9 - m1 - x_hat * m2)
            dy_v[r, :] = (dy_v[r, :].astype(F32) + gx).astype(BF16)
            return 0
        lax.fori_loop(0, TOK // LANES, piece, 0)
        tile_copy(0, t).start()
        tile_copy(1, t).start()
        return 0

    lax.fori_loop(0, 1, dx_body, 0)
    serve2_range(chunks - 3, chunks)
    lax.fori_loop(1, images * tiles, dx_body, 0)
    gb_all[me] = jnp.concatenate([jnp.sum(dgb[i], axis=0).reshape(dim // LANES, LANES) for i in range(2)], axis=0)
    for k in far_first:
        rcopy(gb_all.at[me], gb_all.at[me], gb_s.at[0], gb_r.at[k], (me + k) % n).start()

    lane = lax.broadcasted_iota(jnp.int32, (1, LANES), 1)
    dtau = jnp.zeros((1, LANES), F32)
    for d in range(n):
        row = c_all[0, d, 2:3, :]
        for b in range(1, images):
            row = row + c_all[b, d, 2:3, :]
        if d:
            row = pltpu.roll(row, 2 * d, 1)
        dtau = jnp.where(jnp.logical_and(lane >= 2 * d, lane < 2 * d + 2), row, dtau)
    dtau_ref[...] = dtau

    def chunk_copy(c, src, dst, base, which):
        cols = pl.ds(pl.multiple_of(base + c * COLS, COLS), COLS)
        return pltpu.make_async_copy(src.at[:, cols], dst.at[:, cols], w_sem.at[which])

    def finish_chunks(c0, c1, src, dst, base, which):
        def body(c, _):
            src[:, pl.ds(pl.multiple_of(base + c * COLS, COLS), COLS)] = serve3(c)
            chunk_copy(c, src, dst, base, which).start()
            return 0
        lax.fori_loop(c0, c1, body, 0)

    finish_chunks(0, o_chunks, dwo_ref, dwo_hbm, 0, 0)
    finish_chunks(o_chunks, 2 * o_chunks, dwqkv_ref, dwqkv_hbm, v0, 1)

    for k in peers:
        src = (me + n - k) % n
        rcopy(gb_all.at[me], gb_all.at[src], gb_s.at[0], gb_r.at[k], me).wait_recv()
    tot = gb_all[0]
    for d in peers:
        tot = tot + gb_all[d]
    dgain_ref[...] = tot[:dim // LANES]
    dbias_ref[...] = tot[dim // LANES:]
    small_copies = [pltpu.make_async_copy(v, h, w_sem.at[2 + i]) for i, (v, h) in enumerate(
        ((dgain_ref, dgain_hbm), (dbias_ref, dbias_hbm), (dtau_ref, dtau_hbm)))]
    for c in small_copies:
        c.start()
    finish_chunks(2 * o_chunks, chunks, dwqkv_ref, dwqkv_hbm, -2 * o_chunks * COLS, 1)

    sent = (
        (gs_mid, gs_s, 0), (gs_in.at[:, pl.ds(1, chips - 1)], gs_s, 1),
        (ds_mid, ds_s, 0), (ds_in.at[:, pl.ds(1, chips - 1)], ds_s, 1),
        (a_all.at[:, pl.ds(0, n - 1)], a_s, 0), (g_all.at[:, pl.ds(0, n - 1)], g_s, 0), (c_all.at[:, pl.ds(0, n - 1)], c_s, 0),
        (gb_all.at[pl.ds(0, n - 1)], gb_s, 0), (r1, d2d_s, 0), (r2, p1_s, 0), (r3, p2_s, 0))
    for ref, sem, i in sent:
        rcopy(ref, ref, sem.at[i], gb_r.at[0], partner).wait_send()
    pltpu.make_async_copy(x_v, y_hbm, out_sem.at[0]).wait()
    pltpu.make_async_copy(dy_v, dx_hbm, out_sem.at[1]).wait()
    for c in small_copies:
        c.wait()
    pltpu.make_async_copy(dwo_ref, dwo_hbm, w_sem.at[0]).wait()
    pltpu.make_async_copy(dwqkv_ref, dwqkv_hbm, w_sem.at[1]).wait()


def finish_kernel(heads, y_hbm, dx_hbm, *refs):
    moved, outputs, (buf, *stage, sem_in, sem_out) = refs[:5], refs[5:12], refs[12:]
    landed, shaped = stage[:5], stage[:2] + stage[5:]
    images, tokens, _dim = outputs[0].shape
    parts = tokens // TOK
    ins, outs = [], []

    def copy(src, dst, sem, into):
        into.append(pltpu.make_async_copy(src, dst, sem.at[len(into)]))

    for src, dst in ((y_hbm, outputs[0]), (dx_hbm, outputs[1])):
        for b in range(images):
            for t in range(parts):
                slot = buf.at[len(ins)]
                copy(src.at[pl.ds((b * parts + t) * TOK, TOK)], slot, sem_in, ins)
                copy(slot, dst.at[b, pl.ds(t * TOK, TOK)], sem_out, outs)
    big = len(ins)
    for src, mid, last, dst in zip(moved, landed, shaped, outputs[2:]):
        copy(src, mid, sem_in, ins)
        copy(last, dst, sem_out, outs)
    for c in ins:
        c.start()
    for c in ins[big:]:
        c.wait()
    for mid, last in zip(landed[2:], shaped[2:]):
        last[...] = mid[...].reshape(mid.size)[:last.shape[0]]
    for o in outs[big:]:
        o.start()
    for c, o in zip(ins[:big], outs[:big]):
        c.wait()
        o.start()
    for o in outs:
        o.wait()


def solution(mesh):
    n = mesh.shape["sp"]

    def local_step(x_in, grad_y, ln_gain, ln_bias, w_qkv, w_out, temp_tau):
        images, tokens, dim = x_in.shape
        heads = temp_tau.shape[0]
        hd = dim // heads
        rows = images * tokens
        per_dev = dim // n
        chunks = 4 * dim // COLS
        nwin = -(-heads // (COLS // hd))
        any_spec = pl.BlockSpec(memory_space=pl.ANY)
        dma = pltpu.SemaphoreType.DMA
        pairs = (images, n)
        one, by_chip = dma((1,)), dma((images, n // 2))
        out = pl.pallas_call(
            functools.partial(xca_kernel, n, heads),
            out_shape=(
                jax.ShapeDtypeStruct((rows, dim), BF16),
                jax.ShapeDtypeStruct((rows, dim), BF16),
                jax.ShapeDtypeStruct((per_dev, 3 * dim), BF16),
                jax.ShapeDtypeStruct((per_dev, dim), BF16),
                jax.ShapeDtypeStruct((dim // LANES, LANES), F32),
                jax.ShapeDtypeStruct((dim // LANES, LANES), F32),
                jax.ShapeDtypeStruct((1, LANES), F32),
            ),
            in_specs=[any_spec] * 7,
            out_specs=(any_spec,) * 7,
            scratch_shapes=[
                pltpu.VMEM((per_dev, 3 * dim), BF16),
                pltpu.VMEM((per_dev, dim), BF16),
                pltpu.VMEM((dim // LANES, LANES), F32),
                pltpu.VMEM((dim // LANES, LANES), F32),
                pltpu.VMEM((1, LANES), F32),
                pltpu.VMEM((dim,), F32),
                pltpu.VMEM((dim,), F32),
                pltpu.VMEM((heads,), F32),
                pltpu.VMEM((rows, dim), BF16),
                pltpu.VMEM((rows, dim), BF16),
                pltpu.VMEM((dim, 3 * dim), BF16),
                pltpu.VMEM((3 * dim, dim), BF16),
                pltpu.VMEM((dim, dim), BF16),
                pltpu.VMEM((dim, rows), BF16),
                pltpu.VMEM((3 * dim, rows), BF16),
                pltpu.VMEM((dim, rows), BF16),
                pltpu.VMEM((dim, rows), BF16),
                pltpu.VMEM((images, 2 * dim, LANES), F32),
                pltpu.VMEM((images, 2, n // 2, hd, LANES), F32),
                pltpu.VMEM((images, n // 2, hd, LANES), F32),
                pltpu.VMEM((images, n // 2, hd, LANES), F32),
                pltpu.VMEM((images, hd, LANES), F32),
                pltpu.VMEM((images, n, hd, LANES), BF16),
                pltpu.VMEM((images, 2, n // 2, hd, LANES), F32),
                pltpu.VMEM((images, n // 2, hd, LANES), F32),
                pltpu.VMEM((images, n // 2, hd, LANES), F32),
                pltpu.VMEM((images, n, hd, LANES), BF16),
                pltpu.VMEM((images, n, 8, LANES), F32),
                pltpu.VMEM((images, nwin, 2, COLS, COLS), BF16),
                pltpu.VMEM((dim, LANES), F32),
                pltpu.VMEM((dim, LANES), F32),
                pltpu.VMEM((2, 8, dim), F32),
                pltpu.VMEM((n, 2 * dim // LANES, LANES), F32),
                pltpu.VMEM((chunks, 2, n // 2, per_dev, COLS), F32),
                pltpu.VMEM((chunks, n // 2, per_dev, COLS), F32),
                pltpu.VMEM((chunks, 2, per_dev // 2, COLS), F32),
                pltpu.VMEM((chunks, 2, per_dev, COLS), F32),
                dma((rows // TOK + images + 7,)), dma((2,)), dma((5,)),
                one, dma((chunks,)), one, dma((chunks, 2)), one, dma((chunks, 2)),
                dma((2,)), by_chip, one, dma(pairs), dma((2,)), by_chip,
                one, dma(pairs), one, dma(pairs), one, dma((n,)),
            ],
            compiler_params=pltpu.CompilerParams(
                collective_id=0, has_side_effects=True, vmem_limit_bytes=VMEM_LIMIT),
            name="xca_block",
        )(x_in, grad_y, ln_gain, ln_bias, w_qkv, w_out, temp_tau)
        return pl.pallas_call(
            functools.partial(finish_kernel, heads),
            out_shape=(
                jax.ShapeDtypeStruct(x_in.shape, BF16),
                jax.ShapeDtypeStruct(x_in.shape, BF16),
                jax.ShapeDtypeStruct((per_dev, 3 * dim), BF16),
                jax.ShapeDtypeStruct((per_dev, dim), BF16),
                jax.ShapeDtypeStruct((dim,), F32),
                jax.ShapeDtypeStruct((dim,), F32),
                jax.ShapeDtypeStruct((heads,), F32),
            ),
            in_specs=[any_spec] * 7,
            out_specs=(any_spec,) * 7,
            scratch_shapes=[
                pltpu.VMEM((2 * rows // TOK, TOK, dim), BF16),
                pltpu.VMEM((per_dev, 3 * dim), BF16),
                pltpu.VMEM((per_dev, dim), BF16),
                pltpu.VMEM((dim // LANES, LANES), F32),
                pltpu.VMEM((dim // LANES, LANES), F32),
                pltpu.VMEM((1, LANES), F32),
                pltpu.VMEM((dim,), F32),
                pltpu.VMEM((dim,), F32),
                pltpu.VMEM((heads,), F32),
                dma((2 * rows // TOK + 5,)), dma((2 * rows // TOK + 5,)),
            ],
            name="finish",
        )(*out)

    tok = P("dp", "sp", None)
    return jax.shard_map(
        local_step, mesh=mesh,
        in_specs=(tok, tok, P(), P(), P(), P(), P()),
        out_specs=(tok, tok, P(("dp", "sp"), None), P(("dp", "sp"), None), P("dp"), P("dp"), P("dp")),
        check_vma=False)
```

```python
import functools

import jax
import jax.numpy as jnp
from jax import lax
from jax.experimental import pallas as pl
from jax.experimental.pallas import tpu as pltpu
from jax.sharding import PartitionSpec as P

LN_EPS = 1e-6
F32 = jnp.float32
BF16 = jnp.bfloat16
LANES = 128
TOK = 512
COLS = 256
VMEM_LIMIT = 67043328
NN = (((1,), (0,)), ((), ()))
NT = (((1,), (1,)), ((), ()))


def mm(a, b, dims=NN):
    return lax.dot_general(a, b, dims, preferred_element_type=F32)


def xca_kernel(
    n, heads,
    x_hbm, dy_hbm, gain_hbm, bias_hbm, wqkv_hbm, wo_hbm, tau_hbm,
    y_hbm, dx_hbm, dwqkv_hbm, dwo_hbm, dgain_hbm, dbias_hbm, dtau_hbm,
    dwqkv_ref, dwo_ref, dgain_ref, dbias_ref, dtau_ref, gain_ref, bias_ref, tau_ref, x_v, dy_v, w_v, wt_v, wo_v, ut, zt, dot_v, ot,
    sq_acc, gs_out, gs_mid, gs_in, gs_sum, a_all, ds_out, ds_mid, ds_in, g_all, c_all, bd, colq, colk, dgb, gb_all,
    part, r1, r2, r3,
    in_sem, out_sem, w_sem, d2d_s, d2d_r, p1_s, p1_r, p2_s, p2_r,
    gs_s, gs_r, a_s, a_r, ds_s, ds_r, g_s, g_r, c_s, c_r, gb_s, gb_r,
):
    images, tokens, dim = x_hbm.shape
    hd = dim // heads
    rows = images * tokens
    per_dev = dim // n
    chips = n // 2
    wheads = COLS // hd
    wrow = wheads * hd
    nwin = -(-heads // wheads)
    tiles = tokens // TOK
    o_chunks = dim // COLS
    chunks = 4 * o_chunks
    me = lax.axis_index("sp")
    chip, core = me // 2, me % 2
    right = ((chip + 1) % chips) * 2 + core
    left = ((chip + chips - 1) % chips) * 2 + core
    partner = chip * 2 + (1 - core)
    cr, cl, co = (chip + 1) % chips, (chip + chips - 1) % chips, (chip + 2) % chips

    peers = range(1, n)
    most = pl.ds(0, n - 1)
    far_first = sorted(peers, key=lambda k: abs(2 * k - n))

    def rcopy(src, dst, ss, rs, dev):
        return pltpu.make_async_remote_copy(
            src_ref=src, dst_ref=dst, send_sem=ss, recv_sem=rs,
            device_id={"sp": dev}, device_id_type=pl.DeviceIdType.MESH)

    def cp_x(b, t):
        return pltpu.make_async_copy(x_hbm.at[b, pl.ds(t * TOK, TOK)], x_v.at[pl.ds(b * tokens + t * TOK, TOK)], in_sem.at[b * tiles + t])

    def cp_dy(b):
        return pltpu.make_async_copy(dy_hbm.at[b], dy_v.at[pl.ds(b * tokens, tokens)], in_sem.at[images * tiles + b])

    base = images * tiles + images
    cp_small = [pltpu.make_async_copy(h, v, in_sem.at[base + i]) for i, (h, v) in enumerate(
        ((gain_hbm, gain_ref), (bias_hbm, bias_ref), (tau_hbm, tau_ref)))]
    base += 3
    cp_wq, cp_wk, cp_wv = [pltpu.make_async_copy(wqkv_hbm.at[:, pl.ds(i * dim, dim)], w_v.at[:, pl.ds(i * dim, dim)], in_sem.at[base + i])
                           for i in range(3)]
    cp_wo = pltpu.make_async_copy(wo_hbm, wo_v, in_sem.at[base + 3])
    for c in cp_small:
        c.start()
    cp_x(0, 0).start()
    cp_wq.start()
    cp_x(0, 1).start()
    cp_wk.start()

    barrier = pltpu.get_barrier_semaphore()
    for k in peers:
        pl.semaphore_signal(barrier, inc=1, device_id={"sp": (me + k) % n},
                            device_id_type=pl.DeviceIdType.MESH)
    sq_acc[...] = jnp.zeros_like(sq_acc)
    bd[...] = jnp.zeros_like(bd)
    dgb[...] = jnp.zeros_like(dgb)
    for c in cp_small:
        c.wait()
    cp_x(0, 0).wait()

    def phase(f, *args):
        f(*args)

    def norm(xt):
        mean = jnp.sum(xt, axis=-1, keepdims=True) * (1.0 / dim)
        cen = xt - mean
        inv = lax.rsqrt(jnp.sum(cen * cen, axis=-1, keepdims=True) * (1.0 / dim) + LN_EPS)
        return cen * inv, inv

    gain_row = gain_ref[...].reshape(1, dim)
    bias_row = bias_ref[...].reshape(1, dim)

    def norm_rows(r0, count):
        x_hat, _inv = norm(x_v[pl.ds(r0, count), :].astype(F32))
        ut[:, pl.ds(r0, count)] = (x_hat * gain_row + bias_row).astype(BF16).T

    def transpose_w(c0, count):
        def body(i, _):
            off = pl.multiple_of(c0 + i * COLS, COLS)
            wt_v[pl.ds(off, COLS), :] = w_v[:, pl.ds(off, COLS)].T
            return 0
        lax.fori_loop(0, count // COLS, body, 0)

    other_chips = range(1, chips)
    others = pl.ds(1, chips - 1)

    def pair_sum(out, mid, ss, rs, b):
        return rcopy(out.at[b, 1 - core], mid.at[b], ss.at[0], rs.at[b, 0], partner)

    def chip_copy(out, into, ss, rs, b, k):
        to = (chip + k) % chips
        return rcopy(out.at[b, core, to], into.at[b, k], ss.at[1], rs.at[b, 1], to * 2 + core)

    def chips_in(into, ss, rs, b):
        got = into.at[b, others]
        rcopy(got, got, ss.at[1], rs.at[b, 1], partner).wait_recv()

    def scatter_state(out, mid, into, ss, rs, b):
        pair_sum(out, mid, ss, rs, b).wait_recv()
        out[b, core] += mid[b]
        for k in (2, 1, 3):
            chip_copy(out, into, ss, rs, b, k).start()

    def state_total(out, into, ss, rs, b):
        tot = out[b, core, chip]
        for k in other_chips:
            tot = tot + into[b, k]
        return tot

    lane_w = lax.broadcasted_iota(jnp.int32, (hd, LANES), 1)

    def to_pairs(blocks, out_ref, extra=None):
        for d in range(n):
            picked = []
            for s in range(2):
                w, k = divmod(2 * d + s, wheads)
                strip = blocks[w][k * hd:(k + 1) * hd, :]
                shift = (s * hd - k * hd) % COLS
                if shift:
                    strip = pltpu.roll(strip, shift, 1)
                picked.append(strip[:, :LANES])
            rest = 0.0
            if extra is not None:
                for i, col in enumerate(extra):
                    for s in range(2):
                        r0 = (2 * d + s) * hd
                        rest = jnp.where(lane_w == 2 * hd + 2 * i + s, col[r0:r0 + hd], rest)
            out_ref[d % 2, d // 2] = jnp.where(lane_w < hd, picked[0], jnp.where(lane_w < 2 * hd, picked[1], rest))

    def gram(b, l_ref, l0, r_ref, r0):
        blocks = []
        for w in range(nwin):
            m = min(wrow, dim - w * wrow)
            lo, ro = l0 + w * wrow, r0 + w * wrow
            nw = min(COLS, dim - w * wrow)
            left_op = l_ref[lo:lo + m, b * tokens:(b + 1) * tokens]
            right_op = r_ref[ro:ro + nw, b * tokens:(b + 1) * tokens]
            g = mm(left_op, right_op, NT)
            if nw < COLS:
                g = jnp.pad(g, ((0, 0), (0, COLS - nw)))
            blocks.append(g)
        return blocks

    def qk_tile(off, following, wt_cols=None):
        if wt_cols == dim:
            wt_v[dim:2 * dim, :] = w_v[:, dim:2 * dim].T
        for m in range(2):
            z = mm(wt_v[m * dim:(m + 1) * dim, :], ut[:, pl.ds(off, TOK)]).astype(BF16)
            zt[m * dim:(m + 1) * dim, pl.ds(off, TOK)] = z
            zf = z.astype(F32)
            sq = zf * zf
            tot = sq[:, 0:LANES]
            for j in range(1, TOK // LANES):
                tot = tot + sq[:, j * LANES:(j + 1) * LANES]
            sq_acc[off // tokens, m * dim:(m + 1) * dim] += tot
        if following is not None:
            norm_rows(following, TOK)
        if wt_cols is not None and wt_cols > dim:
            wt_v[wt_cols:wt_cols + dim // 2, :] = w_v[:, wt_cols:wt_cols + dim // 2].T

    def send_gram(b):
        cols = [jnp.sum(sq_acc[b, m * dim:(m + 1) * dim], axis=1, keepdims=True) for m in range(2)]
        to_pairs(gram(b, zt, 0, zt, dim), gs_out.at[b], cols)
        if b == 0:
            pl.semaphore_wait(barrier, n - 1)
        pair_sum(gs_out, gs_mid, gs_s, gs_r, b).start()

    for b in range(1, images):
        for t in range(tiles):
            cp_x(b, t).start()
    phase(norm_rows, 0, TOK)
    cp_wq.wait()
    cp_wv.start()
    cp_wo.start()
    for b in range(images):
        cp_dy(b).start()
    transpose_w(0, dim)
    cp_x(0, 1).wait()
    cp_wk.wait()
    phase(qk_tile, 0, TOK, dim)
    for t in range(tiles):
        cp_x(1, t).wait()
    for t in range(1, tiles):
        phase(qk_tile, t * TOK, (t + 1) * TOK)
    phase(send_gram, 0)
    cp_wv.wait()
    for t in range(tiles):
        if t == 1:
            phase(scatter_state, gs_out, gs_mid, gs_in, gs_s, gs_r, 0)
        off = tokens + t * TOK
        phase(qk_tile, off, off + TOK if t + 1 < tiles else None, 2 * dim + t * dim // tiles)
    phase(send_gram, 1)

    def values(b):
        for t in range(tiles):
            tok_t = pl.ds(b * tokens + t * TOK, TOK)
            zt[2 * dim:3 * dim, tok_t] = mm(wt_v[2 * dim:3 * dim, :], ut[:, tok_t]).astype(BF16)

    eye = lax.broadcasted_iota(jnp.int32, (hd, hd), 0) == lax.broadcasted_iota(jnp.int32, (hd, hd), 1)

    def row_of(col):
        return jnp.sum(jnp.where(eye, col, 0.0), axis=0, keepdims=True)

    head_lane = lax.broadcasted_iota(jnp.int32, (1, heads), 1)
    tau_row = tau_ref[...].reshape(1, heads)

    def attn_state(b, s):
        blk = gs_sum[b]
        g = blk[:, s * hd:(s + 1) * hd]
        qc = blk[:, 2 * hd + s:2 * hd + s + 1]
        kr = row_of(blk[:, 2 * hd + 2 + s:2 * hd + 3 + s])
        unit = lax.rsqrt(qc) * lax.rsqrt(kr)
        tau = jnp.sum(jnp.where(head_lane == me * 2 + s, tau_row, 0.0), axis=1, keepdims=True)
        cosine = g * unit
        logits = tau * cosine
        e = jnp.exp(logits - jnp.max(logits, axis=-1, keepdims=True))
        probs = e / jnp.sum(e, axis=-1, keepdims=True)
        return cosine, logits, probs, tau * unit, qc, kr

    def pair(a0, a1):
        r = a0.shape[0]
        z = jnp.zeros((r, LANES - 2 * hd), a0.dtype)
        return jnp.concatenate([a0, a1, z], axis=1)

    def owner_forward(b):
        chips_in(gs_in, gs_s, gs_r, b)
        gs_sum[b] = state_total(gs_out, gs_in, gs_s, gs_r, b)
        p0 = attn_state(b, 0)[2]
        p1 = attn_state(b, 1)[2]
        a_all[b, me] = pair(p0, p1).astype(BF16)
        for k in far_first:
            dst = (me + k) % n
            rcopy(a_all.at[b, me], a_all.at[b, me], a_s.at[0], a_r.at[b, 0], dst).start()

    def owner_backward():
        for b in range(images):
            chips_in(ds_in, ds_s, ds_r, b)
        sub = lax.broadcasted_iota(jnp.int32, (8, LANES), 0)
        lane = lax.broadcasted_iota(jnp.int32, (8, LANES), 1)
        for b in range(images):
            tot = state_total(ds_out, ds_in, ds_s, ds_r, b).astype(BF16).astype(F32)
            gs, qs, ks, ts = [], [], [], []
            for s in range(2):
                cosine, logits, probs, scale, qc, kr = attn_state(b, s)
                dp = tot[:, s * hd:(s + 1) * hd]
                gl = probs * (dp - jnp.sum(probs * dp, axis=-1, keepdims=True))
                weighted = gl * logits
                gs.append(gl * scale)
                qs.append(row_of(-jnp.sum(weighted, axis=1, keepdims=True) / qc))
                ks.append(-jnp.sum(weighted, axis=0, keepdims=True) / kr)
                ts.append(jnp.sum(jnp.sum(gl * cosine, axis=1, keepdims=True), axis=0, keepdims=True))
            g_all[b, me] = pair(gs[0], gs[1]).astype(BF16)
            taus = jnp.where(lane == 0, ts[0], jnp.where(lane == 1, ts[1], 0.0))
            c_all[b, me] = jnp.where(sub == 0, pair(qs[0], qs[1]), jnp.where(sub == 1, pair(ks[0], ks[1]), jnp.where(sub == 2, taus, 0.0)))
        for b in range(images):
            for ref, ss, rs in states:
                for k in (4, 2, 6, 1):
                    dst = (me + k) % n if k > 1 else partner
                    rcopy(ref.at[b, me], ref.at[b, me], ss.at[0], rs.at[b, 1 if k == 1 else 0], dst).start()

    states = ((g_all, g_s, g_r), (c_all, c_s, c_r))

    def pass_on(b):
        for ref, ss, rs in states:
            got = ref.at[b, pl.ds(0, chips - 1)]
            rcopy(got, got, ss.at[0], rs.at[b, 0], partner).wait_recv()
            for k in (2, 6, 4):
                src = (me + n - k) % n
                rcopy(ref.at[b, src], ref.at[b, src], ss.at[0], rs.at[b, 1], partner).start()

    def passed(b):
        for ref, ss, rs in states:
            got = ref.at[b, pl.ds(0, chips)]
            rcopy(got, got, ss.at[0], rs.at[b, 1], partner).wait_recv()

    def gathered(ref, ss, rs, b):
        got = ref.at[b, most]
        rcopy(got, got, ss.at[0], rs.at[b, 0], partner).wait_recv()

    def grad_heads(b):
        cp_dy(b).wait()
        if b == 0:
            cp_wo.wait()

        for t in range(tiles):
            tok_t = pl.ds(b * tokens + t * TOK, TOK)
            dot_v[:, tok_t] = mm(wo_v[...], dy_v[tok_t, :], NT).astype(BF16)

    def send_dprobs(b):
        to_pairs(gram(b, dot_v, 0, zt, 2 * dim), ds_out.at[b])
        pair_sum(ds_out, ds_mid, ds_s, ds_r, b).start()

    sj = lax.broadcasted_iota(jnp.int32, (LANES, COLS), 0)
    slane = lax.broadcasted_iota(jnp.int32, (LANES, COLS), 1)
    sels = []
    for s in range(2):
        hit = jnp.zeros((LANES, COLS), jnp.bool_)
        for k in range(wheads):
            hit = jnp.logical_or(hit, slane - k * hd == sj - s * hd)
        hit = jnp.logical_and(hit, jnp.logical_and(sj >= s * hd, sj < (s + 1) * hd))
        sels.append(jnp.where(hit, 1.0, 0.0).astype(BF16))
    blane = lax.broadcasted_iota(jnp.int32, (hd, COLS), 1)

    def build(ref, b):
        flat = ref[b].reshape(n * hd, LANES)
        for s in range(2):
            spread = mm(flat, sels[s])
            for d in range(n):
                w, k = divmod(2 * d + s, wheads)
                blk = jnp.where(jnp.logical_and(blane >= k * hd, blane < (k + 1) * hd), spread[d * hd:(d + 1) * hd], 0.0)
                bd[b, w, 0, k * hd:(k + 1) * hd, :] = blk.astype(BF16)
        for w in range(nwin):
            bd[b, w, 1] = bd[b, w, 0].T

    def windows():
        for w in range(nwin):
            r0 = w * wrow
            yield w, r0, min(wrow, dim - r0), min(COLS, dim - r0)

    def heads_out(b):
        for t in range(tiles):
            tok_t = pl.ds(b * tokens + t * TOK, TOK)
            for w, r0, m, kk in windows():
                ot[r0:r0 + m, tok_t] = mm(bd[b, w, 0, 0:m, 0:kk], zt[2 * dim + r0:2 * dim + r0 + kk, tok_t]).astype(BF16)

    def grad_values(b):
        def body(t, _):
            off = pl.multiple_of(b * tokens + t * TOK, TOK)
            for w, r0, m, kk in windows():
                zt[2 * dim + r0:2 * dim + r0 + m, pl.ds(off, TOK)] = mm(bd[b, w, 1, 0:m, 0:kk], dot_v[r0:r0 + kk, pl.ds(off, TOK)]).astype(BF16)
            return 0
        lax.fori_loop(0, tiles, body, 0)

    def dq_and_dk(b):
        ct = c_all[b].reshape(n * 8, LANES).T
        for d in range(n):
            colq[d * per_dev:(d + 1) * per_dev, :] = jnp.broadcast_to(ct[0:per_dev, 8 * d:8 * d + 1], (per_dev, LANES))
            colk[d * per_dev:(d + 1) * per_dev, :] = jnp.broadcast_to(ct[0:per_dev, 8 * d + 1:8 * d + 2], (per_dev, LANES))

        def body(t, _):
            off = pl.multiple_of(b * tokens + t * TOK, TOK)
            for w, r0, m, kk in windows():
                qw = zt[r0:r0 + kk, pl.ds(off, TOK)]
                kw = zt[dim + r0:dim + r0 + kk, pl.ds(off, TOK)]
                cq = jnp.concatenate([colq[r0:r0 + m, :]] * (TOK // LANES), axis=1)
                ck = jnp.concatenate([colk[r0:r0 + m, :]] * (TOK // LANES), axis=1)
                dq = mm(bd[b, w, 0, 0:m, 0:kk], kw) + cq * qw[0:m].astype(F32)
                dk = mm(bd[b, w, 1, 0:m, 0:kk], qw) + ck * kw[0:m].astype(F32)
                zt[r0:r0 + m, pl.ds(off, TOK)] = dq.astype(BF16)
                zt[dim + r0:dim + r0 + m, pl.ds(off, TOK)] = dk.astype(BF16)
            return 0
        lax.fori_loop(0, tiles, body, 0)

    def put_part(c, val):
        for j in range(n):
            part[c, j % 2, j // 2] = val[j * per_dev:(j + 1) * per_dev, :]

    def d2d(c):
        return rcopy(part.at[c, 1 - core], r1.at[c], d2d_s.at[0], d2d_r.at[c], partner)

    half = per_dev // 2

    def hop1(c):
        return (rcopy(r1.at[c, co, pl.ds(0, half)], r2.at[c, 0], p1_s.at[0], p1_r.at[c], right),
                rcopy(r1.at[c, co, pl.ds(half, half)], r2.at[c, 1], p1_s.at[0], p1_r.at[c], left))

    def hop2(c):
        return (rcopy(r1.at[c, cr], r3.at[c, 0], p2_s.at[0], p2_r.at[c], right),
                rcopy(r1.at[c, cl], r3.at[c, 1], p2_s.at[0], p2_r.at[c], left))

    def serve1(c):
        d2d(c).wait_recv()
        for blk in (co, cr, cl, chip):
            r1[c, blk] += part[c, core, blk]
        for h in hop1(c):
            h.start()

    def serve2(c):
        rcopy(r2.at[c], r2.at[c], p1_s.at[0], p1_r.at[c], partner).wait_recv()
        r1[c, cr, 0:half] += r2[c, 0]
        r1[c, cl, half:per_dev] += r2[c, 1]
        for h in hop2(c):
            h.start()

    def serve3(c):
        rcopy(r3.at[c], r3.at[c], p2_s.at[0], p2_r.at[c], partner).wait_recv()
        return (r1[c, chip] + r3[c, 0] + r3[c, 1]).astype(BF16)

    def wo_chunk(c):
        off = pl.multiple_of(c * COLS, COLS)
        put_part(c, mm(ot[...], dy_v[:, pl.ds(off, COLS)]))
        d2d(c).start()

    def qkv_chunk(c, base):
        off = pl.multiple_of(base + c * COLS, COLS)
        put_part(c, mm(ut[...], zt[pl.ds(off, COLS), :], NT))
        d2d(c).start()

    phase(values, 0)
    phase(scatter_state, gs_out, gs_mid, gs_in, gs_s, gs_r, 1)
    phase(grad_heads, 0)
    phase(owner_forward, 0)
    phase(send_dprobs, 0)
    phase(values, 1)
    phase(scatter_state, ds_out, ds_mid, ds_in, ds_s, ds_r, 0)
    phase(owner_forward, 1)
    phase(grad_heads, 1)
    phase(send_dprobs, 1)
    gathered(a_all, a_s, a_r, 0)
    phase(build, a_all, 0)
    phase(heads_out, 0)
    phase(scatter_state, ds_out, ds_mid, ds_in, ds_s, ds_r, 1)
    gathered(a_all, a_s, a_r, 1)
    phase(build, a_all, 1)
    phase(heads_out, 1)

    def wo_loop(c, _):
        wo_chunk(c)

        @pl.when(c > 0)
        def _():
            serve1(c - 1)
        return 0
    lax.fori_loop(0, o_chunks, wo_loop, 0)
    phase(owner_backward)
    serve1(o_chunks - 1)
    grad_values(0)
    grad_values(1)
    v0 = 2 * dim - o_chunks * COLS
    qkv_chunk(o_chunks, v0)

    def s2_body(c, _):
        serve2(c)
        return 0

    def serve2_range(c0, c1):
        lax.fori_loop(c0, c1, s2_body, 0)

    serve2_range(0, 2)

    def v_loop(c, _):
        qkv_chunk(c, v0)
        serve1(c - 1)
        return 0
    lax.fori_loop(o_chunks + 1, 2 * o_chunks, v_loop, 0)
    for b in range(images):
        pass_on(b)
    serve2_range(2, 3)
    for b in range(images):
        passed(b)
        phase(build, g_all, b)
        dq_and_dk(b)
        if b == 0:
            serve1(2 * o_chunks - 1)
    serve2_range(3, 4)
    qkv_chunk(2 * o_chunks, -2 * o_chunks * COLS)

    def qk_loop(c, _):
        qkv_chunk(c, -2 * o_chunks * COLS)
        serve1(c - 1)
        return 0
    lax.fori_loop(2 * o_chunks + 1, chunks, qk_loop, 0)
    serve1(chunks - 1)
    serve2_range(4, chunks - 3)

    def tile_copy(i, t):
        rows_t = pl.ds(pl.multiple_of(t * TOK, TOK), TOK)
        src, dst = ((x_v, y_hbm), (dy_v, dx_hbm))[i]
        return pltpu.make_async_copy(src.at[rows_t], dst.at[rows_t], out_sem.at[i])

    def dx_body(t, _):
        off = pl.multiple_of(t * TOK, TOK)
        dot_v[:, pl.ds(off, TOK)] = mm(w_v[...], zt[:, pl.ds(off, TOK)]).astype(BF16)

        def piece(i, _):
            r = pl.ds(pl.multiple_of(off + i * LANES, LANES), LANES)
            du = dot_v[:, r].T.astype(F32)
            xt = x_v[r, :].astype(F32)
            x_v[r, :] = (xt + mm(ot[:, r].T, wo_v[...])).astype(BF16)
            x_hat, inv = norm(xt)
            prod = du * x_hat
            dgb[0] += jnp.sum(prod.reshape(LANES // 8, 8, dim), axis=0)
            dgb[1] += jnp.sum(du.reshape(LANES // 8, 8, dim), axis=0)
            a9 = du * gain_row
            m1 = jnp.sum(a9, axis=-1, keepdims=True) * (1.0 / dim)
            m2 = jnp.sum(a9 * x_hat, axis=-1, keepdims=True) * (1.0 / dim)
            gx = inv * (a9 - m1 - x_hat * m2)
            dy_v[r, :] = (dy_v[r, :].astype(F32) + gx).astype(BF16)
            return 0
        lax.fori_loop(0, TOK // LANES, piece, 0)
        tile_copy(0, t).start()
        tile_copy(1, t).start()
        return 0

    lax.fori_loop(0, 1, dx_body, 0)
    serve2_range(chunks - 3, chunks)
    lax.fori_loop(1, images * tiles, dx_body, 0)
    gb_all[me] = jnp.concatenate([jnp.sum(dgb[i], axis=0).reshape(dim // LANES, LANES) for i in range(2)], axis=0)
    for k in far_first:
        rcopy(gb_all.at[me], gb_all.at[me], gb_s.at[0], gb_r.at[0], (me + k) % n).start()

    lane = lax.broadcasted_iota(jnp.int32, (1, LANES), 1)
    dtau = jnp.zeros((1, LANES), F32)
    for d in range(n):
        row = c_all[0, d, 2:3, :]
        for b in range(1, images):
            row = row + c_all[b, d, 2:3, :]
        if d:
            row = pltpu.roll(row, 2 * d, 1)
        dtau = jnp.where(jnp.logical_and(lane >= 2 * d, lane < 2 * d + 2), row, dtau)
    dtau_ref[...] = dtau

    def chunk_copy(c, src, dst, base, which):
        cols = pl.ds(pl.multiple_of(base + c * COLS, COLS), COLS)
        return pltpu.make_async_copy(src.at[:, cols], dst.at[:, cols], w_sem.at[which])

    def finish_chunks(c0, c1, src, dst, base, which):
        def body(c, _):
            src[:, pl.ds(pl.multiple_of(base + c * COLS, COLS), COLS)] = serve3(c)
            chunk_copy(c, src, dst, base, which).start()
            return 0
        lax.fori_loop(c0, c1, body, 0)

    finish_chunks(0, o_chunks, dwo_ref, dwo_hbm, 0, 0)
    finish_chunks(o_chunks, 2 * o_chunks, dwqkv_ref, dwqkv_hbm, v0, 1)

    got = gb_all.at[most]
    rcopy(got, got, gb_s.at[0], gb_r.at[0], partner).wait_recv()
    tot = gb_all[0]
    for d in peers:
        tot = tot + gb_all[d]
    dgain_ref[...] = tot[:dim // LANES]
    dbias_ref[...] = tot[dim // LANES:]
    small_copies = [pltpu.make_async_copy(v, h, w_sem.at[2 + i]) for i, (v, h) in enumerate(
        ((dgain_ref, dgain_hbm), (dbias_ref, dbias_hbm), (dtau_ref, dtau_hbm)))]
    for c in small_copies:
        c.start()
    finish_chunks(2 * o_chunks, chunks, dwqkv_ref, dwqkv_hbm, -2 * o_chunks * COLS, 1)

    sent = (
        (gs_mid, gs_s, 0), (gs_in.at[:, others], gs_s, 1),
        (ds_mid, ds_s, 0), (ds_in.at[:, others], ds_s, 1),
        (a_all.at[:, most], a_s, 0), (g_all.at[:, most], g_s, 0), (c_all.at[:, most], c_s, 0),
        (gb_all.at[most], gb_s, 0), (r1, d2d_s, 0), (r2, p1_s, 0), (r3, p2_s, 0))
    for ref, sem, i in sent:
        rcopy(ref, ref, sem.at[i], gb_r.at[0], partner).wait_send()
    pltpu.make_async_copy(x_v, y_hbm, out_sem.at[0]).wait()
    pltpu.make_async_copy(dy_v, dx_hbm, out_sem.at[1]).wait()
    for c in small_copies:
        c.wait()
    pltpu.make_async_copy(dwo_ref, dwo_hbm, w_sem.at[0]).wait()
    pltpu.make_async_copy(dwqkv_ref, dwqkv_hbm, w_sem.at[1]).wait()


def finish_kernel(heads, y_hbm, dx_hbm, *refs):
    moved, outputs, (buf, *stage, sem_in, sem_out) = refs[:5], refs[5:12], refs[12:]
    landed, shaped = stage[:5], stage[:2] + stage[5:]
    images, tokens, _dim = outputs[0].shape
    parts = tokens // TOK
    ins, outs = [], []

    def copy(src, dst, sem, into):
        into.append(pltpu.make_async_copy(src, dst, sem.at[len(into)]))

    for src, dst in ((y_hbm, outputs[0]), (dx_hbm, outputs[1])):
        for b in range(images):
            for t in range(parts):
                slot = buf.at[len(ins)]
                copy(src.at[pl.ds((b * parts + t) * TOK, TOK)], slot, sem_in, ins)
                copy(slot, dst.at[b, pl.ds(t * TOK, TOK)], sem_out, outs)
    big = len(ins)
    for src, mid, last, dst in zip(moved, landed, shaped, outputs[2:]):
        copy(src, mid, sem_in, ins)
        copy(last, dst, sem_out, outs)
    for c in ins:
        c.start()
    for c in ins[big:]:
        c.wait()
    for mid, last in zip(landed[2:], shaped[2:]):
        last[...] = mid[...].reshape(mid.size)[:last.shape[0]]
    for o in outs[big:]:
        o.start()
    for c, o in zip(ins[:big], outs[:big]):
        c.wait()
        o.start()
    for o in outs:
        o.wait()


def solution(mesh):
    n = mesh.shape["sp"]

    def local_step(x_in, grad_y, ln_gain, ln_bias, w_qkv, w_out, temp_tau):
        images, tokens, dim = x_in.shape
        heads = temp_tau.shape[0]
        hd = dim // heads
        rows = images * tokens
        per_dev = dim // n
        chunks = 4 * dim // COLS
        nwin = -(-heads // (COLS // hd))
        any_spec = pl.BlockSpec(memory_space=pl.ANY)
        dma = pltpu.SemaphoreType.DMA
        one, pairs = dma((1,)), dma((images, 2))
        out = pl.pallas_call(
            functools.partial(xca_kernel, n, heads),
            out_shape=(
                jax.ShapeDtypeStruct((rows, dim), BF16),
                jax.ShapeDtypeStruct((rows, dim), BF16),
                jax.ShapeDtypeStruct((per_dev, 3 * dim), BF16),
                jax.ShapeDtypeStruct((per_dev, dim), BF16),
                jax.ShapeDtypeStruct((dim // LANES, LANES), F32),
                jax.ShapeDtypeStruct((dim // LANES, LANES), F32),
                jax.ShapeDtypeStruct((1, LANES), F32),
            ),
            in_specs=[any_spec] * 7,
            out_specs=(any_spec,) * 7,
            scratch_shapes=[
                pltpu.VMEM((per_dev, 3 * dim), BF16),
                pltpu.VMEM((per_dev, dim), BF16),
                pltpu.VMEM((dim // LANES, LANES), F32),
                pltpu.VMEM((dim // LANES, LANES), F32),
                pltpu.VMEM((1, LANES), F32),
                pltpu.VMEM((dim,), F32),
                pltpu.VMEM((dim,), F32),
                pltpu.VMEM((heads,), F32),
                pltpu.VMEM((rows, dim), BF16),
                pltpu.VMEM((rows, dim), BF16),
                pltpu.VMEM((dim, 3 * dim), BF16),
                pltpu.VMEM((3 * dim, dim), BF16),
                pltpu.VMEM((dim, dim), BF16),
                pltpu.VMEM((dim, rows), BF16),
                pltpu.VMEM((3 * dim, rows), BF16),
                pltpu.VMEM((dim, rows), BF16),
                pltpu.VMEM((dim, rows), BF16),
                pltpu.VMEM((images, 2 * dim, LANES), F32),
                pltpu.VMEM((images, 2, n // 2, hd, LANES), F32),
                pltpu.VMEM((images, n // 2, hd, LANES), F32),
                pltpu.VMEM((images, n // 2, hd, LANES), F32),
                pltpu.VMEM((images, hd, LANES), F32),
                pltpu.VMEM((images, n, hd, LANES), BF16),
                pltpu.VMEM((images, 2, n // 2, hd, LANES), F32),
                pltpu.VMEM((images, n // 2, hd, LANES), F32),
                pltpu.VMEM((images, n // 2, hd, LANES), F32),
                pltpu.VMEM((images, n, hd, LANES), BF16),
                pltpu.VMEM((images, n, 8, LANES), F32),
                pltpu.VMEM((images, nwin, 2, COLS, COLS), BF16),
                pltpu.VMEM((dim, LANES), F32),
                pltpu.VMEM((dim, LANES), F32),
                pltpu.VMEM((2, 8, dim), F32),
                pltpu.VMEM((n, 2 * dim // LANES, LANES), F32),
                pltpu.VMEM((chunks, 2, n // 2, per_dev, COLS), F32),
                pltpu.VMEM((chunks, n // 2, per_dev, COLS), F32),
                pltpu.VMEM((chunks, 2, per_dev // 2, COLS), F32),
                pltpu.VMEM((chunks, 2, per_dev, COLS), F32),
                dma((rows // TOK + images + 7,)), dma((2,)), dma((5,)),
                one, dma((chunks,)), one, dma((chunks,)), one, dma((chunks,)),
                dma((2,)), pairs, one, pairs, dma((2,)), pairs,
                one, pairs, one, pairs, one, one,
            ],
            compiler_params=pltpu.CompilerParams(
                collective_id=0, has_side_effects=True, vmem_limit_bytes=VMEM_LIMIT),
            name="xca_block",
        )(x_in, grad_y, ln_gain, ln_bias, w_qkv, w_out, temp_tau)
        return pl.pallas_call(
            functools.partial(finish_kernel, heads),
            out_shape=(
                jax.ShapeDtypeStruct(x_in.shape, BF16),
                jax.ShapeDtypeStruct(x_in.shape, BF16),
                jax.ShapeDtypeStruct((per_dev, 3 * dim), BF16),
                jax.ShapeDtypeStruct((per_dev, dim), BF16),
                jax.ShapeDtypeStruct((dim,), F32),
                jax.ShapeDtypeStruct((dim,), F32),
                jax.ShapeDtypeStruct((heads,), F32),
            ),
            in_specs=[any_spec] * 7,
            out_specs=(any_spec,) * 7,
            scratch_shapes=[
                pltpu.VMEM((2 * rows // TOK, TOK, dim), BF16),
                pltpu.VMEM((per_dev, 3 * dim), BF16),
                pltpu.VMEM((per_dev, dim), BF16),
                pltpu.VMEM((dim // LANES, LANES), F32),
                pltpu.VMEM((dim // LANES, LANES), F32),
                pltpu.VMEM((1, LANES), F32),
                pltpu.VMEM((dim,), F32),
                pltpu.VMEM((dim,), F32),
                pltpu.VMEM((heads,), F32),
                dma((2 * rows // TOK + 5,)), dma((2 * rows // TOK + 5,)),
            ],
            name="finish",
        )(*out)

    tok = P("dp", "sp", None)
    return jax.shard_map(
        local_step, mesh=mesh,
        in_specs=(tok, tok, P(), P(), P(), P(), P()),
        out_specs=(tok, tok, P(("dp", "sp"), None), P(("dp", "sp"), None), P("dp"), P("dp"), P("dp")),
        check_vma=False)
```
